128 devices in a mesh: gx: 32 (over y, z, core), gy: 4 (over x).
Axes of the slice: x: 4, y: 4, z: 4, core: 2. Of those that a mesh axis runs over, the one named last changes fastest.
Arguments:
- emb_table: float32 [262144, 128], P(('gx', 'gy')), may hold values from -0.6 to 0.6
- row_state: float32 [262144], P(('gx', 'gy')), may hold values from 1e-05 to 0.001
- pair_mask: int32 [32], P('gx'), may hold values from 0 to 3
- look_rows: int32 [786432], P(('gx', 'gy')), may hold values from 0 to 2047
- bag_sizes: int32 [128, 2048], P(('gx', 'gy')), may hold values from 1 to 12, 6144 in all within a row
- bag_owner: int32 [262144, 1], P(('gx', 'gy')), may hold values from 0 to 127, as said below
- bag_slot: int32 [262144], P(('gx', 'gy')), may hold values from 0 to 2047, as said below
- dense_vectors: float32 [16384, 128], P(('gx', 'gy')), may hold values from -3 to 3
- labels: float32 [16384], P(('gx', 'gy')), may hold values from 0 to 1
- top_weight: float32 [264, 1024], replicated, may hold values from -0.375 to 0.375
- out_weight: float32 [1024], replicated, may hold values from -0.1875 to 0.1875
Outputs:
- moved_table: float32 [262144, 128], P(('gx', 'gy'))
- moved_state: float32 [262144], P(('gx', 'gy'))
- top_grad: float32 [264, 1024], replicated
- out_grad: float32 [1024], replicated
The draws below stay inside these ranges and needn't reach their ends.
Inputs may be any that keep to these rules, and one draw needn't show every extreme that they name: Device (g, y) trades with device (g, y xor pair_mask[g]); 0 keeps the block. `look_rows`: a row of the block that the device holds after the trade. `bag_sizes`: each device's sizes sum to 6144. `bag_owner`: among one device's 2048 bags every owner is named either never or exactly 32 times; each owner is named so by exactly half of the devices. `bag_slot`: sample times 16 plus feature; the bags that reach one owner name every one of its slots exactly once.
All inputs are finite; a program needn't handle non-finite values.
Results may differ from the reference program's by a relative error of at most 0.0003.
Values sent between devices are 32-bit elements; how exact they have to be, the bound alone decides.
A program may use at most 64 MiB of HBM per device.

```python
import math
import jax
import jax.numpy as jnp
import numpy as np
from jax import lax

E = 128
F = 16
H1 = 1024
ROWS_DEV = 2048
B_DEV = 128
BAG_MOST = 12
BAGS_DEV = 2048
LOOK_DEV = 6144
CAP = 32
INTER = 264
ROWS = 262144
SAMPLES = 16384
N_GX = 32
N_GY = 4
DEVICES = 128


def plan_routes(key):
    folded = jax.random.fold_in(key, 7001)
    first_key, second_key, third_key = jax.random.split(folded, 3)
    offsets = jax.random.permutation(first_key, DEVICES).astype(jnp.int32)
    ordering = jax.vmap(lambda k: jax.random.permutation(k, BAGS_DEV))(jax.random.split(second_key, DEVICES)).astype(jnp.int32)
    owners = (offsets[:, None] + ordering // CAP) % DEVICES
    spread = jax.vmap(lambda k: jax.random.permutation(k, BAGS_DEV))(jax.random.split(third_key, DEVICES)).astype(jnp.int32)
    slots = spread[owners, ordering] % (B_DEV * F)
    return (owners.astype(jnp.int32), slots.astype(jnp.int32))


def draw_bag_owner(key, part):
    owners, slots = plan_routes(key)
    return owners.reshape(DEVICES * BAGS_DEV, 1)


def draw_bag_slot(key, part):
    owners, slots = plan_routes(key)
    return slots.reshape(DEVICES * BAGS_DEV)


def with_ends(values, key, smallest, top_value):
    longest = values.shape.index(max(values.shape))
    spots = []
    for shift in (0, 1):
        where = [jax.random.randint(jax.random.fold_in(key, axis), (), 0, length) for axis, length in enumerate(values.shape)]
        where[longest] = (where[longest] + shift) % values.shape[longest]
        spots.append(tuple(where))
    return values.at[spots[0]].set(smallest).at[spots[1]].set(top_value)


def steps_of(stream_key, extent, shards, least, high):
    gain, own = 1.0, jax.random.fold_in(stream_key, 6)
    for dim, blocks in shards:
        steps = jnp.exp(jax.random.uniform(jax.random.fold_in(own, dim), (blocks,), jnp.float32, least / len(shards), high / len(shards)))
        gain = gain * jnp.repeat(steps, extent[dim] // blocks).reshape([-1 if axis == dim else 1 for axis in range(len(extent))])
    return gain


def rank_bounds(amount, slope):
    loads = [(1 << 20) // math.isqrt(grade ** slope) + 1 for grade in range(1, amount + 1)]
    deviation = 1 + sum(loads) // (1 << 30)
    return np.cumsum(np.array([max(1, weight // deviation) for weight in loads]))


def ranked_ids(stream_key, dims, number_of, lean):
    listing = rank_bounds(number_of, lean)
    lot = jax.random.randint(jax.random.fold_in(stream_key, 1), dims, 0, int(listing[number_of - 1]))
    rank = jnp.searchsorted(jnp.asarray(listing, jnp.int32), lot, side="right")
    return jax.random.permutation(jax.random.fold_in(stream_key, 2), number_of)[rank].astype(jnp.int32)


def length_profile(number_of, total, bound, slope):
    weights = [(1 << 20) // math.isqrt(rank ** slope) + 1 for rank in range(2, number_of + 1)]
    surplus, given = total - bound - (number_of - 1), [1] * (number_of - 1)
    while surplus > 0:
        candidates = [i for i in range(number_of - 1) if given[i] < bound]
        pool, budget = sum([weights[i] for i in candidates]), surplus
        for i in candidates:
            extra = min(bound - given[i], max(1, budget * weights[i] // pool), surplus)
            given[i] = given[i] + extra
            surplus = surplus - extra
    return np.array([bound] + given)


def ragged(rng, count, total, limit, slope):
    if count == 2:
        one = jax.random.randint(rng, (), max(1, total - limit), min(limit, total - 1) + 1)
        return jnp.stack([one, total - one])
    lengths = jnp.asarray(length_profile(count, total, limit, slope), jnp.int32)
    couples = (count - 1) // 2
    donor, taker = lengths[1:1 + 2 * couples:2], lengths[2:2 + 2 * couples:2]
    slack = jnp.minimum(donor - 1, limit - taker)
    shifted = jax.random.randint(jax.random.fold_in(rng, 1), (couples,), 0, 1 << 20) % (slack + 1)
    lengths = lengths.at[1:1 + 2 * couples:2].set(donor - shifted).at[2:2 + 2 * couples:2].set(taker + shifted)
    return lengths[jax.random.permutation(jax.random.fold_in(rng, 2), count)]


def centred(rng, dims, scale, limit, cuts=(), kind=jnp.bfloat16):
    values = scale * jax.random.normal(rng, dims, jnp.float32)
    if cuts:
        values = values * steps_of(rng, dims, cuts, -0.22, 0.18)
    return jnp.clip(values, -limit, limit).astype(kind)


def setup_inputs(seed: int = 0) -> dict:
    key_of = jax.random.split(jax.random.key(seed), 12)
    emb_table = centred(key_of[0], (ROWS, E), 0.1, 0.6, ((0, 128),), jnp.float32)
    row_state = jnp.clip(jnp.exp(math.log(0.001) - 4.6051703 * jax.random.uniform(key_of[1], (ROWS,), jnp.float32) ** steps_of(key_of[1], (ROWS,), ((0, 128),), -0.2, 0.2)), 9.999999747378752e-06, 0.001)
    pair_mask = with_ends(jax.random.randint(key_of[2], (N_GX,), 0, N_GY), jax.random.fold_in(key_of[2], 1), 0, N_GY - 1).astype(jnp.int32)
    look_rows = with_ends(ranked_ids(key_of[3], (DEVICES * LOOK_DEV,), ROWS_DEV, 2), jax.random.fold_in(key_of[3], 3), 0, ROWS_DEV - 1).astype(jnp.int32)
    bag_sizes = jax.vmap(lambda own: ragged(own, BAGS_DEV, LOOK_DEV, BAG_MOST, 1))(jax.random.split(key_of[4], DEVICES)).reshape((DEVICES, BAGS_DEV)).astype(jnp.int32)
    bag_owner = draw_bag_owner(jax.random.fold_in(key_of[11], 71), 0)
    bag_slot = draw_bag_slot(jax.random.fold_in(key_of[11], 71), 0)
    dense_vectors = centred(key_of[7], (SAMPLES, E), 0.5, 3.0, ((0, 128),), jnp.float32)
    labels = jnp.clip(1.0 * jax.random.uniform(key_of[8], (SAMPLES,), jnp.float32) ** steps_of(key_of[8], (SAMPLES,), ((0, 128),), -0.2, 0.2), 0.0, 1.0)
    top_weight = centred(key_of[9], (INTER, H1), INTER ** -0.5, 0.375, (), jnp.float32)
    out_weight = centred(key_of[10], (H1,), H1 ** -0.5, 0.1875, (), jnp.float32)
    return dict(emb_table=emb_table, row_state=row_state, pair_mask=pair_mask, look_rows=look_rows, bag_sizes=bag_sizes, bag_owner=bag_owner, bag_slot=bag_slot, dense_vectors=dense_vectors, labels=labels, top_weight=top_weight, out_weight=out_weight)


learn_rate = 0.05
epsilon = 1e-08

def pair_terms(vectors):
    gram_all = jnp.einsum('bie,bje->bij', vectors, vectors, precision=lax.Precision.HIGHEST)
    upper_row, upper_col = np.triu_indices(F + 1, 1)
    return gram_all[:, upper_row, upper_col]

def sample_loss(pooled, dense_vectors, labels, top_weight, out_weight):
    sample_count = dense_vectors.shape[0]
    vectors = jnp.concatenate([dense_vectors[:, None, :], pooled.reshape(sample_count, F, E)], axis=1)
    interact = jnp.concatenate([dense_vectors, pair_terms(vectors)], axis=1)
    hidden = jax.nn.silu(jnp.dot(interact, top_weight, precision=lax.Precision.HIGHEST))
    logits = jnp.dot(hidden, out_weight, precision=lax.Precision.HIGHEST)
    return jnp.sum(jax.nn.softplus(logits) - labels * logits)

def bag_index(sizes_row, lookup_count):
    ending = jnp.cumsum(sizes_row)
    positions = jnp.arange(lookup_count, dtype=jnp.int32)
    return jnp.searchsorted(ending, positions, side='right').astype(jnp.int32)

def reference(emb_table, row_state, pair_mask, look_rows, bag_sizes, bag_owner, bag_slot, dense_vectors, labels, top_weight, out_weight):
    blocks = emb_table.reshape(N_GX, N_GY, ROWS_DEV, E)
    states = row_state.reshape(N_GX, N_GY, ROWS_DEV)
    column = jnp.arange(N_GY, dtype=jnp.int32)
    partner = jnp.bitwise_xor(column[None, :], pair_mask[:, None])
    groups = jnp.arange(N_GX, dtype=jnp.int32)[:, None]
    held_table = blocks[groups, partner].reshape(DEVICES, ROWS_DEV, E)
    held_state = states[groups, partner].reshape(DEVICES, ROWS_DEV)
    lookups = look_rows.reshape(DEVICES, LOOK_DEV)

    def pool_device(inputs):
        table_block, lookup_ids, sizes_row = inputs
        return jax.ops.segment_sum(table_block[lookup_ids], bag_index(sizes_row, LOOK_DEV), num_segments=BAGS_DEV)
    partial_value = lax.map(pool_device, (held_table, lookups, bag_sizes)).reshape(DEVICES * BAGS_DEV, E)
    target = bag_owner[:, 0] * (B_DEV * F) + bag_slot
    pooled = jax.ops.segment_sum(partial_value, target, num_segments=SAMPLES * F)
    d_pooled, top_grad, out_grad = jax.grad(sample_loss, argnums=(0, 3, 4))(pooled, dense_vectors, labels, top_weight, out_weight)
    d_partial = d_pooled[target].reshape(DEVICES, BAGS_DEV, E)

    def rows_device(inputs):
        bag_grads, lookup_ids, sizes_row = inputs
        return jax.ops.segment_sum(bag_grads[bag_index(sizes_row, LOOK_DEV)], lookup_ids, num_segments=ROWS_DEV)
    row_grad = lax.map(rows_device, (d_partial, lookups, bag_sizes))
    moved_state = held_state + lax.optimization_barrier(jnp.mean(row_grad * row_grad, axis=2))
    moved_table = held_table - learn_rate * row_grad / (jnp.sqrt(moved_state)[:, :, None] + epsilon)
    return (moved_table.reshape(ROWS, E), moved_state.reshape(ROWS), top_grad, out_grad)
```

```python
import jax
import jax.numpy as jnp
from jax import lax
from jax.experimental import pallas as pl
from jax.experimental.pallas import tpu as pltpu
from jax.sharding import PartitionSpec as P

E = 128
F = 16
B_DEV = 128
BAGS = 2048
ROWS = 2048
LOOKS = 6144
DEVICES = 128
CAP = 32
INTER = 264
HID = 1024
CHUNK = 256
SPAN = CHUNK + 16
C_ROWS = 2304
PAIRS = [(i, j) for i in range(F + 1) for j in range(i + 1, F + 1)]
PAIR_ROW = {pair: 128 + n for n, pair in enumerate(PAIRS)}

learn_rate = 0.05
epsilon = 1e-08
f32, bf16, i32 = jnp.float32, jnp.bfloat16, jnp.int32

VMEM = pl.BlockSpec(memory_space=pltpu.VMEM)
SMEM = pl.BlockSpec(memory_space=pltpu.SMEM)


def split(x):
    hi = x.astype(bf16)
    return hi, (x - hi.astype(f32)).astype(bf16)


def mxu(a, b, dims):
    return lax.dot_general(a, b, (dims, ((), ())), preferred_element_type=f32)


def dot3(a, b, dims):
    return mxu(a[0], b[0], dims) + (mxu(a[0], b[1], dims) + mxu(a[1], b[0], dims))


NN = ((1,), (0,))
NT = ((1,), (1,))


def down_sublanes(row):
    return jnp.broadcast_to(row, (128, 128)).T


def count_kernel(first_ref, look_ref, start_ref, end_ref, c_ref, start_t, end_t):
    for r in range(C_ROWS // 128):
        here = slice(r * 128, (r + 1) * 128)
        start_t[here, :] = down_sublanes(start_ref[r : r + 1, :])
        end_t[here, :] = down_sublanes(end_ref[r : r + 1, :])
    c_ref[0:16, :] = jnp.zeros((16, ROWS), bf16)
    lane = lax.broadcasted_iota(i32, (1, 128), 1)

    def chunk(t, carry):
        at = pl.multiple_of(first_ref[t], 16)
        start, end = start_t[pl.ds(at, SPAN), :], end_t[pl.ds(at, SPAN), :]
        halves, columns = [], []
        for h in range(2):
            k = lane + (t * CHUNK + h * 128)
            halves.append(((start <= k) & (k < end)).astype(f32).astype(bf16))
            columns.append(down_sublanes(look_ref[pl.ds(2 * t + h, 1), :]))
        in_bag = jnp.concatenate(halves, axis=1)
        column = jnp.concatenate(columns, axis=0)
        for n in range(0, 16, 4):
            of_row = jnp.concatenate(
                [(column == lane + 128 * q).astype(f32).astype(bf16) for q in range(n, n + 4)],
                axis=1,
            )
            counts = mxu(in_bag, of_row, NN)
            cols = slice(n * 128, (n + 4) * 128)
            before = c_ref[pl.ds(at, 16), cols].astype(f32)
            c_ref[pl.ds(at, 16), cols] = (counts[:16] + before).astype(bf16)
            c_ref[pl.ds(pl.multiple_of(at + 16, 16), SPAN - 16), cols] = counts[16:].astype(bf16)
        return carry

    lax.fori_loop(0, LOOKS // CHUNK, chunk, 0)


def pool_kernel(where_ref, c_ref, table_ref, send_ref, split_ref, partial_ref):
    hi, lo = split(table_ref[...])
    split_ref[:, :128] = hi
    split_ref[:, 128:] = lo

    def block(m, carry):
        at = pl.multiple_of(m * 256, 256)
        both = mxu(c_ref[pl.ds(at, 256), :], split_ref[...], NN)
        partial_ref[pl.ds(at, 256), :] = both[:, :128] + both[:, 128:]
        return carry

    lax.fori_loop(0, BAGS // 256, block, 0)

    def place(n, carry):
        for u in range(16):
            b = n * 16 + u
            send_ref[pl.ds(where_ref[b], 1), :] = partial_ref[pl.ds(b, 1), :]
        return carry

    lax.fori_loop(0, BAGS // 16, place, 0)


def dense_kernel(
    slot_ref, got_ref, dense_ref, label_ref, w_ref, wo_ref, back_ref, grad_ref, pooled, vt, inter_t
):
    def place(c, carry):
        @pl.when(slot_ref[c * CAP] < BAGS)
        def _():
            for u in range(CAP):
                p = c * CAP + u
                pooled[pl.ds(slot_ref[p], 1), :] = got_ref[pl.ds(p, 1), :]

        return carry

    lax.fori_loop(0, DEVICES, place, 0)

    dense_t = dense_ref[...].T
    vt[0] = dense_t
    inter_t[0:128, :] = dense_t
    for f in range(F):
        vt[f + 1] = pooled[f * 128 : (f + 1) * 128, :].T
    for i in range(F):
        for j in range(i + 1, F + 1):
            row = PAIR_ROW[i, j]
            inter_t[row : row + 1, :] = jnp.sum(vt[i] * vt[j], axis=0, keepdims=True)

    it = inter_t[...]
    w = split(w_ref[...])
    pre = dot3(split(it.T), w, NN)
    sig = 1.0 / (1.0 + jnp.exp(-pre))
    hidden = pre * sig
    logits = jnp.sum(hidden * wo_ref[...], axis=1, keepdims=True)
    d_logits = 1.0 / (1.0 + jnp.exp(-logits)) - label_ref[...]
    grad_ref[INTER : INTER + 8, :] = jnp.broadcast_to(
        jnp.sum(hidden * d_logits, axis=0, keepdims=True), (8, HID)
    )
    d_pre = split(d_logits * wo_ref[...] * (sig * (1.0 + pre * (1.0 - sig))))
    grad_ref[0:INTER, :] = dot3(split(it), d_pre, NN)
    inter_t[...] = dot3(w, d_pre, NT)

    for j in range(1, F + 1):
        total = None
        for i in range(F + 1):
            if i != j:
                row = PAIR_ROW[min(i, j), max(i, j)]
                term = inter_t[row : row + 1, :] * vt[i]
                total = term if total is None else total + term
        pooled[(j - 1) * 128 : j * 128, :] = total.T

    def give(c, carry):
        @pl.when(slot_ref[c * CAP] < BAGS)
        def _():
            for u in range(CAP):
                p = c * CAP + u
                back_ref[pl.ds(p, 1), :] = pooled[pl.ds(slot_ref[p], 1), :]

        return carry

    lax.fori_loop(0, DEVICES, give, 0)


def update_kernel(
    where_ref, c_ref, came_ref, table_ref, state_ref, new_table_ref, new_state_ref, grads, sides
):
    def take(n, carry):
        for u in range(16):
            b = n * 16 + u
            grads[pl.ds(b, 1), :] = came_ref[pl.ds(where_ref[b], 1), :]
        return carry

    lax.fori_loop(0, BAGS // 16, take, 0)
    for q in range(BAGS // 128):
        here = slice(q * 128, (q + 1) * 128)
        hi, lo = split(grads[here, :].T)
        sides[0:128, here] = hi
        sides[128:256, here] = lo

    def block(n, carry):
        here = pl.ds(pl.multiple_of(n * 256, 256), 256)
        both = mxu(sides[...], c_ref[0:BAGS, here], NN)
        row_grad = both[:128] + both[128:]
        state = state_ref[:, here] + jnp.sum(row_grad * row_grad, axis=0, keepdims=True) * (1.0 / E)
        new_state_ref[:, here] = state
        step = row_grad * (learn_rate / (jnp.sqrt(state) + epsilon))
        new_table_ref[here, :] = table_ref[here, :] - step.T
        return carry

    lax.fori_loop(0, ROWS // 256, block, 0)


def params(**kw):
    return pltpu.CompilerParams(**kw)


def from_partner(block, flip):
    return lax.ppermute(block, "gy", [(y, y ^ flip) for y in range(4)])


def trade_blocks(table, state, mask):
    first, second = (mask == 1) | (mask == 2), mask >= 2
    cut = ROWS // 2
    pieces = [table[:cut], jnp.concatenate([table[cut:], state.reshape(16, 128)], axis=0)]
    out = []
    for piece in pieces:
        piece = jnp.where(first, from_partner(piece, 1), piece)
        piece = jnp.where(second, from_partner(piece, 3), piece)
        out.append(piece)
    held = jnp.concatenate([out[0], out[1][:cut]], axis=0)
    return held, out[1][cut:].reshape(1, ROWS)


def swap_all(x):
    return lax.all_to_all(x, ("gx", "gy"), split_axis=0, concat_axis=0, tiled=True)


def on_device(
    emb_table,
    row_state,
    pair_mask,
    look_rows,
    bag_sizes,
    bag_owner,
    bag_slot,
    dense_vectors,
    labels,
    top_weight,
    out_weight,
):
    held, held_state = trade_blocks(emb_table, row_state, pair_mask[0])

    owners = bag_owner[:, 0]
    onehot = (owners[:, None] == jnp.arange(DEVICES, dtype=i32)[None, :]).astype(i32)
    placed_at = jnp.sum((jnp.cumsum(onehot, axis=0) - onehot) * onehot, axis=1)
    where_to = owners * CAP + placed_at
    spot = (placed_at[:, None] == jnp.arange(CAP, dtype=i32)[None, :]).astype(f32)
    sample, feature = bag_slot // F, bag_slot % F
    parts = jnp.concatenate(
        [spot * (sample.astype(f32)[:, None]), spot * ((feature + 1).astype(f32)[:, None])], axis=1
    )
    coded = mxu(onehot.astype(bf16), parts.astype(bf16), ((0,), (0,))).astype(i32)
    sample_at, feature_at = coded[:, :CAP], coded[:, CAP:]
    send_slots = jnp.where(feature_at > 0, (feature_at - 1) * B_DEV + sample_at, BAGS)
    got_slots = swap_all(send_slots).reshape(DEVICES * CAP)

    sizes = bag_sizes[0]
    ends = jnp.cumsum(sizes)
    starts = ends - sizes
    bounds = jnp.arange(LOOKS // CHUNK, dtype=i32) * CHUNK
    first_bag = jnp.sum((ends[None, :] <= bounds[:, None]).astype(i32), axis=1) // 16 * 16
    extra = C_ROWS - BAGS
    ends2 = jnp.concatenate([ends, jnp.zeros((extra,), i32)]).reshape(C_ROWS // 128, 128)
    starts2 = jnp.concatenate([starts, jnp.full((extra,), LOOKS, i32)]).reshape(C_ROWS // 128, 128)
    counts = pl.pallas_call(
        count_kernel,
        out_shape=jax.ShapeDtypeStruct((C_ROWS, ROWS), bf16),
        in_specs=[SMEM, VMEM, VMEM, VMEM],
        out_specs=VMEM,
        scratch_shapes=[pltpu.VMEM((C_ROWS, 128), i32), pltpu.VMEM((C_ROWS, 128), i32)],
        compiler_params=params(vmem_limit_bytes=24 << 20),
        cost_estimate=pl.CostEstimate(flops=2 * LOOKS * SPAN * ROWS, bytes_accessed=10 << 20, transcendentals=0),
        name="count",
    )(first_bag, look_rows.reshape(LOOKS // 128, 128), starts2, ends2)

    send_rows = pl.pallas_call(
        pool_kernel,
        out_shape=jax.ShapeDtypeStruct((DEVICES * CAP, E), f32),
        in_specs=[SMEM, VMEM, VMEM],
        out_specs=VMEM,
        scratch_shapes=[pltpu.VMEM((ROWS, 256), bf16), pltpu.VMEM((BAGS, E), f32)],
        compiler_params=params(vmem_limit_bytes=24 << 20),
        name="pool",
    )(where_to, counts, held)
    got_rows = swap_all(send_rows.reshape(DEVICES, CAP, E)).reshape(DEVICES * CAP, E)

    back_rows, grads = pl.pallas_call(
        dense_kernel,
        out_shape=(
            jax.ShapeDtypeStruct((DEVICES * CAP, E), f32),
            jax.ShapeDtypeStruct((INTER + 8, HID), f32),
        ),
        in_specs=[SMEM, VMEM, VMEM, VMEM, VMEM, VMEM],
        out_specs=(VMEM, VMEM),
        scratch_shapes=[
            pltpu.VMEM((BAGS, E), f32),
            pltpu.VMEM((F + 1, E, B_DEV), f32),
            pltpu.VMEM((INTER, B_DEV), f32),
        ],
        compiler_params=params(vmem_limit_bytes=24 << 20),
        name="dense",
    )(got_slots, got_rows, dense_vectors, labels[:, None], top_weight, out_weight[None, :])

    came_back = swap_all(back_rows.reshape(DEVICES, CAP, E)).reshape(DEVICES * CAP, E)
    total = lax.psum(grads[: INTER + 1], ("gx", "gy"))

    new_table, new_state = pl.pallas_call(
        update_kernel,
        out_shape=(
            jax.ShapeDtypeStruct((ROWS, E), f32),
            jax.ShapeDtypeStruct((1, ROWS), f32),
        ),
        in_specs=[SMEM, VMEM, VMEM, VMEM, VMEM],
        out_specs=(VMEM, VMEM),
        scratch_shapes=[pltpu.VMEM((BAGS, E), f32), pltpu.VMEM((2 * E, BAGS), bf16)],
        compiler_params=params(vmem_limit_bytes=24 << 20),
        name="update",
    )(where_to, counts, came_back, held, held_state)
    return new_table, new_state.reshape(ROWS), total[:INTER], total[INTER]


def solution(mesh):
    both = ("gx", "gy")
    in_specs = (
        P(both, None),
        P(both),
        P("gx"),
        P(both),
        P(both, None),
        P(both, None),
        P(both),
        P(both, None),
        P(both),
        P(),
        P(),
    )
    out_specs = (P(both, None), P(both), P(), P())
    return jax.shard_map(
        on_device, mesh=mesh, in_specs=in_specs, out_specs=out_specs, check_vma=False
    )
```

```python
import jax
import jax.numpy as jnp
from jax import lax
from jax.experimental import pallas as pl
from jax.experimental.pallas import tpu as pltpu
from jax.sharding import PartitionSpec as P

E = 128
F = 16
B_DEV = 128
BAGS = 2048
ROWS = 2048
LOOKS = 6144
DEVICES = 128
CAP = 32
INTER = 264
HID = 1024
CHUNK = 256
SPAN = CHUNK + 16
C_ROWS = 2304
G_ROWS = 2304
HALF = G_ROWS // 2
SEG = HALF // 16
PAIRS = [(i, j) for i in range(F + 1) for j in range(i + 1, F + 1)]
PAIR_ROW = {pair: 128 + n for n, pair in enumerate(PAIRS)}

learn_rate = 0.05
epsilon = 1e-08
MESH = pl.DeviceIdType.MESH
f32, bf16, i32 = jnp.float32, jnp.bfloat16, jnp.int32

VMEM = pl.BlockSpec(memory_space=pltpu.VMEM)
SMEM = pl.BlockSpec(memory_space=pltpu.SMEM)


def split(x):
    hi = x.astype(bf16)
    return hi, (x - hi.astype(f32)).astype(bf16)


def mxu(a, b, dims):
    return lax.dot_general(a, b, (dims, ((), ())), preferred_element_type=f32)


def dot3(a, b, dims):
    return mxu(a[0], b[0], dims) + (mxu(a[0], b[1], dims) + mxu(a[1], b[0], dims))


NN = ((1,), (0,))
NT = ((1,), (1,))


def down_sublanes(row):
    return jnp.broadcast_to(row, (128, 128)).T


def count_kernel(first_ref, look_ref, start_ref, end_ref, c_ref, start_t, end_t):
    for r in range(C_ROWS // 128):
        here = slice(r * 128, (r + 1) * 128)
        start_t[here, :] = down_sublanes(start_ref[r : r + 1, :])
        end_t[here, :] = down_sublanes(end_ref[r : r + 1, :])
    c_ref[0:16, :] = jnp.zeros((16, ROWS), bf16)
    lane = lax.broadcasted_iota(i32, (1, 128), 1)

    def chunk(t, carry):
        at = pl.multiple_of(first_ref[t], 16)
        start, end = start_t[pl.ds(at, SPAN), :], end_t[pl.ds(at, SPAN), :]
        halves, columns = [], []
        for h in range(2):
            k = lane + (t * CHUNK + h * 128)
            halves.append(((start <= k) & (k < end)).astype(f32).astype(bf16))
            columns.append(down_sublanes(look_ref[pl.ds(2 * t + h, 1), :]))
        in_bag = jnp.concatenate(halves, axis=1)
        column = jnp.concatenate(columns, axis=0)
        for n in range(0, 16, 4):
            of_row = jnp.concatenate(
                [(column == lane + 128 * q).astype(f32).astype(bf16) for q in range(n, n + 4)],
                axis=1,
            )
            counts = mxu(in_bag, of_row, NN)
            cols = slice(n * 128, (n + 4) * 128)
            before = c_ref[pl.ds(at, 16), cols].astype(f32)
            c_ref[pl.ds(at, 16), cols] = (counts[:16] + before).astype(bf16)
            c_ref[pl.ds(pl.multiple_of(at + 16, 16), SPAN - 16), cols] = counts[16:].astype(bf16)
        return carry

    lax.fori_loop(0, LOOKS // CHUNK, chunk, 0)


def pool_kernel(where_ref, c_ref, table_ref, send_ref, split_ref, partial_ref):
    hi, lo = split(table_ref[...])
    split_ref[:, :128] = hi
    split_ref[:, 128:] = lo

    def block(m, carry):
        at = pl.multiple_of(m * 256, 256)
        both = mxu(c_ref[pl.ds(at, 256), :], split_ref[...], NN)
        partial_ref[pl.ds(at, 256), :] = both[:, :128] + both[:, 128:]
        return carry

    lax.fori_loop(0, BAGS // 256, block, 0)

    def place(n, carry):
        for u in range(16):
            b = n * 16 + u
            send_ref[pl.ds(where_ref[b], 1), :] = partial_ref[pl.ds(b, 1), :]
        return carry

    lax.fori_loop(0, BAGS // 16, place, 0)


def dense_kernel(
    slot_ref, got_ref, dense_ref, label_ref, w_ref, wo_ref, back_ref, grad_ref, pooled, vt, inter_t
):
    def place(c, carry):
        @pl.when(slot_ref[c * CAP] < BAGS)
        def _():
            for u in range(CAP):
                p = c * CAP + u
                pooled[pl.ds(slot_ref[p], 1), :] = got_ref[pl.ds(p, 1), :]

        return carry

    lax.fori_loop(0, DEVICES, place, 0)

    dense_t = dense_ref[...].T
    vt[0] = dense_t
    inter_t[0:128, :] = dense_t
    for f in range(F):
        vt[f + 1] = pooled[f * 128 : (f + 1) * 128, :].T
    for i in range(F):
        for j in range(i + 1, F + 1):
            row = PAIR_ROW[i, j]
            inter_t[row : row + 1, :] = jnp.sum(vt[i] * vt[j], axis=0, keepdims=True)

    it = inter_t[...]
    w = split(w_ref[...])
    pre = dot3(split(it.T), w, NN)
    sig = 1.0 / (1.0 + jnp.exp(-pre))
    hidden = pre * sig
    logits = jnp.sum(hidden * wo_ref[...], axis=1, keepdims=True)
    d_logits = 1.0 / (1.0 + jnp.exp(-logits)) - label_ref[...]
    out_grad = jnp.sum(hidden * d_logits, axis=0, keepdims=True)
    for q in range(8):
        grad_ref[8 * INTER + q : 8 * INTER + q + 1, :] = out_grad[:, q * 128 : (q + 1) * 128]
    grad_ref[8 * INTER + 8 :, :] = jnp.zeros((G_ROWS - 8 * INTER - 8, 128), f32)
    d_pre = split(d_logits * wo_ref[...] * (sig * (1.0 + pre * (1.0 - sig))))
    top_grad = dot3(split(it), d_pre, NN)
    for q in range(8):
        grad_ref[q * INTER : (q + 1) * INTER, :] = top_grad[:, q * 128 : (q + 1) * 128]
    inter_t[...] = dot3(w, d_pre, NT)

    for j in range(1, F + 1):
        total = None
        for i in range(F + 1):
            if i != j:
                row = PAIR_ROW[min(i, j), max(i, j)]
                term = inter_t[row : row + 1, :] * vt[i]
                total = term if total is None else total + term
        pooled[(j - 1) * 128 : j * 128, :] = total.T

    def give(c, carry):
        @pl.when(slot_ref[c * CAP] < BAGS)
        def _():
            for u in range(CAP):
                p = c * CAP + u
                back_ref[pl.ds(p, 1), :] = pooled[pl.ds(slot_ref[p], 1), :]

        return carry

    lax.fori_loop(0, DEVICES, give, 0)


def total_kernel(g_ref, fin_ref, r1, acc, r2, mine, r3, s1, q1, s2, q2, s3, q3, s4, q4, s5, q5):
    gx, x = lax.axis_index("gx"), lax.axis_index("gy")
    yz, core = gx // 2, gx % 2
    twin = (gx + 1 - 2 * core, x)

    def chip(k):
        return (((yz + k) % 16) * 2 + core, x)

    def along(k):
        return (gx, (x + k) % 4)

    barrier = pltpu.get_barrier_semaphore()

    def hello(device):
        pl.semaphore_signal(barrier, inc=1, device_id=device, device_id_type=MESH)

    def greet(k, carry):
        hello(chip(k))
        return carry

    hello(twin)
    lax.fori_loop(1, 16, greet, 0)
    for k in range(1, 4):
        hello(along(k))
    pl.semaphore_wait(barrier, 19)

    def put(src, dst, send, recv, device):
        return pltpu.make_async_remote_copy(
            src_ref=src, dst_ref=dst, send_sem=send, recv_sem=recv, device_id=device, device_id_type=MESH
        )

    my_half = pl.multiple_of(core * HALF, 8)
    other = pl.multiple_of((1 - core) * HALF, 8)
    swap = put(g_ref.at[pl.ds(other, HALF)], r1, s1, q1, twin)
    swap.start()
    swap.wait()
    acc[...] = g_ref[pl.ds(my_half, HALF), :] + r1[...]

    def seg(n):
        return pl.ds(pl.multiple_of(n * SEG, 8), SEG)

    def scatter(k):
        return put(acc.at[seg((yz + k) % 16)], r2.at[k], s2.at[k], q2.at[k], chip(k))

    def start_scatter(k, carry):
        scatter(k).start()
        return carry

    lax.fori_loop(1, 16, start_scatter, 0)
    r2[0] = acc[seg(yz), :]

    def wait_scatter(k, carry):
        scatter(k).wait()
        return carry

    lax.fori_loop(1, 16, wait_scatter, 0)
    part = r2[0]
    for k in range(1, 16):
        part = part + r2[k]
    mine[...] = part
    r3[x] = part
    sends = [put(mine, r3.at[x], s3.at[k], q3.at[k], along(k)) for k in range(1, 4)]
    for copy in sends:
        copy.start()
    for k in range(1, 4):
        put(mine, r3.at[(x + 4 - k) % 4], s3.at[k], q3.at[k], along(k)).wait()
    whole = (r3[0] + r3[1]) + (r3[2] + r3[3])
    place = pl.ds(pl.multiple_of(my_half + yz * SEG, 8), SEG)
    fin_ref[place, :] = whole

    def gather(k, who):
        there = pl.ds(pl.multiple_of(my_half + who * SEG, 8), SEG)
        return put(fin_ref.at[there], fin_ref.at[there], s4.at[k], q4.at[k], chip(k))

    def start_gather(k, carry):
        gather(k, yz).start()
        return carry

    def wait_gather(k, carry):
        gather(k, yz).wait_send()
        gather(k, (yz + 16 - k) % 16).wait_recv()
        return carry

    lax.fori_loop(1, 16, start_gather, 0)
    lax.fori_loop(1, 16, wait_gather, 0)
    half = fin_ref.at[pl.ds(my_half, HALF)]
    last = put(half, half, s5, q5, twin)
    last.start()
    last.wait_send()
    rest = fin_ref.at[pl.ds(other, HALF)]
    put(rest, rest, s5, q5, twin).wait_recv()


def all_total(grads):
    dma = pltpu.SemaphoreType.DMA
    return pl.pallas_call(
        total_kernel,
        out_shape=jax.ShapeDtypeStruct((G_ROWS, 128), f32),
        in_specs=[VMEM],
        out_specs=VMEM,
        scratch_shapes=[
            pltpu.VMEM((HALF, 128), f32),
            pltpu.VMEM((HALF, 128), f32),
            pltpu.VMEM((16, SEG, 128), f32),
            pltpu.VMEM((SEG, 128), f32),
            pltpu.VMEM((4, SEG, 128), f32),
            dma,
            dma,
            dma((16,)),
            dma((16,)),
            dma((4,)),
            dma((4,)),
            dma((16,)),
            dma((16,)),
            dma,
            dma,
        ],
        compiler_params=params(collective_id=0, has_side_effects=True, vmem_limit_bytes=24 << 20),
        cost_estimate=pl.CostEstimate(flops=50_000_000, bytes_accessed=4 << 20, transcendentals=0),
        name="total",
    )(grads)


def update_kernel(
    where_ref,
    c_ref,
    came_ref,
    table_ref,
    state_ref,
    total_ref,
    new_table_ref,
    new_state_ref,
    top_ref,
    out_ref,
    grads,
    sides,
):
    for q in range(8):
        top_ref[:, q * 128 : (q + 1) * 128] = total_ref[q * INTER : (q + 1) * INTER, :]
        out_ref[:, q * 128 : (q + 1) * 128] = total_ref[8 * INTER + q : 8 * INTER + q + 1, :]

    def take(n, carry):
        for u in range(16):
            b = n * 16 + u
            grads[pl.ds(b, 1), :] = came_ref[pl.ds(where_ref[b], 1), :]
        return carry

    lax.fori_loop(0, BAGS // 16, take, 0)
    for q in range(BAGS // 128):
        here = slice(q * 128, (q + 1) * 128)
        hi, lo = split(grads[here, :].T)
        sides[0:128, here] = hi
        sides[128:256, here] = lo

    def block(n, carry):
        here = pl.ds(pl.multiple_of(n * 256, 256), 256)
        both = mxu(sides[...], c_ref[0:BAGS, here], NN)
        row_grad = both[:128] + both[128:]
        state = state_ref[:, here] + jnp.sum(row_grad * row_grad, axis=0, keepdims=True) * (1.0 / E)
        new_state_ref[:, here] = state
        step = row_grad * (learn_rate / (jnp.sqrt(state) + epsilon))
        new_table_ref[here, :] = table_ref[here, :] - step.T
        return carry

    lax.fori_loop(0, ROWS // 256, block, 0)


def params(**kw):
    return pltpu.CompilerParams(**kw)


def from_partner(block, flip):
    return lax.ppermute(block, "gy", [(y, y ^ flip) for y in range(4)])


def trade_blocks(table, state, mask):
    first, second = (mask == 1) | (mask == 2), mask >= 2
    cut = ROWS // 2
    pieces = [table[:cut], jnp.concatenate([table[cut:], state.reshape(16, 128)], axis=0)]
    out = []
    for piece in pieces:
        piece = jnp.where(first, from_partner(piece, 1), piece)
        piece = jnp.where(second, from_partner(piece, 3), piece)
        out.append(piece)
    held = jnp.concatenate([out[0], out[1][:cut]], axis=0)
    return held, out[1][cut:].reshape(1, ROWS)


def swap_all(x):
    return lax.all_to_all(x, ("gx", "gy"), split_axis=0, concat_axis=0, tiled=True)


def on_device(
    emb_table,
    row_state,
    pair_mask,
    look_rows,
    bag_sizes,
    bag_owner,
    bag_slot,
    dense_vectors,
    labels,
    top_weight,
    out_weight,
):
    held, held_state = trade_blocks(emb_table, row_state, pair_mask[0])

    owners = bag_owner[:, 0]
    onehot = (owners[:, None] == jnp.arange(DEVICES, dtype=i32)[None, :]).astype(i32)
    placed_at = jnp.sum((jnp.cumsum(onehot, axis=0) - onehot) * onehot, axis=1)
    where_to = owners * CAP + placed_at
    spot = (placed_at[:, None] == jnp.arange(CAP, dtype=i32)[None, :]).astype(f32)
    sample, feature = bag_slot // F, bag_slot % F
    parts = jnp.concatenate(
        [spot * (sample.astype(f32)[:, None]), spot * ((feature + 1).astype(f32)[:, None])], axis=1
    )
    coded = mxu(onehot.astype(bf16), parts.astype(bf16), ((0,), (0,))).astype(i32)
    sample_at, feature_at = coded[:, :CAP], coded[:, CAP:]
    send_slots = jnp.where(feature_at > 0, (feature_at - 1) * B_DEV + sample_at, BAGS)
    got_slots = swap_all(send_slots).reshape(DEVICES * CAP)

    sizes = bag_sizes[0]
    ends = jnp.cumsum(sizes)
    starts = ends - sizes
    bounds = jnp.arange(LOOKS // CHUNK, dtype=i32) * CHUNK
    first_bag = jnp.sum((ends[None, :] <= bounds[:, None]).astype(i32), axis=1) // 16 * 16
    extra = C_ROWS - BAGS
    ends2 = jnp.concatenate([ends, jnp.zeros((extra,), i32)]).reshape(C_ROWS // 128, 128)
    starts2 = jnp.concatenate([starts, jnp.full((extra,), LOOKS, i32)]).reshape(C_ROWS // 128, 128)
    counts = pl.pallas_call(
        count_kernel,
        out_shape=jax.ShapeDtypeStruct((C_ROWS, ROWS), bf16),
        in_specs=[SMEM, VMEM, VMEM, VMEM],
        out_specs=VMEM,
        scratch_shapes=[pltpu.VMEM((C_ROWS, 128), i32), pltpu.VMEM((C_ROWS, 128), i32)],
        compiler_params=params(vmem_limit_bytes=24 << 20),
        cost_estimate=pl.CostEstimate(flops=2 * LOOKS * SPAN * ROWS, bytes_accessed=10 << 20, transcendentals=0),
        name="count",
    )(first_bag, look_rows.reshape(LOOKS // 128, 128), starts2, ends2)

    send_rows = pl.pallas_call(
        pool_kernel,
        out_shape=jax.ShapeDtypeStruct((DEVICES * CAP, E), f32),
        in_specs=[SMEM, VMEM, VMEM],
        out_specs=VMEM,
        scratch_shapes=[pltpu.VMEM((ROWS, 256), bf16), pltpu.VMEM((BAGS, E), f32)],
        compiler_params=params(vmem_limit_bytes=24 << 20),
        name="pool",
    )(where_to, counts, held)
    got_rows = swap_all(send_rows.reshape(DEVICES, CAP, E)).reshape(DEVICES * CAP, E)

    back_rows, grads = pl.pallas_call(
        dense_kernel,
        out_shape=(
            jax.ShapeDtypeStruct((DEVICES * CAP, E), f32),
            jax.ShapeDtypeStruct((G_ROWS, 128), f32),
        ),
        in_specs=[SMEM, VMEM, VMEM, VMEM, VMEM, VMEM],
        out_specs=(VMEM, VMEM),
        scratch_shapes=[
            pltpu.VMEM((BAGS, E), f32),
            pltpu.VMEM((F + 1, E, B_DEV), f32),
            pltpu.VMEM((INTER, B_DEV), f32),
        ],
        compiler_params=params(vmem_limit_bytes=24 << 20),
        name="dense",
    )(got_slots, got_rows, dense_vectors, labels[:, None], top_weight, out_weight[None, :])

    came_back = swap_all(back_rows.reshape(DEVICES, CAP, E)).reshape(DEVICES * CAP, E)
    total = all_total(grads)

    new_table, new_state, top_grad, out_grad = pl.pallas_call(
        update_kernel,
        out_shape=(
            jax.ShapeDtypeStruct((ROWS, E), f32),
            jax.ShapeDtypeStruct((1, ROWS), f32),
            jax.ShapeDtypeStruct((INTER, HID), f32),
            jax.ShapeDtypeStruct((1, HID), f32),
        ),
        in_specs=[SMEM, VMEM, VMEM, VMEM, VMEM, VMEM],
        out_specs=(VMEM, VMEM, VMEM, VMEM),
        scratch_shapes=[pltpu.VMEM((BAGS, E), f32), pltpu.VMEM((2 * E, BAGS), bf16)],
        compiler_params=params(vmem_limit_bytes=24 << 20),
        name="update",
    )(where_to, counts, came_back, held, held_state, total)
    return new_table, new_state.reshape(ROWS), top_grad, out_grad.reshape(HID)


def solution(mesh):
    both = ("gx", "gy")
    in_specs = (
        P(both, None),
        P(both),
        P("gx"),
        P(both),
        P(both, None),
        P(both, None),
        P(both),
        P(both, None),
        P(both),
        P(),
        P(),
    )
    out_specs = (P(both, None), P(both), P(), P())
    return jax.shard_map(
        on_device, mesh=mesh, in_specs=in_specs, out_specs=out_specs, check_vma=False
    )
```

```python
import jax
import jax.numpy as jnp
from jax import lax
from jax.experimental import pallas as pl
from jax.experimental.pallas import tpu as pltpu
from jax.sharding import PartitionSpec as P

E = 128
F = 16
B_DEV = 128
BAGS = 2048
ROWS = 2048
LOOKS = 6144
DEVICES = 128
CAP = 32
INTER = 264
HID = 1024
CHUNK = 256
SPAN = CHUNK + 16
C_ROWS = 2304
G_ROWS = 2304
HALF = G_ROWS // 2
SEG = HALF // 16
STRIDE = 37
CUT_A, CUT_B = 48, 88
PAIRS = [(i, j) for i in range(F + 1) for j in range(i + 1, F + 1)]
PAIR_ROW = {pair: 128 + n for n, pair in enumerate(PAIRS)}

learn_rate = 0.05
epsilon = 1e-08
MESH = pl.DeviceIdType.MESH
f32, bf16, i32 = jnp.float32, jnp.bfloat16, jnp.int32

VMEM = pl.BlockSpec(memory_space=pltpu.VMEM)
SMEM = pl.BlockSpec(memory_space=pltpu.SMEM)


def split(x):
    hi = x.astype(bf16)
    return hi, (x - hi.astype(f32)).astype(bf16)


def mxu(a, b, dims):
    return lax.dot_general(a, b, (dims, ((), ())), preferred_element_type=f32)


def dot3(a, b, dims):
    return mxu(a[0], b[0], dims) + (mxu(a[0], b[1], dims) + mxu(a[1], b[0], dims))


NN = ((1,), (0,))
NT = ((1,), (1,))


def down_sublanes(row):
    return jnp.broadcast_to(row, (128, 128)).T


def count_kernel(first_ref, look_ref, start_ref, end_ref, c_ref, start_t, end_t):
    for r in range(C_ROWS // 128):
        here = slice(r * 128, (r + 1) * 128)
        start_t[here, :] = down_sublanes(start_ref[r : r + 1, :])
        end_t[here, :] = down_sublanes(end_ref[r : r + 1, :])
    c_ref[0:16, :] = jnp.zeros((16, ROWS), bf16)
    lane = lax.broadcasted_iota(i32, (1, 128), 1)

    def chunk(t, carry):
        at = pl.multiple_of(first_ref[t], 16)
        start, end = start_t[pl.ds(at, SPAN), :], end_t[pl.ds(at, SPAN), :]
        halves, columns = [], []
        for h in range(2):
            k = lane + (t * CHUNK + h * 128)
            halves.append(((start <= k) & (k < end)).astype(f32).astype(bf16))
            columns.append(down_sublanes(look_ref[pl.ds(2 * t + h, 1), :]))
        in_bag = jnp.concatenate(halves, axis=1)
        column = jnp.concatenate(columns, axis=0)
        for n in range(0, 16, 4):
            of_row = jnp.concatenate(
                [(column == lane + 128 * q).astype(f32).astype(bf16) for q in range(n, n + 4)],
                axis=1,
            )
            counts = mxu(in_bag, of_row, NN)
            cols = slice(n * 128, (n + 4) * 128)
            before = c_ref[pl.ds(at, 16), cols].astype(f32)
            c_ref[pl.ds(at, 16), cols] = (counts[:16] + before).astype(bf16)
            c_ref[pl.ds(pl.multiple_of(at + 16, 16), SPAN - 16), cols] = counts[16:].astype(bf16)
        return carry

    lax.fori_loop(0, LOOKS // CHUNK, chunk, 0)


def device_at(n):
    return (n // 4, n % 4)


def my_number():
    return lax.axis_index("gx") * 4 + lax.axis_index("gy")


def peer_of(k):
    return (my_number() + STRIDE * k) % DEVICES


def greet_all(barrier):
    def greet(k, carry):
        pl.semaphore_signal(barrier, inc=1, device_id=device_at(peer_of(k)), device_id_type=MESH)
        return carry

    lax.fori_loop(1, DEVICES, greet, 0)


def put(src, dst, send, recv, device):
    return pltpu.make_async_remote_copy(
        src_ref=src, dst_ref=dst, send_sem=send, recv_sem=recv, device_id=device, device_id_type=MESH
    )


def chunk_at(n):
    return pl.ds(pl.multiple_of(n * CAP, CAP), CAP)


def pick_rows(dst, to, src, index_ref, at):
    for u in range(CAP):
        dst[pl.ds(to + u, 1), :] = src[pl.ds(index_ref[at + u], 1), :]


def pool_kernel(
    bag_ref,
    slots_ref,
    c_ref,
    table_ref,
    recv_ref,
    got_ref,
    split_ref,
    partial_ref,
    send_ref,
    row_send,
    row_recv,
    slot_send,
    slot_recv,
):
    barrier = pltpu.get_barrier_semaphore()
    greet_all(barrier)
    me = my_number()
    hi, lo = split(table_ref[...])
    split_ref[:, :128] = hi
    split_ref[:, 128:] = lo

    def block(m, carry):
        at = pl.multiple_of(m * 256, 256)
        both = mxu(c_ref[pl.ds(at, 256), :], split_ref[...], NN)
        partial_ref[pl.ds(at, 256), :] = both[:, :128] + both[:, 128:]
        return carry

    lax.fori_loop(0, BAGS // 256, block, 0)
    got_ref[me] = slots_ref[me]
    pick_rows(recv_ref, me * CAP, partial_ref, bag_ref, me * CAP)

    def ready(k):
        at = peer_of(k) * CAP
        pick_rows(send_ref, at, partial_ref, bag_ref, at)

    def start(k):
        peer = peer_of(k)
        to = device_at(peer)
        put(slots_ref.at[peer], got_ref.at[me], slot_send, slot_recv, to).start()
        put(send_ref.at[chunk_at(peer)], recv_ref.at[chunk_at(me)], row_send, row_recv, to).start()

    ready(1)
    pl.semaphore_wait(barrier, DEVICES - 1)

    def step(k, carry):
        ready(k)
        start(k - 1)
        return carry

    lax.fori_loop(2, DEVICES, step, 0)
    start(DEVICES - 1)
    to = device_at(peer_of(1))
    some = pl.ds(0, DEVICES - 1)
    put(slots_ref.at[some], got_ref.at[some], slot_send, slot_recv, to).wait()
    rows = pl.ds(0, (DEVICES - 1) * CAP)
    put(send_ref.at[rows], recv_ref.at[rows], row_send, row_recv, to).wait()


def dense_kernel(
    slot_ref, got_ref, dense_ref, label_ref, w_ref, wo_ref, pooled, grad_ref, vt, inter_t
):
    pooled[BAGS:, :] = jnp.zeros((8, E), f32)

    def place(c, carry):
        @pl.when(slot_ref[c * 128] < BAGS)
        def _():
            for u in range(CAP):
                pooled[pl.ds(slot_ref[c * 128 + u], 1), :] = got_ref[pl.ds(c * CAP + u, 1), :]

        return carry

    lax.fori_loop(0, DEVICES, place, 0)

    dense_t = dense_ref[...].T
    vt[0] = dense_t
    inter_t[0:128, :] = dense_t
    for f in range(F):
        vt[f + 1] = pooled[f * 128 : (f + 1) * 128, :].T
    for i in range(F):
        for j in range(i + 1, F + 1):
            row = PAIR_ROW[i, j]
            inter_t[row : row + 1, :] = jnp.sum(vt[i] * vt[j], axis=0, keepdims=True)

    it = inter_t[...]
    w = split(w_ref[...])
    pre = dot3(split(it.T), w, NN)
    sig = 1.0 / (1.0 + jnp.exp(-pre))
    hidden = pre * sig
    logits = jnp.sum(hidden * wo_ref[...], axis=1, keepdims=True)
    d_logits = 1.0 / (1.0 + jnp.exp(-logits)) - label_ref[...]
    out_grad = jnp.sum(hidden * d_logits, axis=0, keepdims=True)
    for q in range(8):
        grad_ref[8 * INTER + q : 8 * INTER + q + 1, :] = out_grad[:, q * 128 : (q + 1) * 128]
    grad_ref[8 * INTER + 8 :, :] = jnp.zeros((G_ROWS - 8 * INTER - 8, 128), f32)
    d_pre = split(d_logits * wo_ref[...] * (sig * (1.0 + pre * (1.0 - sig))))
    top_grad = dot3(split(it), d_pre, NN)
    for q in range(8):
        grad_ref[q * INTER : (q + 1) * INTER, :] = top_grad[:, q * 128 : (q + 1) * 128]
    inter_t[...] = dot3(w, d_pre, NT)

    for j in range(1, F + 1):
        total = None
        for i in range(F + 1):
            if i != j:
                row = PAIR_ROW[min(i, j), max(i, j)]
                term = inter_t[row : row + 1, :] * vt[i]
                total = term if total is None else total + term
        pooled[(j - 1) * 128 : j * 128, :] = total.T


def update_kernel(
    slot_ref,
    where_ref,
    pooled_ref,
    g_ref,
    c_ref,
    table_ref,
    state_ref,
    new_table_ref,
    new_state_ref,
    top_ref,
    out_ref,
    back,
    came,
    grads,
    sides,
    fin,
    r1,
    acc,
    r2,
    mine,
    r3,
    row_send,
    row_recv,
    s1,
    q1,
    s2,
    q2,
    s3,
    q3,
    s4,
    q4,
    s5,
    q5,
):
    barrier = pltpu.get_barrier_semaphore()
    greet_all(barrier)
    me = my_number()
    gx, x = lax.axis_index("gx"), lax.axis_index("gy")
    yz, core = gx // 2, gx % 2
    twin = (gx + 1 - 2 * core, x)

    def chip(k):
        return (((yz + k) % 16) * 2 + core, x)

    def along(k):
        return (gx, (x + k) % 4)

    pick_rows(came, me * CAP, pooled_ref, slot_ref, me * 128)

    def ready(k, carry):
        peer = peer_of(k)
        pick_rows(back, peer * CAP, pooled_ref, slot_ref, peer * 128)
        return carry

    lax.fori_loop(1, DEVICES, ready, 0)

    def start(k, carry):
        peer = peer_of(k)
        put(
            back.at[chunk_at(peer)], came.at[chunk_at(me)], row_send, row_recv, device_at(peer)
        ).start()
        return carry

    pl.semaphore_wait(barrier, DEVICES - 1)

    my_half = pl.multiple_of(core * HALF, 8)
    other = pl.multiple_of((1 - core) * HALF, 8)
    swap = put(g_ref.at[pl.ds(other, HALF)], r1, s1, q1, twin)
    swap.start()
    lax.fori_loop(1, CUT_A, start, 0)
    swap.wait()
    acc[...] = g_ref[pl.ds(my_half, HALF), :] + r1[...]

    def seg(n):
        return pl.ds(pl.multiple_of(n * SEG, 8), SEG)

    def scatter(k):
        return put(acc.at[seg((yz + k) % 16)], r2.at[k], s2.at[k], q2.at[k], chip(k))

    def start_scatter(k, carry):
        scatter(k).start()
        return carry

    lax.fori_loop(1, 16, start_scatter, 0)
    lax.fori_loop(CUT_A, CUT_B, start, 0)
    r2[0] = acc[seg(yz), :]

    def wait_scatter(k, carry):
        scatter(k).wait()
        return carry

    lax.fori_loop(1, 16, wait_scatter, 0)
    part = r2[0]
    for k in range(1, 16):
        part = part + r2[k]
    mine[...] = part
    r3[x] = part
    for k in range(1, 4):
        put(mine, r3.at[x], s3.at[k], q3.at[k], along(k)).start()
    lax.fori_loop(CUT_B, DEVICES, start, 0)
    for k in range(1, 4):
        put(mine, r3.at[(x + 4 - k) % 4], s3.at[k], q3.at[k], along(k)).wait()
    whole = (r3[0] + r3[1]) + (r3[2] + r3[3])
    place = pl.ds(pl.multiple_of(my_half + yz * SEG, 8), SEG)
    fin[place, :] = whole

    def gather(k, who):
        there = pl.ds(pl.multiple_of(my_half + who * SEG, 8), SEG)
        return put(fin.at[there], fin.at[there], s4.at[k], q4.at[k], chip(k))

    def start_gather(k, carry):
        gather(k, yz).start()
        return carry

    lax.fori_loop(1, 16, start_gather, 0)

    rows = pl.ds(0, (DEVICES - 1) * CAP)
    put(back.at[rows], came.at[rows], row_send, row_recv, device_at(peer_of(1))).wait()

    def take(n, carry):
        for u in range(16):
            b = n * 16 + u
            grads[pl.ds(b, 1), :] = came[pl.ds(where_ref[b], 1), :]
        return carry

    lax.fori_loop(0, BAGS // 16, take, 0)
    for q in range(BAGS // 128):
        here = slice(q * 128, (q + 1) * 128)
        hi, lo = split(grads[here, :].T)
        sides[0:128, here] = hi
        sides[128:256, here] = lo

    def block(n, carry):
        here = pl.ds(pl.multiple_of(n * 256, 256), 256)
        both = mxu(sides[...], c_ref[0:BAGS, here], NN)
        row_grad = both[:128] + both[128:]
        state = state_ref[:, here] + jnp.sum(row_grad * row_grad, axis=0, keepdims=True) * (1.0 / E)
        new_state_ref[:, here] = state
        step = row_grad * (learn_rate / (jnp.sqrt(state) + epsilon))
        new_table_ref[here, :] = table_ref[here, :] - step.T
        return carry

    lax.fori_loop(0, ROWS // 256, block, 0)

    def wait_gather(k, carry):
        gather(k, yz).wait_send()
        gather(k, (yz + 16 - k) % 16).wait_recv()
        return carry

    lax.fori_loop(1, 16, wait_gather, 0)
    half = fin.at[pl.ds(my_half, HALF)]
    rest = fin.at[pl.ds(other, HALF)]
    last = put(half, half, s5, q5, twin)
    last.start()
    last.wait_send()
    put(rest, rest, s5, q5, twin).wait_recv()
    for q in range(8):
        top_ref[:, q * 128 : (q + 1) * 128] = fin[q * INTER : (q + 1) * INTER, :]
        out_ref[:, q * 128 : (q + 1) * 128] = fin[8 * INTER + q : 8 * INTER + q + 1, :]


def params(**kw):
    return pltpu.CompilerParams(**kw)


def from_partner(block, flip):
    return lax.ppermute(block, "gy", [(y, y ^ flip) for y in range(4)])


def trade_blocks(table, state, mask):
    first, second = (mask == 1) | (mask == 2), mask >= 2
    cut = ROWS // 2
    pieces = [table[:cut], jnp.concatenate([table[cut:], state.reshape(16, 128)], axis=0)]
    out = []
    for piece in pieces:
        piece = jnp.where(first, from_partner(piece, 1), piece)
        piece = jnp.where(second, from_partner(piece, 3), piece)
        out.append(piece)
    held = jnp.concatenate([out[0], out[1][:cut]], axis=0)
    return held, out[1][cut:].reshape(1, ROWS)


def on_device(
    emb_table,
    row_state,
    pair_mask,
    look_rows,
    bag_sizes,
    bag_owner,
    bag_slot,
    dense_vectors,
    labels,
    top_weight,
    out_weight,
):
    held, held_state = trade_blocks(emb_table, row_state, pair_mask[0])

    owners = bag_owner[:, 0]
    onehot = (owners[:, None] == jnp.arange(DEVICES, dtype=i32)[None, :]).astype(i32)
    placed_at = jnp.sum((jnp.cumsum(onehot, axis=0) - onehot) * onehot, axis=1)
    where_to = owners * CAP + placed_at
    spot = (placed_at[:, None] == jnp.arange(CAP, dtype=i32)[None, :]).astype(f32)
    sample, feature = bag_slot // F, bag_slot % F
    bag = jnp.arange(BAGS, dtype=i32)
    pieces = [sample, feature + 1, bag // 16, bag % 16]
    parts = jnp.concatenate([spot * piece.astype(f32)[:, None] for piece in pieces], axis=1)
    coded = mxu(onehot.astype(bf16), parts.astype(bf16), ((0,), (0,))).astype(i32)
    sample_at, feature_at = coded[:, :CAP], coded[:, CAP : 2 * CAP]
    send_slots = jnp.where(feature_at > 0, (feature_at - 1) * B_DEV + sample_at, BAGS)
    send_slots = jnp.pad(send_slots, ((0, 0), (0, 128 - CAP))).reshape(DEVICES, 1, 128)
    send_bags = (coded[:, 2 * CAP : 3 * CAP] * 16 + coded[:, 3 * CAP :]).reshape(DEVICES * CAP)

    sizes = bag_sizes[0]
    ends = jnp.cumsum(sizes)
    starts = ends - sizes
    bounds = jnp.arange(LOOKS // CHUNK, dtype=i32) * CHUNK
    first_bag = jnp.sum((ends[None, :] <= bounds[:, None]).astype(i32), axis=1) // 16 * 16
    extra = C_ROWS - BAGS
    ends2 = jnp.concatenate([ends, jnp.zeros((extra,), i32)]).reshape(C_ROWS // 128, 128)
    starts2 = jnp.concatenate([starts, jnp.full((extra,), LOOKS, i32)]).reshape(C_ROWS // 128, 128)
    counts = pl.pallas_call(
        count_kernel,
        out_shape=jax.ShapeDtypeStruct((C_ROWS, ROWS), bf16),
        in_specs=[SMEM, VMEM, VMEM, VMEM],
        out_specs=VMEM,
        scratch_shapes=[pltpu.VMEM((C_ROWS, 128), i32), pltpu.VMEM((C_ROWS, 128), i32)],
        compiler_params=params(vmem_limit_bytes=24 << 20),
        cost_estimate=pl.CostEstimate(flops=2 * LOOKS * SPAN * ROWS, bytes_accessed=10 << 20, transcendentals=0),
        name="count",
    )(first_bag, look_rows.reshape(LOOKS // 128, 128), starts2, ends2)

    dma = pltpu.SemaphoreType.DMA
    got_rows, got_slots = pl.pallas_call(
        pool_kernel,
        out_shape=(
            jax.ShapeDtypeStruct((DEVICES * CAP, E), f32),
            jax.ShapeDtypeStruct((DEVICES, 1, 128), i32),
        ),
        in_specs=[SMEM, VMEM, VMEM, VMEM],
        out_specs=(VMEM, VMEM),
        scratch_shapes=[
            pltpu.VMEM((ROWS, 256), bf16),
            pltpu.VMEM((BAGS, E), f32),
            pltpu.VMEM((DEVICES * CAP, E), f32),
            dma,
            dma,
            dma,
            dma,
        ],
        compiler_params=params(collective_id=0, has_side_effects=True, vmem_limit_bytes=20 << 20),
        name="pool",
    )(send_bags, send_slots, counts, held)
    slot_of = got_slots.reshape(DEVICES * 128)

    pooled_grads, grads = pl.pallas_call(
        dense_kernel,
        out_shape=(
            jax.ShapeDtypeStruct((BAGS + 8, E), f32),
            jax.ShapeDtypeStruct((G_ROWS, 128), f32),
        ),
        in_specs=[SMEM, VMEM, VMEM, VMEM, VMEM, VMEM],
        out_specs=(VMEM, VMEM),
        scratch_shapes=[
            pltpu.VMEM((F + 1, E, B_DEV), f32),
            pltpu.VMEM((INTER, B_DEV), f32),
        ],
        compiler_params=params(vmem_limit_bytes=20 << 20),
        name="dense",
    )(slot_of, got_rows, dense_vectors, labels[:, None], top_weight, out_weight[None, :])

    new_table, new_state, top_grad, out_grad = pl.pallas_call(
        update_kernel,
        out_shape=(
            jax.ShapeDtypeStruct((ROWS, E), f32),
            jax.ShapeDtypeStruct((1, ROWS), f32),
            jax.ShapeDtypeStruct((INTER, HID), f32),
            jax.ShapeDtypeStruct((1, HID), f32),
        ),
        in_specs=[SMEM, SMEM, VMEM, VMEM, VMEM, VMEM, VMEM],
        out_specs=(VMEM, VMEM, VMEM, VMEM),
        scratch_shapes=[
            pltpu.VMEM((DEVICES * CAP, E), f32),
            pltpu.VMEM((DEVICES * CAP, E), f32),
            pltpu.VMEM((BAGS, E), f32),
            pltpu.VMEM((2 * E, BAGS), bf16),
            pltpu.VMEM((G_ROWS, 128), f32),
            pltpu.VMEM((HALF, 128), f32),
            pltpu.VMEM((HALF, 128), f32),
            pltpu.VMEM((16, SEG, 128), f32),
            pltpu.VMEM((SEG, 128), f32),
            pltpu.VMEM((4, SEG, 128), f32),
            dma,
            dma,
            dma,
            dma,
            dma((16,)),
            dma((16,)),
            dma((4,)),
            dma((4,)),
            dma((16,)),
            dma((16,)),
            dma,
            dma,
        ],
        compiler_params=params(collective_id=1, has_side_effects=True, vmem_limit_bytes=24 << 20),
        name="update",
    )(slot_of, where_to, pooled_grads, grads, counts, held, held_state)
    return new_table, new_state.reshape(ROWS), top_grad, out_grad.reshape(HID)


def solution(mesh):
    both = ("gx", "gy")
    in_specs = (
        P(both, None),
        P(both),
        P("gx"),
        P(both),
        P(both, None),
        P(both, None),
        P(both),
        P(both, None),
        P(both),
        P(),
        P(),
    )
    out_specs = (P(both, None), P(both), P(), P())
    return jax.shard_map(
        on_device, mesh=mesh, in_specs=in_specs, out_specs=out_specs, check_vma=False
    )
```

```python
import jax
import jax.numpy as jnp
from jax import lax
from jax.experimental import pallas as pl
from jax.experimental.pallas import tpu as pltpu
from jax.sharding import PartitionSpec as P

E = 128
F = 16
B_DEV = 128
BAGS = 2048
ROWS = 2048
LOOKS = 6144
DEVICES = 128
CAP = 32
INTER = 264
HID = 1024
CHUNK = 256
SPAN = CHUNK + 16
C_ROWS = 2304
G_ROWS = 2304
HALF = G_ROWS // 2
SEG = HALF // 16
STRIDE = 37
CUT_A, CUT_B = 48, 88
PAIRS = [(i, j) for i in range(F + 1) for j in range(i + 1, F + 1)]
PAIR_ROW = {pair: 128 + n for n, pair in enumerate(PAIRS)}

learn_rate = 0.05
epsilon = 1e-08
MESH = pl.DeviceIdType.MESH
f32, bf16, i32 = jnp.float32, jnp.bfloat16, jnp.int32

VMEM = pl.BlockSpec(memory_space=pltpu.VMEM)
SMEM = pl.BlockSpec(memory_space=pltpu.SMEM)


def split(x):
    hi = x.astype(bf16)
    return hi, (x - hi.astype(f32)).astype(bf16)


def mxu(a, b, dims):
    return lax.dot_general(a, b, (dims, ((), ())), preferred_element_type=f32)


def dot3(a, b, dims):
    return mxu(a[0], b[0], dims) + (mxu(a[0], b[1], dims) + mxu(a[1], b[0], dims))


NN = ((1,), (0,))
NT = ((1,), (1,))


def down_sublanes(row):
    return jnp.broadcast_to(row, (128, 128)).T


def count_kernel(first_ref, look_ref, start_ref, end_ref, c_ref, start_t, end_t):
    for r in range(C_ROWS // 128):
        here = slice(r * 128, (r + 1) * 128)
        start_t[here, :] = down_sublanes(start_ref[r : r + 1, :])
        end_t[here, :] = down_sublanes(end_ref[r : r + 1, :])
    c_ref[0:16, :] = jnp.zeros((16, ROWS), bf16)
    lane = lax.broadcasted_iota(i32, (1, 128), 1)

    def chunk(t, carry):
        at = pl.multiple_of(first_ref[t], 16)
        start, end = start_t[pl.ds(at, SPAN), :], end_t[pl.ds(at, SPAN), :]
        halves, columns = [], []
        for h in range(2):
            k = lane + (t * CHUNK + h * 128)
            halves.append(((start <= k) & (k < end)).astype(f32).astype(bf16))
            columns.append(down_sublanes(look_ref[pl.ds(2 * t + h, 1), :]))
        in_bag = jnp.concatenate(halves, axis=1)
        column = jnp.concatenate(columns, axis=0)
        for n in range(0, 16, 4):
            of_row = jnp.concatenate(
                [(column == lane + 128 * q).astype(f32).astype(bf16) for q in range(n, n + 4)],
                axis=1,
            )
            counts = mxu(in_bag, of_row, NN)
            cols = slice(n * 128, (n + 4) * 128)
            before = c_ref[pl.ds(at, 16), cols].astype(f32)
            c_ref[pl.ds(at, 16), cols] = (counts[:16] + before).astype(bf16)
            c_ref[pl.ds(pl.multiple_of(at + 16, 16), SPAN - 16), cols] = counts[16:].astype(bf16)
        return carry

    lax.fori_loop(0, LOOKS // CHUNK, chunk, 0)


def device_at(n):
    return (n // 4, n % 4)


def my_number():
    return lax.axis_index("gx") * 4 + lax.axis_index("gy")


def peer_of(k):
    return (my_number() + STRIDE * k) % DEVICES


def greet_all(barrier):
    def greet(k, carry):
        pl.semaphore_signal(barrier, inc=1, device_id=device_at(peer_of(k)), device_id_type=MESH)
        return carry

    lax.fori_loop(1, DEVICES, greet, 0)


def put(src, dst, send, recv, device):
    return pltpu.make_async_remote_copy(
        src_ref=src, dst_ref=dst, send_sem=send, recv_sem=recv, device_id=device, device_id_type=MESH
    )


def chunk_at(n):
    return pl.ds(pl.multiple_of(n * CAP, CAP), CAP)


def pick_rows(dst, to, src, index_ref, at):
    for u in range(CAP):
        dst[pl.ds(to + u, 1), :] = src[pl.ds(index_ref[at + u], 1), :]


def pool_kernel(
    mask_ref,
    bag_ref,
    slots_ref,
    c_ref,
    a_ref,
    a2_ref,
    b_ref,
    b2_ref,
    recv_ref,
    got_ref,
    held_ref,
    split_ref,
    partial_ref,
    send_ref,
    row_send,
    row_recv,
    slot_send,
    slot_recv,
):
    barrier = pltpu.get_barrier_semaphore()
    greet_all(barrier)
    me = my_number()
    mask = jnp.full((ROWS // 2, E), mask_ref[0], i32)
    held_ref[: ROWS // 2, :] = jnp.where(mask >= 2, a2_ref[...], a_ref[...])
    held_ref[ROWS // 2 :, :] = jnp.where((mask == 1) | (mask == 2), b2_ref[...], b_ref[...])
    hi, lo = split(held_ref[...])
    split_ref[:, :128] = hi
    split_ref[:, 128:] = lo

    def block(m, carry):
        at = pl.multiple_of(m * 256, 256)
        both = mxu(c_ref[pl.ds(at, 256), :], split_ref[...], NN)
        partial_ref[pl.ds(at, 256), :] = both[:, :128] + both[:, 128:]
        return carry

    lax.fori_loop(0, BAGS // 256, block, 0)
    got_ref[me] = slots_ref[me]
    pick_rows(recv_ref, me * CAP, partial_ref, bag_ref, me * CAP)

    def ready(k):
        at = peer_of(k) * CAP
        pick_rows(send_ref, at, partial_ref, bag_ref, at)

    def start(k):
        peer = peer_of(k)
        to = device_at(peer)
        put(slots_ref.at[peer], got_ref.at[me], slot_send, slot_recv, to).start()
        put(send_ref.at[chunk_at(peer)], recv_ref.at[chunk_at(me)], row_send, row_recv, to).start()

    ready(1)
    pl.semaphore_wait(barrier, DEVICES - 1)

    def step(k, carry):
        ready(k)
        start(k - 1)
        return carry

    lax.fori_loop(2, DEVICES, step, 0)
    start(DEVICES - 1)
    to = device_at(peer_of(1))
    some = pl.ds(0, DEVICES - 1)
    put(slots_ref.at[some], got_ref.at[some], slot_send, slot_recv, to).wait()
    rows = pl.ds(0, (DEVICES - 1) * CAP)
    put(send_ref.at[rows], recv_ref.at[rows], row_send, row_recv, to).wait()


def dense_kernel(
    slot_ref, got_ref, dense_ref, label_ref, w_ref, wo_ref, pooled, grad_ref, vt, inter_t
):
    pooled[BAGS:, :] = jnp.zeros((8, E), f32)

    def place(c, carry):
        @pl.when(slot_ref[c * 128] < BAGS)
        def _():
            for u in range(CAP):
                pooled[pl.ds(slot_ref[c * 128 + u], 1), :] = got_ref[pl.ds(c * CAP + u, 1), :]

        return carry

    lax.fori_loop(0, DEVICES, place, 0)

    dense_t = dense_ref[...].T
    vt[0] = dense_t
    inter_t[0:128, :] = dense_t
    for f in range(F):
        vt[f + 1] = pooled[f * 128 : (f + 1) * 128, :].T
    for i in range(F):
        for j in range(i + 1, F + 1):
            row = PAIR_ROW[i, j]
            inter_t[row : row + 1, :] = jnp.sum(vt[i] * vt[j], axis=0, keepdims=True)

    it = inter_t[...]
    w = split(w_ref[...])
    pre = dot3(split(it.T), w, NN)
    sig = 1.0 / (1.0 + jnp.exp(-pre))
    hidden = pre * sig
    logits = jnp.sum(hidden * wo_ref[...], axis=1, keepdims=True)
    d_logits = 1.0 / (1.0 + jnp.exp(-logits)) - label_ref[...]
    out_grad = jnp.sum(hidden * d_logits, axis=0, keepdims=True)
    for q in range(8):
        grad_ref[8 * INTER + q : 8 * INTER + q + 1, :] = out_grad[:, q * 128 : (q + 1) * 128]
    grad_ref[8 * INTER + 8 :, :] = jnp.zeros((G_ROWS - 8 * INTER - 8, 128), f32)
    d_pre = split(d_logits * wo_ref[...] * (sig * (1.0 + pre * (1.0 - sig))))
    top_grad = dot3(split(it), d_pre, NN)
    for q in range(8):
        grad_ref[q * INTER : (q + 1) * INTER, :] = top_grad[:, q * 128 : (q + 1) * 128]
    inter_t[...] = dot3(w, d_pre, NT)

    for j in range(1, F + 1):
        total = None
        for i in range(F + 1):
            if i != j:
                row = PAIR_ROW[min(i, j), max(i, j)]
                term = inter_t[row : row + 1, :] * vt[i]
                total = term if total is None else total + term
        pooled[(j - 1) * 128 : j * 128, :] = total.T


def update_kernel(
    mask_ref,
    slot_ref,
    where_ref,
    pooled_ref,
    g_ref,
    c_ref,
    table_ref,
    state_ref,
    new_table_ref,
    new_state_ref,
    top_ref,
    out_ref,
    back,
    came,
    grads,
    sides,
    fin,
    r1,
    acc,
    r2,
    mine,
    r3,
    states,
    state_send,
    state_recv,
    row_send,
    row_recv,
    s1,
    q1,
    s2,
    q2,
    s3,
    q3,
    s4,
    q4,
    s5,
    q5,
):
    barrier = pltpu.get_barrier_semaphore()
    greet_all(barrier)
    me = my_number()
    gx, x = lax.axis_index("gx"), lax.axis_index("gy")
    yz, core = gx // 2, gx % 2
    twin = (gx + 1 - 2 * core, x)

    def chip(k):
        return (((yz + k) % 16) * 2 + core, x)

    def along(k):
        return (gx, (x + k) % 4)

    pick_rows(came, me * CAP, pooled_ref, slot_ref, me * 128)

    def ready(k, carry):
        peer = peer_of(k)
        pick_rows(back, peer * CAP, pooled_ref, slot_ref, peer * 128)
        return carry

    lax.fori_loop(1, DEVICES, ready, 0)

    def start(k, carry):
        peer = peer_of(k)
        put(
            back.at[chunk_at(peer)], came.at[chunk_at(me)], row_send, row_recv, device_at(peer)
        ).start()
        return carry

    pl.semaphore_wait(barrier, DEVICES - 1)

    my_half = pl.multiple_of(core * HALF, 8)
    other = pl.multiple_of((1 - core) * HALF, 8)
    swap = put(g_ref.at[pl.ds(other, HALF)], r1, s1, q1, twin)
    swap.start()
    flips = [None, x + 1 - 2 * (x % 2), (x + 2) % 4, 3 - x]
    state_moves = [
        put(state_ref, states.at[f], state_send.at[f], state_recv.at[f], (gx, flips[f]))
        for f in range(1, 4)
    ]
    for move in state_moves:
        move.start()
    lax.fori_loop(1, CUT_A, start, 0)
    swap.wait()
    acc[...] = g_ref[pl.ds(my_half, HALF), :] + r1[...]

    def seg(n):
        return pl.ds(pl.multiple_of(n * SEG, 8), SEG)

    def scatter(k):
        return put(acc.at[seg((yz + k) % 16)], r2.at[k], s2.at[k], q2.at[k], chip(k))

    def start_scatter(k, carry):
        scatter(k).start()
        return carry

    lax.fori_loop(1, 16, start_scatter, 0)
    lax.fori_loop(CUT_A, CUT_B, start, 0)
    r2[0] = acc[seg(yz), :]

    def wait_scatter(k, carry):
        scatter(k).wait()
        return carry

    lax.fori_loop(1, 16, wait_scatter, 0)
    part = r2[0]
    for k in range(1, 16):
        part = part + r2[k]
    mine[...] = part
    r3[x] = part
    for k in range(1, 4):
        put(mine, r3.at[x], s3.at[k], q3.at[k], along(k)).start()
    lax.fori_loop(CUT_B, DEVICES, start, 0)
    for k in range(1, 4):
        put(mine, r3.at[(x + 4 - k) % 4], s3.at[k], q3.at[k], along(k)).wait()
    whole = (r3[0] + r3[1]) + (r3[2] + r3[3])
    place = pl.ds(pl.multiple_of(my_half + yz * SEG, 8), SEG)
    fin[place, :] = whole

    def gather(k, who):
        there = pl.ds(pl.multiple_of(my_half + who * SEG, 8), SEG)
        return put(fin.at[there], fin.at[there], s4.at[k], q4.at[k], chip(k))

    def start_gather(k, carry):
        gather(k, yz).start()
        return carry

    lax.fori_loop(1, 16, start_gather, 0)

    rows = pl.ds(0, (DEVICES - 1) * CAP)
    put(back.at[rows], came.at[rows], row_send, row_recv, device_at(peer_of(1))).wait()

    for move in state_moves:
        move.wait()
    mask = jnp.full((1, ROWS), mask_ref[0], i32)
    held_state = state_ref[...]
    for f in range(1, 4):
        held_state = jnp.where(mask == f, states[f], held_state)
    states[0] = held_state

    def take(n, carry):
        for u in range(16):
            b = n * 16 + u
            grads[pl.ds(b, 1), :] = came[pl.ds(where_ref[b], 1), :]
        return carry

    lax.fori_loop(0, BAGS // 16, take, 0)
    for q in range(BAGS // 128):
        here = slice(q * 128, (q + 1) * 128)
        hi, lo = split(grads[here, :].T)
        sides[0:128, here] = hi
        sides[128:256, here] = lo

    def block(n, carry):
        here = pl.ds(pl.multiple_of(n * 256, 256), 256)
        both = mxu(sides[...], c_ref[0:BAGS, here], NN)
        row_grad = both[:128] + both[128:]
        state = states[0, :, here] + jnp.sum(row_grad * row_grad, axis=0, keepdims=True) * (1.0 / E)
        new_state_ref[:, here] = state
        step = row_grad * (learn_rate / (jnp.sqrt(state) + epsilon))
        new_table_ref[here, :] = table_ref[here, :] - step.T
        return carry

    lax.fori_loop(0, ROWS // 256, block, 0)

    def wait_gather(k, carry):
        gather(k, yz).wait_send()
        gather(k, (yz + 16 - k) % 16).wait_recv()
        return carry

    lax.fori_loop(1, 16, wait_gather, 0)
    half = fin.at[pl.ds(my_half, HALF)]
    rest = fin.at[pl.ds(other, HALF)]
    last = put(half, half, s5, q5, twin)
    last.start()
    last.wait_send()
    put(rest, rest, s5, q5, twin).wait_recv()
    for q in range(8):
        top_ref[:, q * 128 : (q + 1) * 128] = fin[q * INTER : (q + 1) * INTER, :]
        out_ref[:, q * 128 : (q + 1) * 128] = fin[8 * INTER + q : 8 * INTER + q + 1, :]


def params(**kw):
    return pltpu.CompilerParams(**kw)


def from_partner(block, flip):
    return lax.ppermute(block, "gy", [(y, y ^ flip) for y in range(4)])


def on_device(
    emb_table,
    row_state,
    pair_mask,
    look_rows,
    bag_sizes,
    bag_owner,
    bag_slot,
    dense_vectors,
    labels,
    top_weight,
    out_weight,
):
    mask = pair_mask[0]
    first, second = (mask == 1) | (mask == 2), mask >= 2
    upper, lower = emb_table[: ROWS // 2], emb_table[ROWS // 2 :]
    upper = jnp.where(first, from_partner(upper, 1), upper)
    lower = jnp.where(second, from_partner(lower, 3), lower)

    owners = bag_owner[:, 0]
    onehot = (owners[:, None] == jnp.arange(DEVICES, dtype=i32)[None, :]).astype(i32)
    placed_at = jnp.sum((jnp.cumsum(onehot, axis=0) - onehot) * onehot, axis=1)
    where_to = owners * CAP + placed_at
    spot = (placed_at[:, None] == jnp.arange(CAP, dtype=i32)[None, :]).astype(f32)
    sample, feature = bag_slot // F, bag_slot % F
    bag = jnp.arange(BAGS, dtype=i32)
    pieces = [sample, feature + 1, bag // 16, bag % 16]
    parts = jnp.concatenate([spot * piece.astype(f32)[:, None] for piece in pieces], axis=1)
    coded = mxu(onehot.astype(bf16), parts.astype(bf16), ((0,), (0,))).astype(i32)
    sample_at, feature_at = coded[:, :CAP], coded[:, CAP : 2 * CAP]
    send_slots = jnp.where(feature_at > 0, (feature_at - 1) * B_DEV + sample_at, BAGS)
    send_slots = jnp.pad(send_slots, ((0, 0), (0, 128 - CAP))).reshape(DEVICES, 1, 128)
    send_bags = (coded[:, 2 * CAP : 3 * CAP] * 16 + coded[:, 3 * CAP :]).reshape(DEVICES * CAP)

    sizes = bag_sizes[0]
    ends = jnp.cumsum(sizes)
    starts = ends - sizes
    bounds = jnp.arange(LOOKS // CHUNK, dtype=i32) * CHUNK
    first_bag = jnp.sum((ends[None, :] <= bounds[:, None]).astype(i32), axis=1) // 16 * 16
    extra = C_ROWS - BAGS
    ends2 = jnp.concatenate([ends, jnp.zeros((extra,), i32)]).reshape(C_ROWS // 128, 128)
    starts2 = jnp.concatenate([starts, jnp.full((extra,), LOOKS, i32)]).reshape(C_ROWS // 128, 128)
    upper, lower, look_rows, first_bag, starts2, ends2 = lax.optimization_barrier(
        (upper, lower, look_rows, first_bag, starts2, ends2)
    )
    upper2, lower2 = from_partner(upper, 3), from_partner(lower, 1)
    counts = pl.pallas_call(
        count_kernel,
        out_shape=jax.ShapeDtypeStruct((C_ROWS, ROWS), bf16),
        in_specs=[SMEM, VMEM, VMEM, VMEM],
        out_specs=VMEM,
        scratch_shapes=[pltpu.VMEM((C_ROWS, 128), i32), pltpu.VMEM((C_ROWS, 128), i32)],
        compiler_params=params(vmem_limit_bytes=24 << 20),
        cost_estimate=pl.CostEstimate(flops=2 * LOOKS * SPAN * ROWS, bytes_accessed=10 << 20, transcendentals=0),
        name="count",
    )(first_bag, look_rows.reshape(LOOKS // 128, 128), starts2, ends2)

    dma = pltpu.SemaphoreType.DMA
    got_rows, got_slots, held = pl.pallas_call(
        pool_kernel,
        out_shape=(
            jax.ShapeDtypeStruct((DEVICES * CAP, E), f32),
            jax.ShapeDtypeStruct((DEVICES, 1, 128), i32),
            jax.ShapeDtypeStruct((ROWS, E), f32),
        ),
        in_specs=[SMEM, SMEM, VMEM, VMEM, VMEM, VMEM, VMEM, VMEM],
        out_specs=(VMEM, VMEM, VMEM),
        scratch_shapes=[
            pltpu.VMEM((ROWS, 256), bf16),
            pltpu.VMEM((BAGS, E), f32),
            pltpu.VMEM((DEVICES * CAP, E), f32),
            dma,
            dma,
            dma,
            dma,
        ],
        compiler_params=params(collective_id=0, has_side_effects=True, vmem_limit_bytes=20 << 20),
        name="pool",
    )(pair_mask, send_bags, send_slots, counts, upper, upper2, lower, lower2)
    slot_of = got_slots.reshape(DEVICES * 128)

    pooled_grads, grads = pl.pallas_call(
        dense_kernel,
        out_shape=(
            jax.ShapeDtypeStruct((BAGS + 8, E), f32),
            jax.ShapeDtypeStruct((G_ROWS, 128), f32),
        ),
        in_specs=[SMEM, VMEM, VMEM, VMEM, VMEM, VMEM],
        out_specs=(VMEM, VMEM),
        scratch_shapes=[
            pltpu.VMEM((F + 1, E, B_DEV), f32),
            pltpu.VMEM((INTER, B_DEV), f32),
        ],
        compiler_params=params(vmem_limit_bytes=20 << 20),
        name="dense",
    )(slot_of, got_rows, dense_vectors, labels[:, None], top_weight, out_weight[None, :])

    new_table, new_state, top_grad, out_grad = pl.pallas_call(
        update_kernel,
        out_shape=(
            jax.ShapeDtypeStruct((ROWS, E), f32),
            jax.ShapeDtypeStruct((1, ROWS), f32),
            jax.ShapeDtypeStruct((INTER, HID), f32),
            jax.ShapeDtypeStruct((1, HID), f32),
        ),
        in_specs=[SMEM, SMEM, SMEM, VMEM, VMEM, VMEM, VMEM, VMEM],
        out_specs=(VMEM, VMEM, VMEM, VMEM),
        scratch_shapes=[
            pltpu.VMEM((DEVICES * CAP, E), f32),
            pltpu.VMEM((DEVICES * CAP, E), f32),
            pltpu.VMEM((BAGS, E), f32),
            pltpu.VMEM((2 * E, BAGS), bf16),
            pltpu.VMEM((G_ROWS, 128), f32),
            pltpu.VMEM((HALF, 128), f32),
            pltpu.VMEM((HALF, 128), f32),
            pltpu.VMEM((16, SEG, 128), f32),
            pltpu.VMEM((SEG, 128), f32),
            pltpu.VMEM((4, SEG, 128), f32),
            pltpu.VMEM((4, 1, ROWS), f32),
            dma((4,)),
            dma((4,)),
            dma,
            dma,
            dma,
            dma,
            dma((16,)),
            dma((16,)),
            dma((4,)),
            dma((4,)),
            dma((16,)),
            dma((16,)),
            dma,
            dma,
        ],
        compiler_params=params(collective_id=1, has_side_effects=True, vmem_limit_bytes=24 << 20),
        name="update",
    )(pair_mask, slot_of, where_to, pooled_grads, grads, counts, held, row_state[None, :])
    return new_table, new_state.reshape(ROWS), top_grad, out_grad.reshape(HID)


def solution(mesh):
    both = ("gx", "gy")
    in_specs = (
        P(both, None),
        P(both),
        P("gx"),
        P(both),
        P(both, None),
        P(both, None),
        P(both),
        P(both, None),
        P(both),
        P(),
        P(),
    )
    out_specs = (P(both, None), P(both), P(), P())
    return jax.shard_map(
        on_device, mesh=mesh, in_specs=in_specs, out_specs=out_specs, check_vma=False
    )
```

```python
import jax
import jax.numpy as jnp
from jax import lax
from jax.experimental import pallas as pl
from jax.experimental.pallas import tpu as pltpu
from jax.sharding import PartitionSpec as P

E = 128
F = 16
B_DEV = 128
BAGS = 2048
ROWS = 2048
LOOKS = 6144
DEVICES = 128
CAP = 32
INTER = 264
HID = 1024
CHUNK = 256
SPAN = CHUNK + 16
C_ROWS = 2304
G_ROWS = 2304
HALF = G_ROWS // 2
PART = (40, 32)
STRIDE = 37
CUTS = (1, 36, 60, 84, 108, 128)
PAIRS = [(i, j) for i in range(F + 1) for j in range(i + 1, F + 1)]
PAIR_ROW = {pair: 128 + n for n, pair in enumerate(PAIRS)}

learn_rate = 0.05
epsilon = 1e-08
MESH = pl.DeviceIdType.MESH
f32, bf16, i32 = jnp.float32, jnp.bfloat16, jnp.int32

VMEM = pl.BlockSpec(memory_space=pltpu.VMEM)
SMEM = pl.BlockSpec(memory_space=pltpu.SMEM)


def split(x):
    hi = x.astype(bf16)
    return hi, (x - hi.astype(f32)).astype(bf16)


def mxu(a, b, dims):
    return lax.dot_general(a, b, (dims, ((), ())), preferred_element_type=f32)


def dot3(a, b, dims):
    return mxu(a[0], b[0], dims) + (mxu(a[0], b[1], dims) + mxu(a[1], b[0], dims))


NN = ((1,), (0,))
NT = ((1,), (1,))


def down_sublanes(row):
    return jnp.broadcast_to(row, (128, 128)).T


def count_kernel(first_ref, look_ref, start_ref, end_ref, c_ref, start_t, end_t):
    for r in range(C_ROWS // 128):
        here = slice(r * 128, (r + 1) * 128)
        start_t[here, :] = down_sublanes(start_ref[r : r + 1, :])
        end_t[here, :] = down_sublanes(end_ref[r : r + 1, :])
    c_ref[0:16, :] = jnp.zeros((16, ROWS), bf16)
    lane = lax.broadcasted_iota(i32, (1, 128), 1)

    def chunk(t, carry):
        at = pl.multiple_of(first_ref[t], 16)
        start, end = start_t[pl.ds(at, SPAN), :], end_t[pl.ds(at, SPAN), :]
        halves, columns = [], []
        for h in range(2):
            k = lane + (t * CHUNK + h * 128)
            halves.append(((start <= k) & (k < end)).astype(f32).astype(bf16))
            columns.append(down_sublanes(look_ref[pl.ds(2 * t + h, 1), :]))
        in_bag = jnp.concatenate(halves, axis=1)
        column = jnp.concatenate(columns, axis=0)
        for n in range(0, 16, 4):
            of_row = jnp.concatenate(
                [(column == lane + 128 * q).astype(f32).astype(bf16) for q in range(n, n + 4)],
                axis=1,
            )
            counts = mxu(in_bag, of_row, NN)
            cols = slice(n * 128, (n + 4) * 128)
            before = c_ref[pl.ds(at, 16), cols].astype(f32)
            c_ref[pl.ds(at, 16), cols] = (counts[:16] + before).astype(bf16)
            c_ref[pl.ds(pl.multiple_of(at + 16, 16), SPAN - 16), cols] = counts[16:].astype(bf16)
        return carry

    lax.fori_loop(0, LOOKS // CHUNK, chunk, 0)


def device_at(n):
    return (n // 4, n % 4)


def my_number():
    return lax.axis_index("gx") * 4 + lax.axis_index("gy")


def peer_of(k):
    return (my_number() + STRIDE * k) % DEVICES


def greet_all(barrier):
    def greet(k, carry):
        pl.semaphore_signal(barrier, inc=1, device_id=device_at(peer_of(k)), device_id_type=MESH)
        return carry

    lax.fori_loop(1, DEVICES, greet, 0)


def put(src, dst, send, recv, device):
    return pltpu.make_async_remote_copy(
        src_ref=src, dst_ref=dst, send_sem=send, recv_sem=recv, device_id=device, device_id_type=MESH
    )


def chunk_at(n):
    return pl.ds(pl.multiple_of(n * CAP, CAP), CAP)


def pick_rows(dst, to, src, index_ref, at):
    for u in range(CAP):
        dst[pl.ds(to + u, 1), :] = src[pl.ds(index_ref[at + u], 1), :]


def pool_kernel(
    mask_ref,
    bag_ref,
    slots_ref,
    c_ref,
    a_ref,
    a2_ref,
    b_ref,
    b2_ref,
    recv_ref,
    got_ref,
    held_ref,
    split_ref,
    partial_ref,
    send_ref,
    row_send,
    row_recv,
    slot_send,
    slot_recv,
):
    barrier = pltpu.get_barrier_semaphore()
    greet_all(barrier)
    me = my_number()
    mask = jnp.full((ROWS // 2, E), mask_ref[0], i32)
    held_ref[: ROWS // 2, :] = jnp.where(mask >= 2, a2_ref[...], a_ref[...])
    held_ref[ROWS // 2 :, :] = jnp.where((mask == 1) | (mask == 2), b2_ref[...], b_ref[...])
    hi, lo = split(held_ref[...])
    split_ref[:, :128] = hi
    split_ref[:, 128:] = lo

    def block(m, carry):
        at = pl.multiple_of(m * 256, 256)
        both = mxu(c_ref[pl.ds(at, 256), :], split_ref[...], NN)
        partial_ref[pl.ds(at, 256), :] = both[:, :128] + both[:, 128:]
        return carry

    lax.fori_loop(0, BAGS // 256, block, 0)
    got_ref[me] = slots_ref[me]
    pick_rows(recv_ref, me * CAP, partial_ref, bag_ref, me * CAP)

    def ready(k):
        at = peer_of(k) * CAP
        pick_rows(send_ref, at, partial_ref, bag_ref, at)

    def start(k):
        peer = peer_of(k)
        to = device_at(peer)
        put(slots_ref.at[peer], got_ref.at[me], slot_send, slot_recv, to).start()
        put(send_ref.at[chunk_at(peer)], recv_ref.at[chunk_at(me)], row_send, row_recv, to).start()

    ready(1)
    pl.semaphore_wait(barrier, DEVICES - 1)

    def step(k, carry):
        ready(k)
        start(k - 1)
        return carry

    lax.fori_loop(2, DEVICES, step, 0)
    start(DEVICES - 1)
    to = device_at(peer_of(1))
    some = pl.ds(0, DEVICES - 1)
    put(slots_ref.at[some], got_ref.at[some], slot_send, slot_recv, to).wait()
    rows = pl.ds(0, (DEVICES - 1) * CAP)
    put(send_ref.at[rows], recv_ref.at[rows], row_send, row_recv, to).wait()


def dense_kernel(
    slot_ref, got_ref, dense_ref, label_ref, w_ref, wo_ref, vt, d_pre_ref, grad_ref, pooled, inter_t
):

    def place(c, carry):
        @pl.when(slot_ref[c * 128] < BAGS)
        def _():
            for u in range(CAP):
                pooled[pl.ds(slot_ref[c * 128 + u], 1), :] = got_ref[pl.ds(c * CAP + u, 1), :]

        return carry

    lax.fori_loop(0, DEVICES, place, 0)

    dense_t = dense_ref[...].T
    vt[0] = dense_t
    inter_t[0:128, :] = dense_t
    for f in range(F):
        vt[f + 1] = pooled[f * 128 : (f + 1) * 128, :].T
    for i in range(F):
        for j in range(i + 1, F + 1):
            row = PAIR_ROW[i, j]
            inter_t[row : row + 1, :] = jnp.sum(vt[i] * vt[j], axis=0, keepdims=True)

    it = inter_t[...]
    w = split(w_ref[...])
    pre = dot3(split(it.T), w, NN)
    sig = 1.0 / (1.0 + jnp.exp(-pre))
    hidden = pre * sig
    logits = jnp.sum(hidden * wo_ref[...], axis=1, keepdims=True)
    d_logits = 1.0 / (1.0 + jnp.exp(-logits)) - label_ref[...]
    out_grad = jnp.sum(hidden * d_logits, axis=0, keepdims=True)
    for q in range(8):
        grad_ref[8 * INTER + q : 8 * INTER + q + 1, :] = out_grad[:, q * 128 : (q + 1) * 128]
    grad_ref[8 * INTER + 8 :, :] = jnp.zeros((G_ROWS - 8 * INTER - 8, 128), f32)
    d_pre_ref[...] = d_logits * wo_ref[...] * (sig * (1.0 + pre * (1.0 - sig)))
    top_grad = dot3(split(it), split(d_pre_ref[...]), NN)
    for q in range(8):
        grad_ref[q * INTER : (q + 1) * INTER, :] = top_grad[:, q * 128 : (q + 1) * 128]


def update_kernel(
    mask_ref,
    slot_ref,
    where_ref,
    vt,
    d_pre_ref,
    w_ref,
    g_ref,
    c_ref,
    table_ref,
    state_ref,
    new_table_ref,
    new_state_ref,
    top_ref,
    out_ref,
    back,
    came,
    grads,
    sides,
    fin,
    pooled,
    d_inter,
    r1,
    acc,
    states,
    ra0,
    ra1,
    acc0,
    acc1,
    rb0,
    rb1,
    mine0,
    mine1,
    rx0,
    rx1,
    state_send,
    state_recv,
    row_send,
    row_recv,
    swap_send,
    swap_recv,
    last_send,
    last_recv,
    color_send,
    color_recv,
):
    barrier = pltpu.get_barrier_semaphore()
    greet_all(barrier)
    me = my_number()
    gx, x = lax.axis_index("gx"), lax.axis_index("gy")
    yz, core = gx // 2, gx % 2
    twin = (gx + 1 - 2 * core, x)

    y, z = yz // 4, yz % 4

    def along_x(k):
        return (gx, (x + k) % 4)

    def along_y(k):
        return (((y + k) % 4 * 4 + z) * 2 + core, x)

    def along_z(k):
        return ((y * 4 + (z + k) % 4) * 2 + core, x)

    d_inter[...] = dot3(split(w_ref[...]), split(d_pre_ref[...]), NT)
    for j in range(1, F + 1):
        total = None
        for i in range(F + 1):
            if i != j:
                row = PAIR_ROW[min(i, j), max(i, j)]
                term = d_inter[row : row + 1, :] * vt[i]
                total = term if total is None else total + term
        pooled[(j - 1) * 128 : j * 128, :] = total.T
    pooled[BAGS:, :] = jnp.zeros((8, E), f32)
    pick_rows(came, me * CAP, pooled, slot_ref, me * 128)

    def ready(k):
        peer = peer_of(k)
        pick_rows(back, peer * CAP, pooled, slot_ref, peer * 128)

    def start(k):
        peer = peer_of(k)
        put(
            back.at[chunk_at(peer)], came.at[chunk_at(me)], row_send, row_recv, device_at(peer)
        ).start()

    def send_rows(n):
        def step(k, carry):
            ready(k + 1)
            start(k)
            return carry

        last = DEVICES - 1 if CUTS[n + 1] == DEVICES else CUTS[n + 1]
        lax.fori_loop(CUTS[n], last, step, 0)
        if last < CUTS[n + 1]:
            start(last)

    ready(1)
    my_half = pl.multiple_of(core * HALF, 8)
    other = pl.multiple_of((1 - core) * HALF, 8)

    class Color:
        def __init__(self, n, base, at, to_a, to_b, ra, acc2, rb, mine, rx):
            self.n, self.rows, self.base, self.at = n, PART[n], base, at
            self.to = (to_a, to_b, along_x, to_b, to_a)
            self.ra, self.acc2, self.rb, self.mine, self.rx = ra, acc2, rb, mine, rx

        def move(self, phase, k, src, dst):
            sem = (self.n * 5 + phase) * 4 + k
            return put(src, dst, color_send.at[sem], color_recv.at[sem], self.to[phase](k))

        def rows_a(self, a, base):
            return pl.ds(pl.multiple_of(base + self.base + a * (4 * self.rows), 8), 4 * self.rows)

        def rows_b(self, a, b, base):
            return pl.ds(
                pl.multiple_of(base + self.base + (a * 4 + b) * self.rows, 8), self.rows
            )

        def moves(self, phase, waiting):
            a, b = self.at
            out = []
            for k in range(1, 4):
                if phase == 0:
                    out.append(self.move(0, k, acc.at[self.rows_a((a + k) % 4, 0)], self.ra.at[k]))
                if phase == 1:
                    there = pl.ds(pl.multiple_of((b + k) % 4 * self.rows, 8), self.rows)
                    out.append(self.move(1, k, self.acc2.at[there], self.rb.at[k]))
                if phase == 2:
                    slot = (x + 4 - k) % 4 if waiting else x
                    out.append(self.move(2, k, self.mine, self.rx.at[slot]))
                if phase == 3:
                    who = (b + 4 - k) % 4 if waiting else b
                    there = fin.at[self.rows_b(a, who, my_half)]
                    out.append(self.move(3, k, there, there))
                if phase == 4:
                    who = (a + 4 - k) % 4 if waiting else a
                    there = fin.at[self.rows_a(who, my_half)]
                    out.append(self.move(4, k, there, there))
            return out

        def begin(self, phase):
            for copy in self.moves(phase, False):
                copy.start()

        def finish(self, phase):
            for copy in self.moves(phase, False):
                copy.wait_send()
            for copy in self.moves(phase, True):
                copy.wait_recv()
            a, b = self.at
            if phase == 0:
                own = acc[self.rows_a(a, 0), :]
                self.acc2[...] = (own + self.ra[1]) + (self.ra[2] + self.ra[3])
            if phase == 1:
                own = self.acc2[pl.ds(pl.multiple_of(b * self.rows, 8), self.rows), :]
                part = (own + self.rb[1]) + (self.rb[2] + self.rb[3])
                self.mine[...] = part
                self.rx[x] = part
            if phase == 2:
                whole = (self.rx[0] + self.rx[1]) + (self.rx[2] + self.rx[3])
                fin[self.rows_b(a, b, my_half), :] = whole

    colors = (
        Color(0, 0, (z, y), along_z, along_y, ra0, acc0, rb0, mine0, rx0),
        Color(1, 16 * PART[0], (y, z), along_y, along_z, ra1, acc1, rb1, mine1, rx1),
    )

    def phase_on(phase):
        for color in colors:
            color.begin(phase)

    def phase_off(phase):
        for color in colors:
            color.finish(phase)

    pl.semaphore_wait(barrier, DEVICES - 1)
    swap = put(g_ref.at[pl.ds(other, HALF)], r1, swap_send, swap_recv, twin)
    swap.start()
    flips = [None, x + 1 - 2 * (x % 2), (x + 2) % 4, 3 - x]
    state_moves = [
        put(state_ref, states.at[f], state_send.at[f], state_recv.at[f], (gx, flips[f]))
        for f in range(1, 4)
    ]
    for move in state_moves:
        move.start()
    send_rows(0)
    swap.wait()
    acc[...] = g_ref[pl.ds(my_half, HALF), :] + r1[...]
    phase_on(0)
    for phase in range(4):
        send_rows(phase + 1)
        phase_off(phase)
        phase_on(phase + 1)

    rows = pl.ds(0, (DEVICES - 1) * CAP)
    put(back.at[rows], came.at[rows], row_send, row_recv, device_at(peer_of(1))).wait()
    for move in state_moves:
        move.wait()
    mask = jnp.full((1, ROWS), mask_ref[0], i32)
    held_state = state_ref[...]
    for f in range(1, 4):
        held_state = jnp.where(mask == f, states[f], held_state)
    states[0] = held_state

    def take(n, carry):
        for u in range(16):
            b = n * 16 + u
            grads[pl.ds(b, 1), :] = came[pl.ds(where_ref[b], 1), :]
        return carry

    lax.fori_loop(0, BAGS // 16, take, 0)
    for q in range(BAGS // 128):
        here = slice(q * 128, (q + 1) * 128)
        hi, lo = split(grads[here, :].T)
        sides[0:128, here] = hi
        sides[128:256, here] = lo

    def block(n, carry):
        here = pl.ds(pl.multiple_of(n * 256, 256), 256)
        both = mxu(sides[...], c_ref[0:BAGS, here], NN)
        row_grad = both[:128] + both[128:]
        state = states[0, :, here] + jnp.sum(row_grad * row_grad, axis=0, keepdims=True) * (1.0 / E)
        new_state_ref[:, here] = state
        step = row_grad * (learn_rate / (jnp.sqrt(state) + epsilon))
        new_table_ref[here, :] = table_ref[here, :] - step.T
        return carry

    lax.fori_loop(0, ROWS // 256, block, 0)

    phase_off(4)
    half = fin.at[pl.ds(my_half, HALF)]
    rest = fin.at[pl.ds(other, HALF)]
    last = put(half, half, last_send, last_recv, twin)
    last.start()
    last.wait_send()
    put(rest, rest, last_send, last_recv, twin).wait_recv()
    for q in range(8):
        top_ref[:, q * 128 : (q + 1) * 128] = fin[q * INTER : (q + 1) * INTER, :]
        out_ref[:, q * 128 : (q + 1) * 128] = fin[8 * INTER + q : 8 * INTER + q + 1, :]


def params(**kw):
    return pltpu.CompilerParams(**kw)


def from_partner(block, flip):
    return lax.ppermute(block, "gy", [(y, y ^ flip) for y in range(4)])


def on_device(
    emb_table,
    row_state,
    pair_mask,
    look_rows,
    bag_sizes,
    bag_owner,
    bag_slot,
    dense_vectors,
    labels,
    top_weight,
    out_weight,
):
    mask = pair_mask[0]
    first, second = (mask == 1) | (mask == 2), mask >= 2
    upper, lower = emb_table[: ROWS // 2], emb_table[ROWS // 2 :]
    upper = jnp.where(first, from_partner(upper, 1), upper)
    lower = jnp.where(second, from_partner(lower, 3), lower)

    owners = bag_owner[:, 0]
    onehot = (owners[:, None] == jnp.arange(DEVICES, dtype=i32)[None, :]).astype(i32)
    placed_at = jnp.sum((jnp.cumsum(onehot, axis=0) - onehot) * onehot, axis=1)
    where_to = owners * CAP + placed_at
    spot = (placed_at[:, None] == jnp.arange(CAP, dtype=i32)[None, :]).astype(f32)
    sample, feature = bag_slot // F, bag_slot % F
    bag = jnp.arange(BAGS, dtype=i32)
    pieces = [sample, feature + 1, bag // 16, bag % 16]
    parts = jnp.concatenate([spot * piece.astype(f32)[:, None] for piece in pieces], axis=1)
    coded = mxu(onehot.astype(bf16), parts.astype(bf16), ((0,), (0,))).astype(i32)
    sample_at, feature_at = coded[:, :CAP], coded[:, CAP : 2 * CAP]
    send_slots = jnp.where(feature_at > 0, (feature_at - 1) * B_DEV + sample_at, BAGS)
    send_slots = jnp.pad(send_slots, ((0, 0), (0, 128 - CAP))).reshape(DEVICES, 1, 128)
    send_bags = (coded[:, 2 * CAP : 3 * CAP] * 16 + coded[:, 3 * CAP :]).reshape(DEVICES * CAP)

    sizes = bag_sizes[0]
    ends = jnp.cumsum(sizes)
    starts = ends - sizes
    bounds = jnp.arange(LOOKS // CHUNK, dtype=i32) * CHUNK
    first_bag = jnp.sum((ends[None, :] <= bounds[:, None]).astype(i32), axis=1) // 16 * 16
    extra = C_ROWS - BAGS
    ends2 = jnp.concatenate([ends, jnp.zeros((extra,), i32)]).reshape(C_ROWS // 128, 128)
    starts2 = jnp.concatenate([starts, jnp.full((extra,), LOOKS, i32)]).reshape(C_ROWS // 128, 128)
    upper, lower, look_rows, first_bag, starts2, ends2 = lax.optimization_barrier(
        (upper, lower, look_rows, first_bag, starts2, ends2)
    )
    upper2, lower2 = from_partner(upper, 3), from_partner(lower, 1)
    counts = pl.pallas_call(
        count_kernel,
        out_shape=jax.ShapeDtypeStruct((C_ROWS, ROWS), bf16),
        in_specs=[SMEM, VMEM, VMEM, VMEM],
        out_specs=VMEM,
        scratch_shapes=[pltpu.VMEM((C_ROWS, 128), i32), pltpu.VMEM((C_ROWS, 128), i32)],
        compiler_params=params(vmem_limit_bytes=24 << 20),
        cost_estimate=pl.CostEstimate(flops=2 * LOOKS * SPAN * ROWS, bytes_accessed=10 << 20, transcendentals=0),
        name="count",
    )(first_bag, look_rows.reshape(LOOKS // 128, 128), starts2, ends2)

    dma = pltpu.SemaphoreType.DMA
    got_rows, got_slots, held = pl.pallas_call(
        pool_kernel,
        out_shape=(
            jax.ShapeDtypeStruct((DEVICES * CAP, E), f32),
            jax.ShapeDtypeStruct((DEVICES, 1, 128), i32),
            jax.ShapeDtypeStruct((ROWS, E), f32),
        ),
        in_specs=[SMEM, SMEM, VMEM, VMEM, VMEM, VMEM, VMEM, VMEM],
        out_specs=(VMEM, VMEM, VMEM),
        scratch_shapes=[
            pltpu.VMEM((ROWS, 256), bf16),
            pltpu.VMEM((BAGS, E), f32),
            pltpu.VMEM((DEVICES * CAP, E), f32),
            dma,
            dma,
            dma,
            dma,
        ],
        compiler_params=params(collective_id=0, has_side_effects=True, vmem_limit_bytes=20 << 20),
        name="pool",
    )(pair_mask, send_bags, send_slots, counts, upper, upper2, lower, lower2)
    slot_of = got_slots.reshape(DEVICES * 128)

    vectors_t, d_pre, grads = pl.pallas_call(
        dense_kernel,
        out_shape=(
            jax.ShapeDtypeStruct((F + 1, E, B_DEV), f32),
            jax.ShapeDtypeStruct((B_DEV, HID), f32),
            jax.ShapeDtypeStruct((G_ROWS, 128), f32),
        ),
        in_specs=[SMEM, VMEM, VMEM, VMEM, VMEM, VMEM],
        out_specs=(VMEM, VMEM, VMEM),
        scratch_shapes=[
            pltpu.VMEM((BAGS, E), f32),
            pltpu.VMEM((INTER, B_DEV), f32),
        ],
        compiler_params=params(vmem_limit_bytes=20 << 20),
        name="dense",
    )(slot_of, got_rows, dense_vectors, labels[:, None], top_weight, out_weight[None, :])

    new_table, new_state, top_grad, out_grad = pl.pallas_call(
        update_kernel,
        out_shape=(
            jax.ShapeDtypeStruct((ROWS, E), f32),
            jax.ShapeDtypeStruct((1, ROWS), f32),
            jax.ShapeDtypeStruct((INTER, HID), f32),
            jax.ShapeDtypeStruct((1, HID), f32),
        ),
        in_specs=[SMEM, SMEM, SMEM] + [VMEM] * 7,
        out_specs=(VMEM, VMEM, VMEM, VMEM),
        scratch_shapes=[
            pltpu.VMEM((DEVICES * CAP, E), f32),
            pltpu.VMEM((DEVICES * CAP, E), f32),
            pltpu.VMEM((BAGS, E), f32),
            pltpu.VMEM((2 * E, BAGS), bf16),
            pltpu.VMEM((G_ROWS, 128), f32),
            pltpu.VMEM((BAGS + 8, E), f32),
            pltpu.VMEM((INTER, B_DEV), f32),
            pltpu.VMEM((HALF, 128), f32),
            pltpu.VMEM((HALF, 128), f32),
            pltpu.VMEM((4, 1, ROWS), f32),
            *[pltpu.VMEM((4, 4 * rows, 128), f32) for rows in PART],
            *[pltpu.VMEM((4 * rows, 128), f32) for rows in PART],
            *[pltpu.VMEM((4, rows, 128), f32) for rows in PART],
            *[pltpu.VMEM((rows, 128), f32) for rows in PART],
            *[pltpu.VMEM((4, rows, 128), f32) for rows in PART],
            dma((4,)),
            dma((4,)),
            dma,
            dma,
            dma,
            dma,
            dma,
            dma,
            dma((40,)),
            dma((40,)),
        ],
        compiler_params=params(collective_id=1, has_side_effects=True, vmem_limit_bytes=26 << 20),
        name="update",
    )(
        pair_mask,
        slot_of,
        where_to,
        vectors_t,
        d_pre,
        top_weight,
        grads,
        counts,
        held,
        row_state[None, :],
    )
    return new_table, new_state.reshape(ROWS), top_grad, out_grad.reshape(HID)


def solution(mesh):
    both = ("gx", "gy")
    in_specs = (
        P(both, None),
        P(both),
        P("gx"),
        P(both),
        P(both, None),
        P(both, None),
        P(both),
        P(both, None),
        P(both),
        P(),
        P(),
    )
    out_specs = (P(both, None), P(both), P(), P())
    return jax.shard_map(
        on_device, mesh=mesh, in_specs=in_specs, out_specs=out_specs, check_vma=False
    )
```

```python
import jax
import jax.numpy as jnp
from jax import lax
from jax.experimental import pallas as pl
from jax.experimental.pallas import tpu as pltpu
from jax.sharding import PartitionSpec as P

E = 128
F = 16
B_DEV = 128
BAGS = 2048
ROWS = 2048
LOOKS = 6144
DEVICES = 128
CAP = 32
INTER = 264
HID = 1024
CHUNK = 256
SPAN = CHUNK + 16
C_ROWS = 2304
G_ROWS = 2304
HALF = G_ROWS // 2
PART = (40, 32)
STRIDE = 37
CUTS = (1, 32, 58, 82, 106, 128)
PAIRS = [(i, j) for i in range(F + 1) for j in range(i + 1, F + 1)]
PAIR_ROW = {pair: 128 + n for n, pair in enumerate(PAIRS)}

learn_rate = 0.05
epsilon = 1e-08
MESH = pl.DeviceIdType.MESH
f32, bf16, i32 = jnp.float32, jnp.bfloat16, jnp.int32

VMEM = pl.BlockSpec(memory_space=pltpu.VMEM)
SMEM = pl.BlockSpec(memory_space=pltpu.SMEM)


def split(x):
    hi = x.astype(bf16)
    return hi, (x - hi.astype(f32)).astype(bf16)


def mxu(a, b, dims):
    return lax.dot_general(a, b, (dims, ((), ())), preferred_element_type=f32)


def dot3(a, b, dims):
    return mxu(a[0], b[0], dims) + (mxu(a[0], b[1], dims) + mxu(a[1], b[0], dims))


NN = ((1,), (0,))
NT = ((1,), (1,))


def down_sublanes(row):
    return jnp.broadcast_to(row, (128, 128)).T


def count_kernel(first_ref, look_ref, start_ref, end_ref, c_ref, start_t, end_t):
    for r in range(C_ROWS // 128):
        here = slice(r * 128, (r + 1) * 128)
        start_t[here, :] = down_sublanes(start_ref[r : r + 1, :])
        end_t[here, :] = down_sublanes(end_ref[r : r + 1, :])
    c_ref[0:16, :] = jnp.zeros((16, ROWS), bf16)
    lane = lax.broadcasted_iota(i32, (1, 128), 1)

    def chunk(t, carry):
        at = pl.multiple_of(first_ref[t], 16)
        start, end = start_t[pl.ds(at, SPAN), :], end_t[pl.ds(at, SPAN), :]
        halves, columns = [], []
        for h in range(2):
            k = lane + (t * CHUNK + h * 128)
            halves.append(((start <= k) & (k < end)).astype(f32).astype(bf16))
            columns.append(down_sublanes(look_ref[pl.ds(2 * t + h, 1), :]))
        in_bag = jnp.concatenate(halves, axis=1)
        column = jnp.concatenate(columns, axis=0)
        for n in range(0, 16, 4):
            of_row = jnp.concatenate(
                [(column == lane + 128 * q).astype(f32).astype(bf16) for q in range(n, n + 4)],
                axis=1,
            )
            counts = mxu(in_bag, of_row, NN)
            cols = slice(n * 128, (n + 4) * 128)
            before = c_ref[pl.ds(at, 16), cols].astype(f32)
            c_ref[pl.ds(at, 16), cols] = (counts[:16] + before).astype(bf16)
            c_ref[pl.ds(pl.multiple_of(at + 16, 16), SPAN - 16), cols] = counts[16:].astype(bf16)
        return carry

    lax.fori_loop(0, LOOKS // CHUNK, chunk, 0, unroll=2)


def device_at(n):
    return (n // 4, n % 4)


def my_number():
    return lax.axis_index("gx") * 4 + lax.axis_index("gy")


def peer_of(k):
    return (my_number() + STRIDE * k) % DEVICES


def greet_all(barrier):
    def greet(k, carry):
        pl.semaphore_signal(barrier, inc=1, device_id=device_at(peer_of(k)), device_id_type=MESH)
        return carry

    lax.fori_loop(1, DEVICES, greet, 0)


def put(src, dst, send, recv, device):
    return pltpu.make_async_remote_copy(
        src_ref=src, dst_ref=dst, send_sem=send, recv_sem=recv, device_id=device, device_id_type=MESH
    )


def chunk_at(n):
    return pl.ds(pl.multiple_of(n * CAP, CAP), CAP)


def pick_rows(dst, to, src, index_ref, at):
    for u in range(CAP):
        dst[pl.ds(to + u, 1), :] = src[pl.ds(index_ref[at + u], 1), :]


def pool_kernel(
    mask_ref,
    bag_ref,
    slots_ref,
    c_ref,
    a_ref,
    a2_ref,
    b_ref,
    b2_ref,
    recv_ref,
    got_ref,
    held_ref,
    split_ref,
    partial_ref,
    send_ref,
    row_send,
    row_recv,
    slot_send,
    slot_recv,
):
    barrier = pltpu.get_barrier_semaphore()
    greet_all(barrier)
    me = my_number()
    mask = jnp.full((ROWS // 2, E), mask_ref[0], i32)
    held_ref[: ROWS // 2, :] = jnp.where(mask >= 2, a2_ref[...], a_ref[...])
    held_ref[ROWS // 2 :, :] = jnp.where((mask == 1) | (mask == 2), b2_ref[...], b_ref[...])
    hi, lo = split(held_ref[...])
    split_ref[:, :128] = hi
    split_ref[:, 128:] = lo

    def block(m, carry):
        at = pl.multiple_of(m * 256, 256)
        both = mxu(c_ref[pl.ds(at, 256), :], split_ref[...], NN)
        partial_ref[pl.ds(at, 256), :] = both[:, :128] + both[:, 128:]
        return carry

    lax.fori_loop(0, BAGS // 256, block, 0)
    got_ref[me] = slots_ref[me]
    pick_rows(recv_ref, me * CAP, partial_ref, bag_ref, me * CAP)

    def ready(k):
        at = peer_of(k) * CAP
        pick_rows(send_ref, at, partial_ref, bag_ref, at)

    def start(k):
        peer = peer_of(k)
        to = device_at(peer)
        put(slots_ref.at[peer], got_ref.at[me], slot_send, slot_recv, to).start()
        put(send_ref.at[chunk_at(peer)], recv_ref.at[chunk_at(me)], row_send, row_recv, to).start()

    ready(1)
    pl.semaphore_wait(barrier, DEVICES - 1)

    def step(k, carry):
        ready(k)
        start(k - 1)
        return carry

    lax.fori_loop(2, DEVICES, step, 0)
    start(DEVICES - 1)
    to = device_at(peer_of(1))
    some = pl.ds(0, DEVICES - 1)
    put(slots_ref.at[some], got_ref.at[some], slot_send, slot_recv, to).wait()
    rows = pl.ds(0, (DEVICES - 1) * CAP)
    put(send_ref.at[rows], recv_ref.at[rows], row_send, row_recv, to).wait()


def place_kernel(slot_ref, got_ref, pooled):
    def place(c, carry):
        @pl.when(slot_ref[c * 128] < BAGS)
        def _():
            for u in range(CAP):
                pooled[pl.ds(slot_ref[c * 128 + u], 1), :] = got_ref[pl.ds(c * CAP + u, 1), :]

        return carry

    lax.fori_loop(0, DEVICES, place, 0)


def update_kernel(
    mask_ref,
    slot_ref,
    where_ref,
    sums_ref,
    dense_ref,
    label_ref,
    w_ref,
    wo_ref,
    c_ref,
    table_ref,
    state_ref,
    new_table_ref,
    new_state_ref,
    top_ref,
    out_ref,
    back,
    came,
    grads,
    sides,
    fin,
    pooled,
    inter_t,
    vt,
    d_pre_ref,
    grad_ref,
    r1,
    acc,
    states,
    ra0,
    ra1,
    acc0,
    acc1,
    rb0,
    rb1,
    mine0,
    mine1,
    rx0,
    rx1,
    state_send,
    state_recv,
    row_send,
    row_recv,
    swap_send,
    swap_recv,
    last_send,
    last_recv,
    color_send,
    color_recv,
):
    barrier = pltpu.get_barrier_semaphore()
    greet_all(barrier)
    me = my_number()
    gx, x = lax.axis_index("gx"), lax.axis_index("gy")
    yz, core = gx // 2, gx % 2
    twin = (gx + 1 - 2 * core, x)

    y, z = yz // 4, yz % 4

    def along_x(k):
        return (gx, (x + k) % 4)

    def along_y(k):
        return (((y + k) % 4 * 4 + z) * 2 + core, x)

    def along_z(k):
        return ((y * 4 + (z + k) % 4) * 2 + core, x)

    dense_t = dense_ref[...].T
    vt[0] = dense_t
    inter_t[0:128, :] = dense_t
    for f in range(F):
        vt[f + 1] = sums_ref[f * 128 : (f + 1) * 128, :].T
    for i in range(F):
        for j in range(i + 1, F + 1):
            row = PAIR_ROW[i, j]
            inter_t[row : row + 1, :] = jnp.sum(vt[i] * vt[j], axis=0, keepdims=True)

    it = inter_t[...]
    w = split(w_ref[...])
    pre = dot3(split(it.T), w, NN)
    sig = 1.0 / (1.0 + jnp.exp(-pre))
    hidden = pre * sig
    logits = jnp.sum(hidden * wo_ref[...], axis=1, keepdims=True)
    d_logits = 1.0 / (1.0 + jnp.exp(-logits)) - label_ref[...]
    out_grad = jnp.sum(hidden * d_logits, axis=0, keepdims=True)
    for q in range(8):
        grad_ref[8 * INTER + q : 8 * INTER + q + 1, :] = out_grad[:, q * 128 : (q + 1) * 128]
    grad_ref[8 * INTER + 8 :, :] = jnp.zeros((G_ROWS - 8 * INTER - 8, 128), f32)
    d_pre_ref[...] = d_logits * wo_ref[...] * (sig * (1.0 + pre * (1.0 - sig)))
    d_pre = split(d_pre_ref[...])
    top_grad = dot3(split(it), d_pre, NN)
    for q in range(8):
        grad_ref[q * INTER : (q + 1) * INTER, :] = top_grad[:, q * 128 : (q + 1) * 128]
    inter_t[...] = dot3(w, d_pre, NT)

    def pooled_grad(j):
        total = None
        for i in range(F + 1):
            if i != j:
                row = PAIR_ROW[min(i, j), max(i, j)]
                term = inter_t[row : row + 1, :] * vt[i]
                total = term if total is None else total + term
        pooled[(j - 1) * 128 : j * 128, :] = total.T

    for j in range(1, 7):
        pooled_grad(j)

    my_half = pl.multiple_of(core * HALF, 8)
    other = pl.multiple_of((1 - core) * HALF, 8)
    pl.semaphore_wait(barrier, DEVICES - 1)
    swap = put(grad_ref.at[pl.ds(other, HALF)], r1, swap_send, swap_recv, twin)
    swap.start()
    flips = [None, x + 1 - 2 * (x % 2), (x + 2) % 4, 3 - x]
    state_moves = [
        put(state_ref, states.at[f], state_send.at[f], state_recv.at[f], (gx, flips[f]))
        for f in range(1, 4)
    ]
    for move in state_moves:
        move.start()
    for j in range(7, F + 1):
        pooled_grad(j)
    pooled[BAGS:, :] = jnp.zeros((8, E), f32)

    def ready(k):
        peer = peer_of(k)
        pick_rows(back, peer * CAP, pooled, slot_ref, peer * 128)

    def start(k):
        peer = peer_of(k)
        put(
            back.at[chunk_at(peer)], came.at[chunk_at(me)], row_send, row_recv, device_at(peer)
        ).start()

    def send_rows(n):
        def step(k, carry):
            ready(k + 1)
            start(k)
            return carry

        last = DEVICES - 1 if CUTS[n + 1] == DEVICES else CUTS[n + 1]
        lax.fori_loop(CUTS[n], last, step, 0)
        if last < CUTS[n + 1]:
            start(last)

    class Color:
        def __init__(self, n, base, at, to_a, to_b, ra, acc2, rb, mine, rx):
            self.n, self.rows, self.base, self.at = n, PART[n], base, at
            self.to = (to_a, to_b, along_x, to_b, to_a)
            self.ra, self.acc2, self.rb, self.mine, self.rx = ra, acc2, rb, mine, rx

        def move(self, phase, k, src, dst):
            sem = (self.n * 5 + phase) * 4 + k
            return put(src, dst, color_send.at[sem], color_recv.at[sem], self.to[phase](k))

        def rows_a(self, a, base):
            return pl.ds(pl.multiple_of(base + self.base + a * (4 * self.rows), 8), 4 * self.rows)

        def rows_b(self, a, b, base):
            return pl.ds(
                pl.multiple_of(base + self.base + (a * 4 + b) * self.rows, 8), self.rows
            )

        def moves(self, phase, waiting):
            a, b = self.at
            out = []
            for k in range(1, 4):
                if phase == 0:
                    out.append(self.move(0, k, acc.at[self.rows_a((a + k) % 4, 0)], self.ra.at[k]))
                if phase == 1:
                    there = pl.ds(pl.multiple_of((b + k) % 4 * self.rows, 8), self.rows)
                    out.append(self.move(1, k, self.acc2.at[there], self.rb.at[k]))
                if phase == 2:
                    slot = (x + 4 - k) % 4 if waiting else x
                    out.append(self.move(2, k, self.mine, self.rx.at[slot]))
                if phase == 3:
                    who = (b + 4 - k) % 4 if waiting else b
                    there = fin.at[self.rows_b(a, who, my_half)]
                    out.append(self.move(3, k, there, there))
                if phase == 4:
                    who = (a + 4 - k) % 4 if waiting else a
                    there = fin.at[self.rows_a(who, my_half)]
                    out.append(self.move(4, k, there, there))
            return out

        def begin(self, phase):
            for copy in self.moves(phase, False):
                copy.start()

        def finish(self, phase):
            for copy in self.moves(phase, False):
                copy.wait_send()
            for copy in self.moves(phase, True):
                copy.wait_recv()
            a, b = self.at
            if phase == 0:
                own = acc[self.rows_a(a, 0), :]
                self.acc2[...] = (own + self.ra[1]) + (self.ra[2] + self.ra[3])
            if phase == 1:
                own = self.acc2[pl.ds(pl.multiple_of(b * self.rows, 8), self.rows), :]
                part = (own + self.rb[1]) + (self.rb[2] + self.rb[3])
                self.mine[...] = part
                self.rx[x] = part
            if phase == 2:
                whole = (self.rx[0] + self.rx[1]) + (self.rx[2] + self.rx[3])
                fin[self.rows_b(a, b, my_half), :] = whole

    colors = (
        Color(0, 0, (z, y), along_z, along_y, ra0, acc0, rb0, mine0, rx0),
        Color(1, 16 * PART[0], (y, z), along_y, along_z, ra1, acc1, rb1, mine1, rx1),
    )

    def phase_on(phase):
        for color in colors:
            color.begin(phase)

    def phase_off(phase):
        for color in colors:
            color.finish(phase)

    swap.wait()
    acc[...] = grad_ref[pl.ds(my_half, HALF), :] + r1[...]
    phase_on(0)
    pick_rows(came, me * CAP, pooled, slot_ref, me * 128)
    ready(1)
    for phase in range(4):
        send_rows(phase)
        phase_off(phase)
        phase_on(phase + 1)
    send_rows(4)

    rows = pl.ds(0, (DEVICES - 1) * CAP)
    put(back.at[rows], came.at[rows], row_send, row_recv, device_at(peer_of(1))).wait()
    for move in state_moves:
        move.wait()
    mask = jnp.full((1, ROWS), mask_ref[0], i32)
    held_state = state_ref[...]
    for f in range(1, 4):
        held_state = jnp.where(mask == f, states[f], held_state)
    states[0] = held_state

    def take(n, carry):
        for u in range(16):
            b = n * 16 + u
            grads[pl.ds(b, 1), :] = came[pl.ds(where_ref[b], 1), :]
        return carry

    lax.fori_loop(0, BAGS // 16, take, 0)
    for q in range(BAGS // 128):
        here = slice(q * 128, (q + 1) * 128)
        hi, lo = split(grads[here, :].T)
        sides[0:128, here] = hi
        sides[128:256, here] = lo

    phase_off(4)
    half = fin.at[pl.ds(my_half, HALF)]
    rest = fin.at[pl.ds(other, HALF)]
    last = put(half, half, last_send, last_recv, twin)
    last.start()

    def block(n, carry):
        here = pl.ds(pl.multiple_of(n * 256, 256), 256)
        both = mxu(sides[...], c_ref[0:BAGS, here], NN)
        row_grad = both[:128] + both[128:]
        state = states[0, :, here] + jnp.sum(row_grad * row_grad, axis=0, keepdims=True) * (1.0 / E)
        new_state_ref[:, here] = state
        step = row_grad * (learn_rate / (jnp.sqrt(state) + epsilon))
        new_table_ref[here, :] = table_ref[here, :] - step.T
        return carry

    lax.fori_loop(0, ROWS // 256, block, 0)

    last.wait_send()
    put(rest, rest, last_send, last_recv, twin).wait_recv()
    for q in range(8):
        top_ref[:, q * 128 : (q + 1) * 128] = fin[q * INTER : (q + 1) * INTER, :]
        out_ref[:, q * 128 : (q + 1) * 128] = fin[8 * INTER + q : 8 * INTER + q + 1, :]


def params(**kw):
    return pltpu.CompilerParams(**kw)


def from_partner(block, flip):
    return lax.ppermute(block, "gy", [(y, y ^ flip) for y in range(4)])


def on_device(
    emb_table,
    row_state,
    pair_mask,
    look_rows,
    bag_sizes,
    bag_owner,
    bag_slot,
    dense_vectors,
    labels,
    top_weight,
    out_weight,
):
    mask = pair_mask[0]
    first, second = (mask == 1) | (mask == 2), mask >= 2
    upper, lower = emb_table[: ROWS // 2], emb_table[ROWS // 2 :]
    upper = jnp.where(first, from_partner(upper, 1), upper)
    lower = jnp.where(second, from_partner(lower, 3), lower)

    owners = bag_owner[:, 0]
    onehot = (owners[:, None] == jnp.arange(DEVICES, dtype=i32)[None, :]).astype(i32)
    placed_at = jnp.sum((jnp.cumsum(onehot, axis=0) - onehot) * onehot, axis=1)
    where_to = owners * CAP + placed_at
    spot = (placed_at[:, None] == jnp.arange(CAP, dtype=i32)[None, :]).astype(f32)
    sample, feature = bag_slot // F, bag_slot % F
    bag = jnp.arange(BAGS, dtype=i32)
    pieces = [sample, feature + 1, bag // 16, bag % 16]
    parts = jnp.concatenate([spot * piece.astype(f32)[:, None] for piece in pieces], axis=1)
    coded = mxu(onehot.astype(bf16), parts.astype(bf16), ((0,), (0,))).astype(i32)
    sample_at, feature_at = coded[:, :CAP], coded[:, CAP : 2 * CAP]
    send_slots = jnp.where(feature_at > 0, (feature_at - 1) * B_DEV + sample_at, BAGS)
    send_slots = jnp.pad(send_slots, ((0, 0), (0, 128 - CAP))).reshape(DEVICES, 1, 128)
    send_bags = (coded[:, 2 * CAP : 3 * CAP] * 16 + coded[:, 3 * CAP :]).reshape(DEVICES * CAP)

    sizes = bag_sizes[0]
    ends = jnp.cumsum(sizes)
    starts = ends - sizes
    bounds = jnp.arange(LOOKS // CHUNK, dtype=i32) * CHUNK
    first_bag = jnp.sum((ends[None, :] <= bounds[:, None]).astype(i32), axis=1) // 16 * 16
    extra = C_ROWS - BAGS
    ends2 = jnp.concatenate([ends, jnp.zeros((extra,), i32)]).reshape(C_ROWS // 128, 128)
    starts2 = jnp.concatenate([starts, jnp.full((extra,), LOOKS, i32)]).reshape(C_ROWS // 128, 128)
    upper, lower, look_rows, first_bag, starts2, ends2 = lax.optimization_barrier(
        (upper, lower, look_rows, first_bag, starts2, ends2)
    )
    upper2, lower2 = from_partner(upper, 3), from_partner(lower, 1)
    counts = pl.pallas_call(
        count_kernel,
        out_shape=jax.ShapeDtypeStruct((C_ROWS, ROWS), bf16),
        in_specs=[SMEM, VMEM, VMEM, VMEM],
        out_specs=VMEM,
        scratch_shapes=[pltpu.VMEM((C_ROWS, 128), i32), pltpu.VMEM((C_ROWS, 128), i32)],
        compiler_params=params(vmem_limit_bytes=24 << 20),
        cost_estimate=pl.CostEstimate(flops=2 * LOOKS * SPAN * ROWS, bytes_accessed=10 << 20, transcendentals=0),
        name="count",
    )(first_bag, look_rows.reshape(LOOKS // 128, 128), starts2, ends2)

    dma = pltpu.SemaphoreType.DMA
    got_rows, got_slots, held = pl.pallas_call(
        pool_kernel,
        out_shape=(
            jax.ShapeDtypeStruct((DEVICES * CAP, E), f32),
            jax.ShapeDtypeStruct((DEVICES, 1, 128), i32),
            jax.ShapeDtypeStruct((ROWS, E), f32),
        ),
        in_specs=[SMEM, SMEM, VMEM, VMEM, VMEM, VMEM, VMEM, VMEM],
        out_specs=(VMEM, VMEM, VMEM),
        scratch_shapes=[
            pltpu.VMEM((ROWS, 256), bf16),
            pltpu.VMEM((BAGS, E), f32),
            pltpu.VMEM((DEVICES * CAP, E), f32),
            dma,
            dma,
            dma,
            dma,
        ],
        compiler_params=params(collective_id=0, has_side_effects=True, vmem_limit_bytes=20 << 20),
        name="pool",
    )(pair_mask, send_bags, send_slots, counts, upper, upper2, lower, lower2)
    slot_of = got_slots.reshape(DEVICES * 128)

    sums = pl.pallas_call(
        place_kernel,
        out_shape=jax.ShapeDtypeStruct((BAGS, E), f32),
        in_specs=[SMEM, VMEM],
        out_specs=VMEM,
        compiler_params=params(vmem_limit_bytes=16 << 20),
        name="place",
    )(slot_of, got_rows)

    new_table, new_state, top_grad, out_grad = pl.pallas_call(
        update_kernel,
        out_shape=(
            jax.ShapeDtypeStruct((ROWS, E), f32),
            jax.ShapeDtypeStruct((1, ROWS), f32),
            jax.ShapeDtypeStruct((INTER, HID), f32),
            jax.ShapeDtypeStruct((1, HID), f32),
        ),
        in_specs=[SMEM, SMEM, SMEM] + [VMEM] * 8,
        out_specs=(VMEM, VMEM, VMEM, VMEM),
        scratch_shapes=[
            pltpu.VMEM((DEVICES * CAP, E), f32),
            pltpu.VMEM((DEVICES * CAP, E), f32),
            pltpu.VMEM((BAGS, E), f32),
            pltpu.VMEM((2 * E, BAGS), bf16),
            pltpu.VMEM((G_ROWS, 128), f32),
            pltpu.VMEM((BAGS + 8, E), f32),
            pltpu.VMEM((INTER, B_DEV), f32),
            pltpu.VMEM((F + 1, E, B_DEV), f32),
            pltpu.VMEM((B_DEV, HID), f32),
            pltpu.VMEM((G_ROWS, 128), f32),
            pltpu.VMEM((HALF, 128), f32),
            pltpu.VMEM((HALF, 128), f32),
            pltpu.VMEM((4, 1, ROWS), f32),
            *[pltpu.VMEM((4, 4 * rows, 128), f32) for rows in PART],
            *[pltpu.VMEM((4 * rows, 128), f32) for rows in PART],
            *[pltpu.VMEM((4, rows, 128), f32) for rows in PART],
            *[pltpu.VMEM((rows, 128), f32) for rows in PART],
            *[pltpu.VMEM((4, rows, 128), f32) for rows in PART],
            dma((4,)),
            dma((4,)),
            dma,
            dma,
            dma,
            dma,
            dma,
            dma,
            dma((40,)),
            dma((40,)),
        ],
        compiler_params=params(collective_id=1, has_side_effects=True, vmem_limit_bytes=30 << 20),
        name="update",
    )(
        pair_mask,
        slot_of,
        where_to,
        sums,
        dense_vectors,
        labels[:, None],
        top_weight,
        out_weight[None, :],
        counts,
        held,
        row_state[None, :],
    )
    return new_table, new_state.reshape(ROWS), top_grad, out_grad.reshape(HID)


def solution(mesh):
    both = ("gx", "gy")
    in_specs = (
        P(both, None),
        P(both),
        P("gx"),
        P(both),
        P(both, None),
        P(both, None),
        P(both),
        P(both, None),
        P(both),
        P(),
        P(),
    )
    out_specs = (P(both, None), P(both), P(), P())
    return jax.shard_map(
        on_device, mesh=mesh, in_specs=in_specs, out_specs=out_specs, check_vma=False
    )
```

```python
import jax
import jax.numpy as jnp
from jax import lax
from jax.experimental import pallas as pl
from jax.experimental.pallas import tpu as pltpu
from jax.sharding import PartitionSpec as P

E = 128
F = 16
B_DEV = 128
BAGS = 2048
ROWS = 2048
LOOKS = 6144
DEVICES = 128
CAP = 32
INTER = 264
HID = 1024
CHUNK = 256
SPAN = CHUNK + 16
C_ROWS = 2304
G_ROWS = 2304
HALF = G_ROWS // 2
SEG = HALF // 48
STRIDE = 37
CUTS = (1, 24, 44, 64, 128)
PAIRS = [(i, j) for i in range(F + 1) for j in range(i + 1, F + 1)]
PAIR_ROW = {pair: 128 + n for n, pair in enumerate(PAIRS)}

learn_rate = 0.05
epsilon = 1e-08
MESH = pl.DeviceIdType.MESH
f32, bf16, i32 = jnp.float32, jnp.bfloat16, jnp.int32

VMEM = pl.BlockSpec(memory_space=pltpu.VMEM)
SMEM = pl.BlockSpec(memory_space=pltpu.SMEM)
ANY = pl.BlockSpec(memory_space=pl.ANY)


def split(x):
    hi = x.astype(bf16)
    return hi, (x - hi.astype(f32)).astype(bf16)


def mxu(a, b, dims):
    return lax.dot_general(a, b, (dims, ((), ())), preferred_element_type=f32)


def dot3(a, b, dims):
    return mxu(a[0], b[0], dims) + (mxu(a[0], b[1], dims) + mxu(a[1], b[0], dims))


NN = ((1,), (0,))
NT = ((1,), (1,))


def down_sublanes(row):
    return jnp.broadcast_to(row, (128, 128)).T


def count_kernel(first_ref, look_ref, start_ref, end_ref, c_ref, start_t, end_t):
    for r in range(C_ROWS // 128):
        here = slice(r * 128, (r + 1) * 128)
        start_t[here, :] = down_sublanes(start_ref[r : r + 1, :])
        end_t[here, :] = down_sublanes(end_ref[r : r + 1, :])
    c_ref[0:16, :] = jnp.zeros((16, ROWS), bf16)
    lane = lax.broadcasted_iota(i32, (1, 128), 1)

    def chunk(t, carry):
        at = pl.multiple_of(first_ref[t], 16)
        start, end = start_t[pl.ds(at, SPAN), :], end_t[pl.ds(at, SPAN), :]
        halves, columns = [], []
        for h in range(2):
            k = lane + (t * CHUNK + h * 128)
            halves.append(((start <= k) & (k < end)).astype(f32).astype(bf16))
            columns.append(down_sublanes(look_ref[pl.ds(2 * t + h, 1), :]))
        in_bag = jnp.concatenate(halves, axis=1)
        column = jnp.concatenate(columns, axis=0)
        for n in range(0, 16, 4):
            of_row = jnp.concatenate(
                [(column == lane + 128 * q).astype(f32).astype(bf16) for q in range(n, n + 4)],
                axis=1,
            )
            counts = mxu(in_bag, of_row, NN)
            cols = slice(n * 128, (n + 4) * 128)
            before = c_ref[pl.ds(at, 16), cols].astype(f32)
            c_ref[pl.ds(at, 16), cols] = (counts[:16] + before).astype(bf16)
            c_ref[pl.ds(pl.multiple_of(at + 16, 16), SPAN - 16), cols] = counts[16:].astype(bf16)
        return carry

    lax.fori_loop(0, LOOKS // CHUNK, chunk, 0, unroll=2)


def device_at(n):
    return (n // 4, n % 4)


def my_number():
    return lax.axis_index("gx") * 4 + lax.axis_index("gy")


def peer_of(k):
    return (my_number() + STRIDE * k) % DEVICES


def greet_all(barrier):
    def greet(k, carry):
        pl.semaphore_signal(barrier, inc=1, device_id=device_at(peer_of(k)), device_id_type=MESH)
        return carry

    lax.fori_loop(1, DEVICES, greet, 0)


def put(src, dst, send, recv, device):
    return pltpu.make_async_remote_copy(
        src_ref=src, dst_ref=dst, send_sem=send, recv_sem=recv, device_id=device, device_id_type=MESH
    )


def chunk_at(n):
    return pl.ds(pl.multiple_of(n * CAP, CAP), CAP)


def pick_rows(dst, to, src, index_ref, at):
    for u in range(CAP):
        dst[pl.ds(to + u, 1), :] = src[pl.ds(index_ref[at + u], 1), :]


def pool_kernel(
    mask_ref,
    bag_in,
    slots_ref,
    c_ref,
    a_ref,
    a2_ref,
    b_ref,
    b2_ref,
    recv_ref,
    got_ref,
    held_ref,
    split_ref,
    partial_ref,
    send_ref,
    row_send,
    row_recv,
    slot_send,
    slot_recv,
    bag_ref,
    bag_sem,
):
    bag_copy = pltpu.make_async_copy(bag_in, bag_ref, bag_sem)
    bag_copy.start()
    barrier = pltpu.get_barrier_semaphore()
    greet_all(barrier)
    me = my_number()
    mask = jnp.full((ROWS // 2, E), mask_ref[0], i32)
    held_ref[: ROWS // 2, :] = jnp.where(mask >= 2, a2_ref[...], a_ref[...])
    held_ref[ROWS // 2 :, :] = jnp.where((mask == 1) | (mask == 2), b2_ref[...], b_ref[...])
    hi, lo = split(held_ref[...])
    split_ref[:, :128] = hi
    split_ref[:, 128:] = lo

    def block(m, carry):
        at = pl.multiple_of(m * 256, 256)
        both = mxu(c_ref[pl.ds(at, 256), :], split_ref[...], NN)
        partial_ref[pl.ds(at, 256), :] = both[:, :128] + both[:, 128:]
        return carry

    lax.fori_loop(0, BAGS // 256, block, 0)
    got_ref[me] = slots_ref[me]
    bag_copy.wait()
    pick_rows(recv_ref, me * CAP, partial_ref, bag_ref, me * CAP)

    def ready(k):
        at = peer_of(k) * CAP
        pick_rows(send_ref, at, partial_ref, bag_ref, at)

    def start(k):
        peer = peer_of(k)
        to = device_at(peer)
        put(slots_ref.at[peer], got_ref.at[me], slot_send, slot_recv, to).start()
        put(send_ref.at[chunk_at(peer)], recv_ref.at[chunk_at(me)], row_send, row_recv, to).start()

    ready(1)
    pl.semaphore_wait(barrier, DEVICES - 1)

    def step(k, carry):
        ready(k)
        start(k - 1)
        return carry

    lax.fori_loop(2, DEVICES, step, 0)
    start(DEVICES - 1)
    to = device_at(peer_of(1))
    some = pl.ds(0, DEVICES - 1)
    put(slots_ref.at[some], got_ref.at[some], slot_send, slot_recv, to).wait()
    rows = pl.ds(0, (DEVICES - 1) * CAP)
    put(send_ref.at[rows], recv_ref.at[rows], row_send, row_recv, to).wait()


def place_kernel(slot_in, got_ref, pooled, slot_ref, sems):
    part = DEVICES * 128 // 8
    copies = []
    for q in range(8):
        here = pl.ds(q * part, part)
        copies.append(pltpu.make_async_copy(slot_in.at[here], slot_ref.at[here], sems.at[q]))
        copies[q].start()

    def place(c, carry):
        @pl.when(slot_ref[c * 128] < BAGS)
        def _():
            for u in range(CAP):
                pooled[pl.ds(slot_ref[c * 128 + u], 1), :] = got_ref[pl.ds(c * CAP + u, 1), :]

        return carry

    for q in range(8):
        copies[q].wait()
        lax.fori_loop(q * DEVICES // 8, (q + 1) * DEVICES // 8, place, 0)


def finish_kernel(a, b, c, d, to_a, to_b, to_c, to_d, sems):
    pairs = ((a, to_a), (b, to_b), (c, to_c), (d, to_d))
    copies = [pltpu.make_async_copy(x, y, sems.at[n]) for n, (x, y) in enumerate(pairs)]
    for copy in copies:
        copy.start()
    for copy in copies:
        copy.wait()


def update_kernel(
    mask_ref,
    slot_in,
    where_in,
    sums_ref,
    dense_ref,
    label_ref,
    w_ref,
    wo_ref,
    c_ref,
    table_ref,
    state_ref,
    new_table_ref,
    new_state_ref,
    top_ref,
    out_ref,
    back,
    came,
    grads,
    sides,
    fin,
    pooled,
    inter_t,
    vt,
    d_pre_ref,
    grad_ref,
    r1,
    acc,
    states,
    ra,
    part_a,
    rb,
    mine,
    rc,
    slot_ref,
    where_ref,
    table_sem,
    state_send,
    state_recv,
    row_send,
    row_recv,
    swap_send,
    swap_recv,
    last_send,
    last_recv,
    color_send,
    color_recv,
):
    tables = [
        pltpu.make_async_copy(slot_in, slot_ref, table_sem.at[0]),
        pltpu.make_async_copy(where_in, where_ref, table_sem.at[1]),
    ]
    for copy in tables:
        copy.start()
    barrier = pltpu.get_barrier_semaphore()
    greet_all(barrier)
    me = my_number()
    gx, x = lax.axis_index("gx"), lax.axis_index("gy")
    yz, core = gx // 2, gx % 2
    twin = (gx + 1 - 2 * core, x)

    y, z = yz // 4, yz % 4

    def along_x(k):
        return (gx, (x + k) % 4)

    def along_y(k):
        return (((y + k) % 4 * 4 + z) * 2 + core, x)

    def along_z(k):
        return ((y * 4 + (z + k) % 4) * 2 + core, x)

    dense_t = dense_ref[...].T
    vt[0] = dense_t
    inter_t[0:128, :] = dense_t
    for f in range(F):
        vt[f + 1] = sums_ref[f * 128 : (f + 1) * 128, :].T
    for i in range(F):
        for j in range(i + 1, F + 1):
            row = PAIR_ROW[i, j]
            inter_t[row : row + 1, :] = jnp.sum(vt[i] * vt[j], axis=0, keepdims=True)

    it = inter_t[...]
    w = split(w_ref[...])
    pre = dot3(split(it.T), w, NN)
    sig = 1.0 / (1.0 + jnp.exp(-pre))
    hidden = pre * sig
    logits = jnp.sum(hidden * wo_ref[...], axis=1, keepdims=True)
    d_logits = 1.0 / (1.0 + jnp.exp(-logits)) - label_ref[...]
    out_grad = jnp.sum(hidden * d_logits, axis=0, keepdims=True)
    for q in range(8):
        grad_ref[8 * INTER + q : 8 * INTER + q + 1, :] = out_grad[:, q * 128 : (q + 1) * 128]
    grad_ref[8 * INTER + 8 :, :] = jnp.zeros((G_ROWS - 8 * INTER - 8, 128), f32)
    d_pre_ref[...] = d_logits * wo_ref[...] * (sig * (1.0 + pre * (1.0 - sig)))
    d_pre = split(d_pre_ref[...])
    top_grad = dot3(split(it), d_pre, NN)
    for q in range(8):
        grad_ref[q * INTER : (q + 1) * INTER, :] = top_grad[:, q * 128 : (q + 1) * 128]
    inter_t[...] = dot3(w, d_pre, NT)

    def pooled_grad(j):
        total = None
        for i in range(F + 1):
            if i != j:
                row = PAIR_ROW[min(i, j), max(i, j)]
                term = inter_t[row : row + 1, :] * vt[i]
                total = term if total is None else total + term
        pooled[(j - 1) * 128 : j * 128, :] = total.T

    for j in range(1, 7):
        pooled_grad(j)

    my_half = pl.multiple_of(core * HALF, 8)
    other = pl.multiple_of((1 - core) * HALF, 8)
    pl.semaphore_wait(barrier, DEVICES - 1)
    swap = put(grad_ref.at[pl.ds(other, HALF)], r1, swap_send, swap_recv, twin)
    swap.start()
    flips = [None, x + 1 - 2 * (x % 2), (x + 2) % 4, 3 - x]
    state_moves = [
        put(state_ref, states.at[f], state_send.at[f], state_recv.at[f], (gx, flips[f]))
        for f in range(1, 4)
    ]
    for move in state_moves:
        move.start()
    for j in range(7, F + 1):
        pooled_grad(j)
    pooled[BAGS:, :] = jnp.zeros((8, E), f32)

    def ready(k):
        peer = peer_of(k)
        pick_rows(back, peer * CAP, pooled, slot_ref, peer * 128)

    def start(k):
        peer = peer_of(k)
        put(
            back.at[chunk_at(peer)], came.at[chunk_at(me)], row_send, row_recv, device_at(peer)
        ).start()

    def send_rows(n):
        def step(k, carry):
            ready(k + 1)
            start(k)
            return carry

        last = DEVICES - 1 if CUTS[n + 1] == DEVICES else CUTS[n + 1]
        lax.fori_loop(CUTS[n], last, step, 0)
        if last < CUTS[n + 1]:
            start(last)

    class Color:
        def __init__(self, n, at, to):
            self.n, self.at = n, at
            self.to = (to[0], to[1], to[2], to[1], to[0])
            self.base = n * 16 * SEG

        def move(self, phase, k, src, dst):
            sem = (self.n * 5 + phase) * 4 + k
            return put(src, dst, color_send.at[sem], color_recv.at[sem], self.to[phase](k))

        def rows_a(self, a, base):
            return pl.ds(pl.multiple_of(base + self.base + a * (4 * SEG), 8), 4 * SEG)

        def rows_b(self, a, b, base):
            return pl.ds(pl.multiple_of(base + self.base + (a * 4 + b) * SEG, 8), SEG)

        def moves(self, phase, waiting):
            n = self.n
            a, b, c = self.at
            out = []
            for k in range(1, 4):
                if phase == 0:
                    there = acc.at[self.rows_a((a + k) % 4, 0)]
                    out.append(self.move(0, k, there, ra.at[4 * n + k]))
                if phase == 1:
                    there = pl.ds(pl.multiple_of((b + k) % 4 * SEG, 8), SEG)
                    out.append(self.move(1, k, part_a.at[n, there], rb.at[4 * n + k]))
                if phase == 2:
                    slot = (c + 4 - k) % 4 if waiting else c
                    out.append(self.move(2, k, mine.at[n], rc.at[4 * n + slot]))
                if phase == 3:
                    who = (b + 4 - k) % 4 if waiting else b
                    there = fin.at[self.rows_b(a, who, my_half)]
                    out.append(self.move(3, k, there, there))
                if phase == 4:
                    who = (a + 4 - k) % 4 if waiting else a
                    there = fin.at[self.rows_a(who, my_half)]
                    out.append(self.move(4, k, there, there))
            return out

        def begin(self, phase):
            for copy in self.moves(phase, False):
                copy.start()

        def finish(self, phase):
            for copy in self.moves(phase, False):
                copy.wait_send()
            for copy in self.moves(phase, True):
                copy.wait_recv()
            n = self.n
            a, b, c = self.at
            if phase == 0:
                own = acc[self.rows_a(a, 0), :]
                part_a[n] = (own + ra[4 * n + 1]) + (ra[4 * n + 2] + ra[4 * n + 3])
            if phase == 1:
                own = part_a[n, pl.ds(pl.multiple_of(b * SEG, 8), SEG), :]
                part = (own + rb[4 * n + 1]) + (rb[4 * n + 2] + rb[4 * n + 3])
                mine[n] = part
                rc[4 * n + c] = part
            if phase == 2:
                whole = (rc[4 * n] + rc[4 * n + 1]) + (rc[4 * n + 2] + rc[4 * n + 3])
                fin[self.rows_b(a, b, my_half), :] = whole

    colors = (
        Color(0, (z, y, x), (along_z, along_y, along_x)),
        Color(1, (y, x, z), (along_y, along_x, along_z)),
        Color(2, (x, z, y), (along_x, along_z, along_y)),
    )

    def phase_on(phase):
        for color in colors:
            color.begin(phase)

    def phase_off(phase):
        for color in colors:
            color.finish(phase)

    swap.wait()
    acc[...] = grad_ref[pl.ds(my_half, HALF), :] + r1[...]
    phase_on(0)
    tables[0].wait()
    pick_rows(came, me * CAP, pooled, slot_ref, me * 128)
    ready(1)
    for phase in range(4):
        send_rows(phase)
        phase_off(phase)
        phase_on(phase + 1)

    rows = pl.ds(0, (DEVICES - 1) * CAP)
    put(back.at[rows], came.at[rows], row_send, row_recv, device_at(peer_of(1))).wait()
    tables[1].wait()
    for move in state_moves:
        move.wait()
    mask = jnp.full((1, ROWS), mask_ref[0], i32)
    held_state = state_ref[...]
    for f in range(1, 4):
        held_state = jnp.where(mask == f, states[f], held_state)
    states[0] = held_state

    def take(n, carry):
        for u in range(16):
            b = n * 16 + u
            grads[pl.ds(b, 1), :] = came[pl.ds(where_ref[b], 1), :]
        return carry

    lax.fori_loop(0, BAGS // 16, take, 0)
    for q in range(BAGS // 128):
        here = slice(q * 128, (q + 1) * 128)
        hi, lo = split(grads[here, :].T)
        sides[0:128, here] = hi
        sides[128:256, here] = lo

    phase_off(4)
    half = fin.at[pl.ds(my_half, HALF)]
    rest = fin.at[pl.ds(other, HALF)]
    last = put(half, half, last_send, last_recv, twin)
    last.start()

    def block(n, carry):
        here = pl.ds(pl.multiple_of(n * 256, 256), 256)
        both = mxu(sides[...], c_ref[0:BAGS, here], NN)
        row_grad = both[:128] + both[128:]
        state = states[0, :, here] + jnp.sum(row_grad * row_grad, axis=0, keepdims=True) * (1.0 / E)
        new_state_ref[:, here] = state
        step = row_grad * (learn_rate / (jnp.sqrt(state) + epsilon))
        new_table_ref[here, :] = table_ref[here, :] - step.T
        return carry

    lax.fori_loop(0, ROWS // 256, block, 0)

    last.wait_send()
    put(rest, rest, last_send, last_recv, twin).wait_recv()
    for q in range(8):
        top_ref[:, q * 128 : (q + 1) * 128] = fin[q * INTER : (q + 1) * INTER, :]
        out_ref[:, q * 128 : (q + 1) * 128] = fin[8 * INTER + q : 8 * INTER + q + 1, :]


def params(**kw):
    return pltpu.CompilerParams(**kw)


def from_partner(block, flip):
    return lax.ppermute(block, "gy", [(y, y ^ flip) for y in range(4)])


def on_device(
    emb_table,
    row_state,
    pair_mask,
    look_rows,
    bag_sizes,
    bag_owner,
    bag_slot,
    dense_vectors,
    labels,
    top_weight,
    out_weight,
):
    mask = pair_mask[0]
    first, second = (mask == 1) | (mask == 2), mask >= 2
    upper, lower = emb_table[: ROWS // 2], emb_table[ROWS // 2 :]
    upper = jnp.where(first, from_partner(upper, 1), upper)
    lower = jnp.where(second, from_partner(lower, 3), lower)

    owners = bag_owner[:, 0]
    onehot = (owners[:, None] == jnp.arange(DEVICES, dtype=i32)[None, :]).astype(i32)
    placed_at = jnp.sum((jnp.cumsum(onehot, axis=0) - onehot) * onehot, axis=1)
    where_to = owners * CAP + placed_at
    spot = (placed_at[:, None] == jnp.arange(CAP, dtype=i32)[None, :]).astype(f32)
    sample, feature = bag_slot // F, bag_slot % F
    bag = jnp.arange(BAGS, dtype=i32)
    pieces = [sample, feature + 1, bag // 16, bag % 16]
    parts = jnp.concatenate([spot * piece.astype(f32)[:, None] for piece in pieces], axis=1)
    coded = mxu(onehot.astype(bf16), parts.astype(bf16), ((0,), (0,))).astype(i32)
    sample_at, feature_at = coded[:, :CAP], coded[:, CAP : 2 * CAP]
    send_slots = jnp.where(feature_at > 0, (feature_at - 1) * B_DEV + sample_at, BAGS)
    send_slots = jnp.pad(send_slots, ((0, 0), (0, 128 - CAP))).reshape(DEVICES, 1, 128)
    send_bags = (coded[:, 2 * CAP : 3 * CAP] * 16 + coded[:, 3 * CAP :]).reshape(DEVICES * CAP)

    sizes = bag_sizes[0]
    ends = jnp.cumsum(sizes)
    starts = ends - sizes
    bounds = jnp.arange(LOOKS // CHUNK, dtype=i32) * CHUNK
    first_bag = jnp.sum((ends[None, :] <= bounds[:, None]).astype(i32), axis=1) // 16 * 16
    extra = C_ROWS - BAGS
    ends2 = jnp.concatenate([ends, jnp.zeros((extra,), i32)]).reshape(C_ROWS // 128, 128)
    starts2 = jnp.concatenate([starts, jnp.full((extra,), LOOKS, i32)]).reshape(C_ROWS // 128, 128)
    upper, lower, look_rows, first_bag, starts2, ends2 = lax.optimization_barrier(
        (upper, lower, look_rows, first_bag, starts2, ends2)
    )
    upper2, lower2 = from_partner(upper, 3), from_partner(lower, 1)
    counts = pl.pallas_call(
        count_kernel,
        out_shape=jax.ShapeDtypeStruct((C_ROWS, ROWS), bf16),
        in_specs=[SMEM, VMEM, VMEM, VMEM],
        out_specs=VMEM,
        scratch_shapes=[pltpu.VMEM((C_ROWS, 128), i32), pltpu.VMEM((C_ROWS, 128), i32)],
        compiler_params=params(vmem_limit_bytes=24 << 20),
        cost_estimate=pl.CostEstimate(flops=2 * LOOKS * SPAN * ROWS, bytes_accessed=10 << 20, transcendentals=0),
        name="count",
    )(first_bag, look_rows.reshape(LOOKS // 128, 128), starts2, ends2)

    dma = pltpu.SemaphoreType.DMA
    got_rows, got_slots, held = pl.pallas_call(
        pool_kernel,
        out_shape=(
            jax.ShapeDtypeStruct((DEVICES * CAP, E), f32),
            jax.ShapeDtypeStruct((DEVICES, 1, 128), i32),
            jax.ShapeDtypeStruct((ROWS, E), f32),
        ),
        in_specs=[SMEM, ANY, VMEM, VMEM, VMEM, VMEM, VMEM, VMEM],
        out_specs=(VMEM, VMEM, VMEM),
        scratch_shapes=[
            pltpu.VMEM((ROWS, 256), bf16),
            pltpu.VMEM((BAGS, E), f32),
            pltpu.VMEM((DEVICES * CAP, E), f32),
            dma,
            dma,
            dma,
            dma,
            pltpu.SMEM((DEVICES * CAP,), i32),
            dma,
        ],
        compiler_params=params(collective_id=0, has_side_effects=True, vmem_limit_bytes=20 << 20),
        name="pool",
    )(pair_mask, send_bags, send_slots, counts, upper, upper2, lower, lower2)
    slot_of = got_slots.reshape(DEVICES * 128)

    sums = pl.pallas_call(
        place_kernel,
        out_shape=jax.ShapeDtypeStruct((BAGS, E), f32),
        in_specs=[ANY, VMEM],
        out_specs=VMEM,
        scratch_shapes=[pltpu.SMEM((DEVICES * 128,), i32), dma((8,))],
        compiler_params=params(vmem_limit_bytes=16 << 20),
        name="place",
    )(slot_of, got_rows)

    results = pl.pallas_call(
        update_kernel,
        out_shape=(
            jax.ShapeDtypeStruct((ROWS, E), f32),
            jax.ShapeDtypeStruct((1, ROWS), f32),
            jax.ShapeDtypeStruct((INTER, HID), f32),
            jax.ShapeDtypeStruct((1, HID), f32),
        ),
        in_specs=[SMEM, ANY, ANY] + [VMEM] * 8,
        out_specs=(VMEM, VMEM, VMEM, VMEM),
        scratch_shapes=[
            pltpu.VMEM((DEVICES * CAP, E), f32),
            pltpu.VMEM((DEVICES * CAP, E), f32),
            pltpu.VMEM((BAGS, E), f32),
            pltpu.VMEM((2 * E, BAGS), bf16),
            pltpu.VMEM((G_ROWS, 128), f32),
            pltpu.VMEM((BAGS + 8, E), f32),
            pltpu.VMEM((INTER, B_DEV), f32),
            pltpu.VMEM((F + 1, E, B_DEV), f32),
            pltpu.VMEM((B_DEV, HID), f32),
            pltpu.VMEM((G_ROWS, 128), f32),
            pltpu.VMEM((HALF, 128), f32),
            pltpu.VMEM((HALF, 128), f32),
            pltpu.VMEM((4, 1, ROWS), f32),
            pltpu.VMEM((12, 4 * SEG, 128), f32),
            pltpu.VMEM((3, 4 * SEG, 128), f32),
            pltpu.VMEM((12, SEG, 128), f32),
            pltpu.VMEM((3, SEG, 128), f32),
            pltpu.VMEM((12, SEG, 128), f32),
            pltpu.SMEM((DEVICES * 128,), i32),
            pltpu.SMEM((BAGS,), i32),
            dma((2,)),
            dma((4,)),
            dma((4,)),
            dma,
            dma,
            dma,
            dma,
            dma,
            dma,
            dma((60,)),
            dma((60,)),
        ],
        compiler_params=params(collective_id=1, has_side_effects=True, vmem_limit_bytes=30 << 20),
        name="update",
    )(
        pair_mask,
        slot_of,
        where_to,
        sums,
        dense_vectors,
        labels[:, None],
        top_weight,
        out_weight[None, :],
        counts,
        held,
        row_state[None, :],
    )
    new_table, new_state, top_grad, out_grad = pl.pallas_call(
        finish_kernel,
        out_shape=tuple(jax.ShapeDtypeStruct(r.shape, f32) for r in results),
        in_specs=[ANY] * 4,
        out_specs=(ANY,) * 4,
        scratch_shapes=[dma((4,))],
        compiler_params=params(vmem_limit_bytes=16 << 20),
        name="finish",
    )(*results)
    return new_table, new_state.reshape(ROWS), top_grad, out_grad.reshape(HID)


def solution(mesh):
    both = ("gx", "gy")
    in_specs = (
        P(both, None),
        P(both),
        P("gx"),
        P(both),
        P(both, None),
        P(both, None),
        P(both),
        P(both, None),
        P(both),
        P(),
        P(),
    )
    out_specs = (P(both, None), P(both), P(), P())
    return jax.shard_map(
        on_device, mesh=mesh, in_specs=in_specs, out_specs=out_specs, check_vma=False
    )
```

```python
import jax
import jax.numpy as jnp
from jax import lax
from jax.experimental import pallas as pl
from jax.experimental.pallas import tpu as pltpu
from jax.sharding import PartitionSpec as P

E = 128
F = 16
B_DEV = 128
BAGS = 2048
ROWS = 2048
LOOKS = 6144
DEVICES = 128
CAP = 32
INTER = 264
HID = 1024
CHUNK = 256
SPAN = CHUNK + 16
C_ROWS = 2304
G_ROWS = 2304
HALF = G_ROWS // 2
SEG = HALF // 48
STRIDE = 37
CUTS = (0, 4, 7, 9, 27)
PAIRS = [(i, j) for i in range(F + 1) for j in range(i + 1, F + 1)]
PAIR_ROW = {pair: 128 + n for n, pair in enumerate(PAIRS)}

learn_rate = 0.05
epsilon = 1e-08
MESH = pl.DeviceIdType.MESH
f32, bf16, i32 = jnp.float32, jnp.bfloat16, jnp.int32

VMEM = pl.BlockSpec(memory_space=pltpu.VMEM)
SMEM = pl.BlockSpec(memory_space=pltpu.SMEM)
ANY = pl.BlockSpec(memory_space=pl.ANY)


def split(x):
    hi = x.astype(bf16)
    return hi, (x - hi.astype(f32)).astype(bf16)


def mxu(a, b, dims):
    return lax.dot_general(a, b, (dims, ((), ())), preferred_element_type=f32)


def dot3(a, b, dims):
    return mxu(a[0], b[0], dims) + (mxu(a[0], b[1], dims) + mxu(a[1], b[0], dims))


NN = ((1,), (0,))
NT = ((1,), (1,))


def down_sublanes(row):
    return jnp.broadcast_to(row, (128, 128)).T


def count_kernel(first_ref, look_ref, start_ref, end_ref, c_ref, start_t, end_t):
    for r in range(C_ROWS // 128):
        here = slice(r * 128, (r + 1) * 128)
        start_t[here, :] = down_sublanes(start_ref[r : r + 1, :])
        end_t[here, :] = down_sublanes(end_ref[r : r + 1, :])
    c_ref[0:16, :] = jnp.zeros((16, ROWS), bf16)
    lane = lax.broadcasted_iota(i32, (1, 128), 1)

    def chunk(t, carry):
        at = pl.multiple_of(first_ref[t], 16)
        start, end = start_t[pl.ds(at, SPAN), :], end_t[pl.ds(at, SPAN), :]
        halves, columns = [], []
        for h in range(2):
            k = lane + (t * CHUNK + h * 128)
            halves.append(((start <= k) & (k < end)).astype(f32).astype(bf16))
            columns.append(down_sublanes(look_ref[pl.ds(2 * t + h, 1), :]))
        in_bag = jnp.concatenate(halves, axis=1)
        column = jnp.concatenate(columns, axis=0)
        for n in range(0, 16, 4):
            of_row = jnp.concatenate(
                [(column == lane + 128 * q).astype(f32).astype(bf16) for q in range(n, n + 4)],
                axis=1,
            )
            counts = mxu(in_bag, of_row, NN)
            cols = slice(n * 128, (n + 4) * 128)
            before = c_ref[pl.ds(at, 16), cols].astype(f32)
            c_ref[pl.ds(at, 16), cols] = (counts[:16] + before).astype(bf16)
            c_ref[pl.ds(pl.multiple_of(at + 16, 16), SPAN - 16), cols] = counts[16:].astype(bf16)
        return carry

    lax.fori_loop(0, LOOKS // CHUNK, chunk, 0, unroll=2)


def device_at(n):
    return (n // 4, n % 4)


def my_number():
    return lax.axis_index("gx") * 4 + lax.axis_index("gy")


def peer_of(k):
    return (my_number() + STRIDE * k) % DEVICES


def greet_all(barrier):
    def greet(k, carry):
        pl.semaphore_signal(barrier, inc=1, device_id=device_at(peer_of(k)), device_id_type=MESH)
        return carry

    lax.fori_loop(1, DEVICES, greet, 0)


def put(src, dst, send, recv, device):
    return pltpu.make_async_remote_copy(
        src_ref=src, dst_ref=dst, send_sem=send, recv_sem=recv, device_id=device, device_id_type=MESH
    )


def distance(kind):
    return sum(kind)


KINDS = sorted(
    ((dx, dy, dz) for dx in (2, 1, 0) for dy in (2, 1, 0) for dz in (2, 1, 0)),
    key=lambda kind: -distance(kind),
)


def steps_of(kind):
    return 2 * 2 ** kind.count(1) if distance(kind) else 1


def peer_in(kind, j):
    gx = lax.axis_index("gx")
    at = [lax.axis_index("gy"), gx // 8, gx // 2 % 4]
    core, rest = (1, 0) if distance(kind) == 0 else (j % 2, j // 2)
    there = []
    for here, far in zip(at, kind):
        if far == 1:
            far, rest = 1 + 2 * (rest % 2), rest // 2
        there.append((here + far) % 4)
    x, y, z = there
    return ((y * 4 + z) * 2 + (gx + core) % 2) * 4 + x


def send_kinds(kinds, ready, start, waiting):
    for kind in kinds:
        count = steps_of(kind)
        ready(peer_in(kind, 0))
        if waiting is not None:
            start(waiting)

        def step(j, carry, kind=kind):
            ready(peer_in(kind, j))
            start(peer_in(kind, j - 1))
            return carry

        if count > 1:
            lax.fori_loop(1, count, step, 0)
        waiting = peer_in(kind, count - 1)
    return waiting


def chunk_at(n):
    return pl.ds(pl.multiple_of(n * CAP, CAP), CAP)


def pick_rows(dst, to, src, index_ref, at):
    for u in range(CAP):
        dst[pl.ds(to + u, 1), :] = src[pl.ds(index_ref[at + u], 1), :]


def pool_kernel(
    mask_ref,
    bag_in,
    slots_ref,
    c_ref,
    a_ref,
    a2_ref,
    b_ref,
    b2_ref,
    recv_ref,
    got_ref,
    held_ref,
    split_ref,
    partial_ref,
    send_ref,
    row_send,
    row_recv,
    slot_send,
    slot_recv,
    bag_ref,
    bag_sem,
):
    bag_copy = pltpu.make_async_copy(bag_in, bag_ref, bag_sem)
    bag_copy.start()
    barrier = pltpu.get_barrier_semaphore()
    greet_all(barrier)
    me = my_number()
    mask = jnp.full((ROWS // 2, E), mask_ref[0], i32)
    held_ref[: ROWS // 2, :] = jnp.where(mask >= 2, a2_ref[...], a_ref[...])
    held_ref[ROWS // 2 :, :] = jnp.where((mask == 1) | (mask == 2), b2_ref[...], b_ref[...])
    hi, lo = split(held_ref[...])
    split_ref[:, :128] = hi
    split_ref[:, 128:] = lo

    def block(m, carry):
        at = pl.multiple_of(m * 256, 256)
        both = mxu(c_ref[pl.ds(at, 256), :], split_ref[...], NN)
        partial_ref[pl.ds(at, 256), :] = both[:, :128] + both[:, 128:]
        return carry

    lax.fori_loop(0, BAGS // 256, block, 0)
    got_ref[me] = slots_ref[me]
    bag_copy.wait()
    pick_rows(recv_ref, me * CAP, partial_ref, bag_ref, me * CAP)

    def ready(peer):
        pick_rows(send_ref, peer * CAP, partial_ref, bag_ref, peer * CAP)

    def start(peer):
        to = device_at(peer)
        put(slots_ref.at[peer], got_ref.at[me], slot_send, slot_recv, to).start()
        put(send_ref.at[chunk_at(peer)], recv_ref.at[chunk_at(me)], row_send, row_recv, to).start()

    pl.semaphore_wait(barrier, DEVICES - 1)
    start(send_kinds(KINDS, ready, start, None))
    to = device_at(peer_of(1))
    some = pl.ds(0, DEVICES - 1)
    put(slots_ref.at[some], got_ref.at[some], slot_send, slot_recv, to).wait()
    rows = pl.ds(0, (DEVICES - 1) * CAP)
    put(send_ref.at[rows], recv_ref.at[rows], row_send, row_recv, to).wait()


def place_kernel(slot_in, got_ref, pooled, slot_ref, sems):
    part = DEVICES * 128 // 8
    copies = []
    for q in range(8):
        here = pl.ds(q * part, part)
        copies.append(pltpu.make_async_copy(slot_in.at[here], slot_ref.at[here], sems.at[q]))
        copies[q].start()

    def place(c, carry):
        @pl.when(slot_ref[c * 128] < BAGS)
        def _():
            for u in range(CAP):
                pooled[pl.ds(slot_ref[c * 128 + u], 1), :] = got_ref[pl.ds(c * CAP + u, 1), :]

        return carry

    for q in range(8):
        copies[q].wait()
        lax.fori_loop(q * DEVICES // 8, (q + 1) * DEVICES // 8, place, 0)


def finish_kernel(a, b, c, d, to_a, to_b, to_c, to_d, sems):
    pairs = ((a, to_a), (b, to_b), (c, to_c), (d, to_d))
    copies = [pltpu.make_async_copy(x, y, sems.at[n]) for n, (x, y) in enumerate(pairs)]
    for copy in copies:
        copy.start()
    for copy in copies:
        copy.wait()


def update_kernel(
    mask_ref,
    slot_in,
    where_in,
    sums_ref,
    dense_ref,
    label_ref,
    w_ref,
    wo_ref,
    c_ref,
    table_ref,
    state_ref,
    new_table_ref,
    new_state_ref,
    top_ref,
    out_ref,
    back,
    came,
    grads,
    sides,
    fin,
    pooled,
    inter_t,
    vt,
    d_pre_ref,
    grad_ref,
    r1,
    acc,
    states,
    ra,
    part_a,
    rb,
    mine,
    rc,
    slot_ref,
    where_ref,
    table_sem,
    state_send,
    state_recv,
    row_send,
    row_recv,
    swap_send,
    swap_recv,
    last_send,
    last_recv,
    color_send,
    color_recv,
):
    tables = [
        pltpu.make_async_copy(slot_in, slot_ref, table_sem.at[0]),
        pltpu.make_async_copy(where_in, where_ref, table_sem.at[1]),
    ]
    for copy in tables:
        copy.start()
    barrier = pltpu.get_barrier_semaphore()
    greet_all(barrier)
    me = my_number()
    gx, x = lax.axis_index("gx"), lax.axis_index("gy")
    yz, core = gx // 2, gx % 2
    twin = (gx + 1 - 2 * core, x)

    y, z = yz // 4, yz % 4

    def along_x(k):
        return (gx, (x + k) % 4)

    def along_y(k):
        return (((y + k) % 4 * 4 + z) * 2 + core, x)

    def along_z(k):
        return ((y * 4 + (z + k) % 4) * 2 + core, x)

    dense_t = dense_ref[...].T
    vt[0] = dense_t
    inter_t[0:128, :] = dense_t
    for f in range(F):
        vt[f + 1] = sums_ref[f * 128 : (f + 1) * 128, :].T
    for i in range(F):
        for j in range(i + 1, F + 1):
            row = PAIR_ROW[i, j]
            inter_t[row : row + 1, :] = jnp.sum(vt[i] * vt[j], axis=0, keepdims=True)

    it = inter_t[...]
    w = split(w_ref[...])
    pre = dot3(split(it.T), w, NN)
    sig = 1.0 / (1.0 + jnp.exp(-pre))
    hidden = pre * sig
    logits = jnp.sum(hidden * wo_ref[...], axis=1, keepdims=True)
    d_logits = 1.0 / (1.0 + jnp.exp(-logits)) - label_ref[...]
    out_grad = jnp.sum(hidden * d_logits, axis=0, keepdims=True)
    for q in range(8):
        grad_ref[8 * INTER + q : 8 * INTER + q + 1, :] = out_grad[:, q * 128 : (q + 1) * 128]
    grad_ref[8 * INTER + 8 :, :] = jnp.zeros((G_ROWS - 8 * INTER - 8, 128), f32)
    d_pre_ref[...] = d_logits * wo_ref[...] * (sig * (1.0 + pre * (1.0 - sig)))
    d_pre = split(d_pre_ref[...])
    top_grad = dot3(split(it), d_pre, NN)
    for q in range(8):
        grad_ref[q * INTER : (q + 1) * INTER, :] = top_grad[:, q * 128 : (q + 1) * 128]
    inter_t[...] = dot3(w, d_pre, NT)

    def pooled_grad(j):
        total = None
        for i in range(F + 1):
            if i != j:
                row = PAIR_ROW[min(i, j), max(i, j)]
                term = inter_t[row : row + 1, :] * vt[i]
                total = term if total is None else total + term
        pooled[(j - 1) * 128 : j * 128, :] = total.T

    for j in range(1, 7):
        pooled_grad(j)

    my_half = pl.multiple_of(core * HALF, 8)
    other = pl.multiple_of((1 - core) * HALF, 8)
    pl.semaphore_wait(barrier, DEVICES - 1)
    swap = put(grad_ref.at[pl.ds(other, HALF)], r1, swap_send, swap_recv, twin)
    swap.start()
    flips = [None, x + 1 - 2 * (x % 2), (x + 2) % 4, 3 - x]
    state_moves = [
        put(state_ref, states.at[f], state_send.at[f], state_recv.at[f], (gx, flips[f]))
        for f in range(1, 4)
    ]
    for move in state_moves:
        move.start()
    for j in range(7, F + 1):
        pooled_grad(j)
    pooled[BAGS:, :] = jnp.zeros((8, E), f32)

    def ready(peer):
        pick_rows(back, peer * CAP, pooled, slot_ref, peer * 128)

    def start(peer):
        put(
            back.at[chunk_at(peer)], came.at[chunk_at(me)], row_send, row_recv, device_at(peer)
        ).start()

    class Color:
        def __init__(self, n, at, to):
            self.n, self.at = n, at
            self.to = (to[0], to[1], to[2], to[1], to[0])
            self.base = n * 16 * SEG

        def move(self, phase, k, src, dst):
            sem = (self.n * 5 + phase) * 4 + k
            return put(src, dst, color_send.at[sem], color_recv.at[sem], self.to[phase](k))

        def rows_a(self, a, base):
            return pl.ds(pl.multiple_of(base + self.base + a * (4 * SEG), 8), 4 * SEG)

        def rows_b(self, a, b, base):
            return pl.ds(pl.multiple_of(base + self.base + (a * 4 + b) * SEG, 8), SEG)

        def moves(self, phase, waiting):
            n = self.n
            a, b, c = self.at
            out = []
            for k in range(1, 4):
                if phase == 0:
                    there = acc.at[self.rows_a((a + k) % 4, 0)]
                    out.append(self.move(0, k, there, ra.at[4 * n + k]))
                if phase == 1:
                    there = pl.ds(pl.multiple_of((b + k) % 4 * SEG, 8), SEG)
                    out.append(self.move(1, k, part_a.at[n, there], rb.at[4 * n + k]))
                if phase == 2:
                    slot = (c + 4 - k) % 4 if waiting else c
                    out.append(self.move(2, k, mine.at[n], rc.at[4 * n + slot]))
                if phase == 3:
                    who = (b + 4 - k) % 4 if waiting else b
                    there = fin.at[self.rows_b(a, who, my_half)]
                    out.append(self.move(3, k, there, there))
                if phase == 4:
                    who = (a + 4 - k) % 4 if waiting else a
                    there = fin.at[self.rows_a(who, my_half)]
                    out.append(self.move(4, k, there, there))
            return out

        def begin(self, phase):
            for copy in self.moves(phase, False):
                copy.start()

        def finish(self, phase):
            for copy in self.moves(phase, False):
                copy.wait_send()
            for copy in self.moves(phase, True):
                copy.wait_recv()
            n = self.n
            a, b, c = self.at
            if phase == 0:
                own = acc[self.rows_a(a, 0), :]
                part_a[n] = (own + ra[4 * n + 1]) + (ra[4 * n + 2] + ra[4 * n + 3])
            if phase == 1:
                own = part_a[n, pl.ds(pl.multiple_of(b * SEG, 8), SEG), :]
                part = (own + rb[4 * n + 1]) + (rb[4 * n + 2] + rb[4 * n + 3])
                mine[n] = part
                rc[4 * n + c] = part
            if phase == 2:
                whole = (rc[4 * n] + rc[4 * n + 1]) + (rc[4 * n + 2] + rc[4 * n + 3])
                fin[self.rows_b(a, b, my_half), :] = whole

    colors = (
        Color(0, (z, y, x), (along_z, along_y, along_x)),
        Color(1, (y, x, z), (along_y, along_x, along_z)),
        Color(2, (x, z, y), (along_x, along_z, along_y)),
    )

    def phase_on(phase):
        for color in colors:
            color.begin(phase)

    def phase_off(phase):
        for color in colors:
            color.finish(phase)

    swap.wait()
    acc[...] = grad_ref[pl.ds(my_half, HALF), :] + r1[...]
    phase_on(0)
    tables[0].wait()
    pick_rows(came, me * CAP, pooled, slot_ref, me * 128)
    waiting = None
    for phase in range(4):
        waiting = send_kinds(KINDS[CUTS[phase] : CUTS[phase + 1]], ready, start, waiting)
        if phase == 3:
            start(waiting)
        phase_off(phase)
        phase_on(phase + 1)

    rows = pl.ds(0, (DEVICES - 1) * CAP)
    put(back.at[rows], came.at[rows], row_send, row_recv, device_at(peer_of(1))).wait()
    tables[1].wait()
    for move in state_moves:
        move.wait()
    mask = jnp.full((1, ROWS), mask_ref[0], i32)
    held_state = state_ref[...]
    for f in range(1, 4):
        held_state = jnp.where(mask == f, states[f], held_state)
    states[0] = held_state

    def take(n, carry):
        for u in range(16):
            b = n * 16 + u
            grads[pl.ds(b, 1), :] = came[pl.ds(where_ref[b], 1), :]
        return carry

    lax.fori_loop(0, BAGS // 16, take, 0)
    for q in range(BAGS // 128):
        here = slice(q * 128, (q + 1) * 128)
        hi, lo = split(grads[here, :].T)
        sides[0:128, here] = hi
        sides[128:256, here] = lo

    phase_off(4)
    half = fin.at[pl.ds(my_half, HALF)]
    rest = fin.at[pl.ds(other, HALF)]
    last = put(half, half, last_send, last_recv, twin)
    last.start()

    def block(n, carry):
        here = pl.ds(pl.multiple_of(n * 256, 256), 256)
        both = mxu(sides[...], c_ref[0:BAGS, here], NN)
        row_grad = both[:128] + both[128:]
        state = states[0, :, here] + jnp.sum(row_grad * row_grad, axis=0, keepdims=True) * (1.0 / E)
        new_state_ref[:, here] = state
        step = row_grad * (learn_rate / (jnp.sqrt(state) + epsilon))
        new_table_ref[here, :] = table_ref[here, :] - step.T
        return carry

    lax.fori_loop(0, ROWS // 256, block, 0)

    last.wait_send()
    put(rest, rest, last_send, last_recv, twin).wait_recv()
    for q in range(8):
        top_ref[:, q * 128 : (q + 1) * 128] = fin[q * INTER : (q + 1) * INTER, :]
        out_ref[:, q * 128 : (q + 1) * 128] = fin[8 * INTER + q : 8 * INTER + q + 1, :]


def params(**kw):
    return pltpu.CompilerParams(**kw)


def from_partner(block, flip):
    return lax.ppermute(block, "gy", [(y, y ^ flip) for y in range(4)])


def on_device(
    emb_table,
    row_state,
    pair_mask,
    look_rows,
    bag_sizes,
    bag_owner,
    bag_slot,
    dense_vectors,
    labels,
    top_weight,
    out_weight,
):
    mask = pair_mask[0]
    first, second = (mask == 1) | (mask == 2), mask >= 2
    upper, lower = emb_table[: ROWS // 2], emb_table[ROWS // 2 :]
    upper = jnp.where(first, from_partner(upper, 1), upper)
    lower = jnp.where(second, from_partner(lower, 3), lower)

    owners = bag_owner[:, 0]
    onehot = (owners[:, None] == jnp.arange(DEVICES, dtype=i32)[None, :]).astype(i32)
    placed_at = jnp.sum((jnp.cumsum(onehot, axis=0) - onehot) * onehot, axis=1)
    where_to = owners * CAP + placed_at
    spot = (placed_at[:, None] == jnp.arange(CAP, dtype=i32)[None, :]).astype(f32)
    sample, feature = bag_slot // F, bag_slot % F
    bag = jnp.arange(BAGS, dtype=i32)
    pieces = [sample, feature + 1, bag // 16, bag % 16]
    parts = jnp.concatenate([spot * piece.astype(f32)[:, None] for piece in pieces], axis=1)
    coded = mxu(onehot.astype(bf16), parts.astype(bf16), ((0,), (0,))).astype(i32)
    sample_at, feature_at = coded[:, :CAP], coded[:, CAP : 2 * CAP]
    send_slots = jnp.where(feature_at > 0, (feature_at - 1) * B_DEV + sample_at, BAGS)
    send_slots = jnp.pad(send_slots, ((0, 0), (0, 128 - CAP))).reshape(DEVICES, 1, 128)
    send_bags = (coded[:, 2 * CAP : 3 * CAP] * 16 + coded[:, 3 * CAP :]).reshape(DEVICES * CAP)

    sizes = bag_sizes[0]
    ends = jnp.cumsum(sizes)
    starts = ends - sizes
    bounds = jnp.arange(LOOKS // CHUNK, dtype=i32) * CHUNK
    first_bag = jnp.sum((ends[None, :] <= bounds[:, None]).astype(i32), axis=1) // 16 * 16
    extra = C_ROWS - BAGS
    ends2 = jnp.concatenate([ends, jnp.zeros((extra,), i32)]).reshape(C_ROWS // 128, 128)
    starts2 = jnp.concatenate([starts, jnp.full((extra,), LOOKS, i32)]).reshape(C_ROWS // 128, 128)
    upper, lower, look_rows, first_bag, starts2, ends2 = lax.optimization_barrier(
        (upper, lower, look_rows, first_bag, starts2, ends2)
    )
    upper2, lower2 = from_partner(upper, 3), from_partner(lower, 1)
    counts = pl.pallas_call(
        count_kernel,
        out_shape=jax.ShapeDtypeStruct((C_ROWS, ROWS), bf16),
        in_specs=[SMEM, VMEM, VMEM, VMEM],
        out_specs=VMEM,
        scratch_shapes=[pltpu.VMEM((C_ROWS, 128), i32), pltpu.VMEM((C_ROWS, 128), i32)],
        compiler_params=params(vmem_limit_bytes=24 << 20),
        cost_estimate=pl.CostEstimate(flops=2 * LOOKS * SPAN * ROWS, bytes_accessed=10 << 20, transcendentals=0),
        name="count",
    )(first_bag, look_rows.reshape(LOOKS // 128, 128), starts2, ends2)

    dma = pltpu.SemaphoreType.DMA
    got_rows, got_slots, held = pl.pallas_call(
        pool_kernel,
        out_shape=(
            jax.ShapeDtypeStruct((DEVICES * CAP, E), f32),
            jax.ShapeDtypeStruct((DEVICES, 1, 128), i32),
            jax.ShapeDtypeStruct((ROWS, E), f32),
        ),
        in_specs=[SMEM, ANY, VMEM, VMEM, VMEM, VMEM, VMEM, VMEM],
        out_specs=(VMEM, VMEM, VMEM),
        scratch_shapes=[
            pltpu.VMEM((ROWS, 256), bf16),
            pltpu.VMEM((BAGS, E), f32),
            pltpu.VMEM((DEVICES * CAP, E), f32),
            dma,
            dma,
            dma,
            dma,
            pltpu.SMEM((DEVICES * CAP,), i32),
            dma,
        ],
        compiler_params=params(collective_id=0, has_side_effects=True, vmem_limit_bytes=20 << 20),
        name="pool",
    )(pair_mask, send_bags, send_slots, counts, upper, upper2, lower, lower2)
    slot_of = got_slots.reshape(DEVICES * 128)

    sums = pl.pallas_call(
        place_kernel,
        out_shape=jax.ShapeDtypeStruct((BAGS, E), f32),
        in_specs=[ANY, VMEM],
        out_specs=VMEM,
        scratch_shapes=[pltpu.SMEM((DEVICES * 128,), i32), dma((8,))],
        compiler_params=params(vmem_limit_bytes=16 << 20),
        name="place",
    )(slot_of, got_rows)

    results = pl.pallas_call(
        update_kernel,
        out_shape=(
            jax.ShapeDtypeStruct((ROWS, E), f32),
            jax.ShapeDtypeStruct((1, ROWS), f32),
            jax.ShapeDtypeStruct((INTER, HID), f32),
            jax.ShapeDtypeStruct((1, HID), f32),
        ),
        in_specs=[SMEM, ANY, ANY] + [VMEM] * 8,
        out_specs=(VMEM, VMEM, VMEM, VMEM),
        scratch_shapes=[
            pltpu.VMEM((DEVICES * CAP, E), f32),
            pltpu.VMEM((DEVICES * CAP, E), f32),
            pltpu.VMEM((BAGS, E), f32),
            pltpu.VMEM((2 * E, BAGS), bf16),
            pltpu.VMEM((G_ROWS, 128), f32),
            pltpu.VMEM((BAGS + 8, E), f32),
            pltpu.VMEM((INTER, B_DEV), f32),
            pltpu.VMEM((F + 1, E, B_DEV), f32),
            pltpu.VMEM((B_DEV, HID), f32),
            pltpu.VMEM((G_ROWS, 128), f32),
            pltpu.VMEM((HALF, 128), f32),
            pltpu.VMEM((HALF, 128), f32),
            pltpu.VMEM((4, 1, ROWS), f32),
            pltpu.VMEM((12, 4 * SEG, 128), f32),
            pltpu.VMEM((3, 4 * SEG, 128), f32),
            pltpu.VMEM((12, SEG, 128), f32),
            pltpu.VMEM((3, SEG, 128), f32),
            pltpu.VMEM((12, SEG, 128), f32),
            pltpu.SMEM((DEVICES * 128,), i32),
            pltpu.SMEM((BAGS,), i32),
            dma((2,)),
            dma((4,)),
            dma((4,)),
            dma,
            dma,
            dma,
            dma,
            dma,
            dma,
            dma((60,)),
            dma((60,)),
        ],
        compiler_params=params(collective_id=1, has_side_effects=True, vmem_limit_bytes=30 << 20),
        name="update",
    )(
        pair_mask,
        slot_of,
        where_to,
        sums,
        dense_vectors,
        labels[:, None],
        top_weight,
        out_weight[None, :],
        counts,
        held,
        row_state[None, :],
    )
    new_table, new_state, top_grad, out_grad = pl.pallas_call(
        finish_kernel,
        out_shape=tuple(jax.ShapeDtypeStruct(r.shape, f32) for r in results),
        in_specs=[ANY] * 4,
        out_specs=(ANY,) * 4,
        scratch_shapes=[dma((4,))],
        compiler_params=params(vmem_limit_bytes=16 << 20),
        name="finish",
    )(*results)
    return new_table, new_state.reshape(ROWS), top_grad, out_grad.reshape(HID)


def solution(mesh):
    both = ("gx", "gy")
    in_specs = (
        P(both, None),
        P(both),
        P("gx"),
        P(both),
        P(both, None),
        P(both, None),
        P(both),
        P(both, None),
        P(both),
        P(),
        P(),
    )
    out_specs = (P(both, None), P(both), P(), P())
    return jax.shard_map(
        on_device, mesh=mesh, in_specs=in_specs, out_specs=out_specs, check_vma=False
    )
```

```python
import jax
import jax.numpy as jnp
from jax import lax
from jax.experimental import pallas as pl
from jax.experimental.pallas import tpu as pltpu
from jax.sharding import PartitionSpec as P

E = 128
F = 16
B_DEV = 128
BAGS = 2048
ROWS = 2048
LOOKS = 6144
DEVICES = 128
CAP = 32
INTER = 264
HID = 1024
CHUNK = 256
SPAN = CHUNK + 16
C_ROWS = 2304
G_ROWS = 2304
HALF = G_ROWS // 2
SEG = HALF // 48
STRIDE = 91
CUTS = (1, 32, 64, 96, 128)
PAIRS = [(i, j) for i in range(F + 1) for j in range(i + 1, F + 1)]
PAIR_ROW = {pair: 128 + n for n, pair in enumerate(PAIRS)}

learn_rate = 0.05
epsilon = 1e-08
MESH = pl.DeviceIdType.MESH
f32, bf16, i32 = jnp.float32, jnp.bfloat16, jnp.int32

VMEM = pl.BlockSpec(memory_space=pltpu.VMEM)
SMEM = pl.BlockSpec(memory_space=pltpu.SMEM)
ANY = pl.BlockSpec(memory_space=pl.ANY)


def split(x):
    hi = x.astype(bf16)
    return hi, (x - hi.astype(f32)).astype(bf16)


def mxu(a, b, dims):
    return lax.dot_general(a, b, (dims, ((), ())), preferred_element_type=f32)


def dot3(a, b, dims):
    return mxu(a[0], b[0], dims) + (mxu(a[0], b[1], dims) + mxu(a[1], b[0], dims))


NN = ((1,), (0,))
NT = ((1,), (1,))


def down_sublanes(row):
    return jnp.broadcast_to(row, (128, 128)).T


def count_kernel(first_ref, look_ref, start_ref, end_ref, c_ref, start_t, end_t):
    for r in range(C_ROWS // 128):
        here = slice(r * 128, (r + 1) * 128)
        start_t[here, :] = down_sublanes(start_ref[r : r + 1, :])
        end_t[here, :] = down_sublanes(end_ref[r : r + 1, :])
    c_ref[0:16, :] = jnp.zeros((16, ROWS), bf16)
    lane = lax.broadcasted_iota(i32, (1, 128), 1)

    def chunk(t, carry):
        at = pl.multiple_of(first_ref[t], 16)
        start, end = start_t[pl.ds(at, SPAN), :], end_t[pl.ds(at, SPAN), :]
        halves, columns = [], []
        for h in range(2):
            k = lane + (t * CHUNK + h * 128)
            halves.append(((start <= k) & (k < end)).astype(f32).astype(bf16))
            columns.append(down_sublanes(look_ref[pl.ds(2 * t + h, 1), :]))
        in_bag = jnp.concatenate(halves, axis=1)
        column = jnp.concatenate(columns, axis=0)
        for n in range(0, 16, 4):
            of_row = jnp.concatenate(
                [(column == lane + 128 * q).astype(f32).astype(bf16) for q in range(n, n + 4)],
                axis=1,
            )
            counts = mxu(in_bag, of_row, NN)
            cols = slice(n * 128, (n + 4) * 128)
            before = c_ref[pl.ds(at, 16), cols].astype(f32)
            c_ref[pl.ds(at, 16), cols] = (counts[:16] + before).astype(bf16)
            c_ref[pl.ds(pl.multiple_of(at + 16, 16), SPAN - 16), cols] = counts[16:].astype(bf16)
        return carry

    lax.fori_loop(0, LOOKS // CHUNK, chunk, 0, unroll=2)


def device_at(n):
    return (n // 4, n % 4)


def my_number():
    return lax.axis_index("gx") * 4 + lax.axis_index("gy")


def peer_of(k):
    return (my_number() + STRIDE * k) % DEVICES


def greet_all(barrier):
    def greet(k, carry):
        pl.semaphore_signal(barrier, inc=1, device_id=device_at(peer_of(k)), device_id_type=MESH)
        return carry

    lax.fori_loop(1, DEVICES, greet, 0)


def put(src, dst, send, recv, device):
    return pltpu.make_async_remote_copy(
        src_ref=src, dst_ref=dst, send_sem=send, recv_sem=recv, device_id=device, device_id_type=MESH
    )


def chunk_at(n):
    return pl.ds(pl.multiple_of(n * CAP, CAP), CAP)


def pick_rows(dst, to, src, index_ref, at):
    for u in range(CAP):
        dst[pl.ds(to + u, 1), :] = src[pl.ds(index_ref[at + u], 1), :]


def pool_kernel(
    mask_ref,
    bag_in,
    slots_ref,
    c_ref,
    a_ref,
    a2_ref,
    b_ref,
    b2_ref,
    recv_ref,
    got_ref,
    held_ref,
    split_ref,
    partial_ref,
    send_ref,
    row_send,
    row_recv,
    slot_send,
    slot_recv,
    bag_ref,
    bag_sem,
):
    bag_copy = pltpu.make_async_copy(bag_in, bag_ref, bag_sem)
    bag_copy.start()
    barrier = pltpu.get_barrier_semaphore()
    greet_all(barrier)
    me = my_number()
    mask = jnp.full((ROWS // 2, E), mask_ref[0], i32)
    held_ref[: ROWS // 2, :] = jnp.where(mask >= 2, a2_ref[...], a_ref[...])
    held_ref[ROWS // 2 :, :] = jnp.where((mask == 1) | (mask == 2), b2_ref[...], b_ref[...])
    hi, lo = split(held_ref[...])
    split_ref[:, :128] = hi
    split_ref[:, 128:] = lo

    def block(m, carry):
        at = pl.multiple_of(m * 256, 256)
        both = mxu(c_ref[pl.ds(at, 256), :], split_ref[...], NN)
        partial_ref[pl.ds(at, 256), :] = both[:, :128] + both[:, 128:]
        return carry

    lax.fori_loop(0, BAGS // 256, block, 0)
    got_ref[me] = slots_ref[me]
    bag_copy.wait()
    pick_rows(recv_ref, me * CAP, partial_ref, bag_ref, me * CAP)

    def ready(k):
        at = peer_of(k) * CAP
        pick_rows(send_ref, at, partial_ref, bag_ref, at)

    def start(k):
        peer = peer_of(k)
        to = device_at(peer)
        put(slots_ref.at[peer], got_ref.at[me], slot_send, slot_recv, to).start()
        put(send_ref.at[chunk_at(peer)], recv_ref.at[chunk_at(me)], row_send, row_recv, to).start()

    ready(1)
    pl.semaphore_wait(barrier, DEVICES - 1)

    def step(k, carry):
        ready(k)
        start(k - 1)
        return carry

    lax.fori_loop(2, DEVICES, step, 0)
    start(DEVICES - 1)
    to = device_at(peer_of(1))
    some = pl.ds(0, DEVICES - 1)
    put(slots_ref.at[some], got_ref.at[some], slot_send, slot_recv, to).wait()
    rows = pl.ds(0, (DEVICES - 1) * CAP)
    put(send_ref.at[rows], recv_ref.at[rows], row_send, row_recv, to).wait()


def place_kernel(slot_in, got_ref, pooled, slot_ref, sems):
    part = DEVICES * 128 // 8
    copies = []
    for q in range(8):
        here = pl.ds(q * part, part)
        copies.append(pltpu.make_async_copy(slot_in.at[here], slot_ref.at[here], sems.at[q]))
        copies[q].start()

    def place(c, carry):
        @pl.when(slot_ref[c * 128] < BAGS)
        def _():
            for u in range(CAP):
                pooled[pl.ds(slot_ref[c * 128 + u], 1), :] = got_ref[pl.ds(c * CAP + u, 1), :]

        return carry

    for q in range(8):
        copies[q].wait()
        lax.fori_loop(q * DEVICES // 8, (q + 1) * DEVICES // 8, place, 0)


def finish_kernel(a, b, c, d, to_a, to_b, to_c, to_d, sems):
    pairs = ((a, to_a), (b, to_b), (c, to_c), (d, to_d))
    copies = [pltpu.make_async_copy(x, y, sems.at[n]) for n, (x, y) in enumerate(pairs)]
    for copy in copies:
        copy.start()
    for copy in copies:
        copy.wait()


def update_kernel(
    mask_ref,
    slot_in,
    where_in,
    sums_ref,
    dense_ref,
    label_ref,
    w_ref,
    wo_ref,
    c_ref,
    table_ref,
    state_ref,
    new_table_ref,
    new_state_ref,
    top_ref,
    out_ref,
    back,
    came,
    grads,
    sides,
    fin,
    pooled,
    inter_t,
    vt,
    d_pre_ref,
    grad_ref,
    r1,
    acc,
    states,
    ra,
    part_a,
    rb,
    mine,
    rc,
    slot_ref,
    where_ref,
    table_sem,
    state_send,
    state_recv,
    row_send,
    row_recv,
    swap_send,
    swap_recv,
    last_send,
    last_recv,
    color_send,
    color_recv,
):
    tables = [
        pltpu.make_async_copy(slot_in, slot_ref, table_sem.at[0]),
        pltpu.make_async_copy(where_in, where_ref, table_sem.at[1]),
    ]
    for copy in tables:
        copy.start()
    barrier = pltpu.get_barrier_semaphore()
    greet_all(barrier)
    me = my_number()
    gx, x = lax.axis_index("gx"), lax.axis_index("gy")
    yz, core = gx // 2, gx % 2
    twin = (gx + 1 - 2 * core, x)

    y, z = yz // 4, yz % 4

    def along_x(k):
        return (gx, (x + k) % 4)

    def along_y(k):
        return (((y + k) % 4 * 4 + z) * 2 + core, x)

    def along_z(k):
        return ((y * 4 + (z + k) % 4) * 2 + core, x)

    dense_t = dense_ref[...].T
    vt[0] = dense_t
    inter_t[0:128, :] = dense_t
    for f in range(F):
        vt[f + 1] = sums_ref[f * 128 : (f + 1) * 128, :].T
    for i in range(F):
        for j in range(i + 1, F + 1):
            row = PAIR_ROW[i, j]
            inter_t[row : row + 1, :] = jnp.sum(vt[i] * vt[j], axis=0, keepdims=True)

    it = inter_t[...]
    w = split(w_ref[...])
    pre = dot3(split(it.T), w, NN)
    sig = 1.0 / (1.0 + jnp.exp(-pre))
    hidden = pre * sig
    logits = jnp.sum(hidden * wo_ref[...], axis=1, keepdims=True)
    d_logits = 1.0 / (1.0 + jnp.exp(-logits)) - label_ref[...]
    out_grad = jnp.sum(hidden * d_logits, axis=0, keepdims=True)
    for q in range(8):
        grad_ref[8 * INTER + q : 8 * INTER + q + 1, :] = out_grad[:, q * 128 : (q + 1) * 128]
    grad_ref[8 * INTER + 8 :, :] = jnp.zeros((G_ROWS - 8 * INTER - 8, 128), f32)
    d_pre_ref[...] = d_logits * wo_ref[...] * (sig * (1.0 + pre * (1.0 - sig)))
    d_pre = split(d_pre_ref[...])
    top_grad = dot3(split(it), d_pre, NN)
    for q in range(8):
        grad_ref[q * INTER : (q + 1) * INTER, :] = top_grad[:, q * 128 : (q + 1) * 128]
    inter_t[...] = dot3(w, d_pre, NT)

    def pooled_grad(j):
        total = None
        for i in range(F + 1):
            if i != j:
                row = PAIR_ROW[min(i, j), max(i, j)]
                term = inter_t[row : row + 1, :] * vt[i]
                total = term if total is None else total + term
        pooled[(j - 1) * 128 : j * 128, :] = total.T

    for j in range(1, 7):
        pooled_grad(j)

    my_half = pl.multiple_of(core * HALF, 8)
    other = pl.multiple_of((1 - core) * HALF, 8)
    pl.semaphore_wait(barrier, DEVICES - 1)
    swap = put(grad_ref.at[pl.ds(other, HALF)], r1, swap_send, swap_recv, twin)
    swap.start()
    flips = [None, x + 1 - 2 * (x % 2), (x + 2) % 4, 3 - x]
    state_moves = [
        put(state_ref, states.at[f], state_send.at[f], state_recv.at[f], (gx, flips[f]))
        for f in range(1, 4)
    ]
    for move in state_moves:
        move.start()
    for j in range(7, F + 1):
        pooled_grad(j)
    pooled[BAGS:, :] = jnp.zeros((8, E), f32)

    def ready(k):
        peer = peer_of(k)
        pick_rows(back, peer * CAP, pooled, slot_ref, peer * 128)

    def start(k):
        peer = peer_of(k)
        put(
            back.at[chunk_at(peer)], came.at[chunk_at(me)], row_send, row_recv, device_at(peer)
        ).start()

    def send_rows(n):
        def step(k, carry):
            ready(k + 1)
            start(k)
            return carry

        last = DEVICES - 1 if CUTS[n + 1] == DEVICES else CUTS[n + 1]
        lax.fori_loop(CUTS[n], last, step, 0)
        if last < CUTS[n + 1]:
            start(last)

    class Color:
        def __init__(self, n, at, to):
            self.n, self.at = n, at
            self.to = (to[0], to[1], to[2], to[1], to[0])
            self.base = n * 16 * SEG

        def move(self, phase, k, src, dst):
            sem = (self.n * 5 + phase) * 4 + k
            return put(src, dst, color_send.at[sem], color_recv.at[sem], self.to[phase](k))

        def rows_a(self, a, base):
            return pl.ds(pl.multiple_of(base + self.base + a * (4 * SEG), 8), 4 * SEG)

        def rows_b(self, a, b, base):
            return pl.ds(pl.multiple_of(base + self.base + (a * 4 + b) * SEG, 8), SEG)

        def moves(self, phase, waiting):
            n = self.n
            a, b, c = self.at
            out = []
            for k in range(1, 4):
                if phase == 0:
                    there = acc.at[self.rows_a((a + k) % 4, 0)]
                    out.append(self.move(0, k, there, ra.at[4 * n + k]))
                if phase == 1:
                    there = pl.ds(pl.multiple_of((b + k) % 4 * SEG, 8), SEG)
                    out.append(self.move(1, k, part_a.at[n, there], rb.at[4 * n + k]))
                if phase == 2:
                    slot = (c + 4 - k) % 4 if waiting else c
                    out.append(self.move(2, k, mine.at[n], rc.at[4 * n + slot]))
                if phase == 3:
                    who = (b + 4 - k) % 4 if waiting else b
                    there = fin.at[self.rows_b(a, who, my_half)]
                    out.append(self.move(3, k, there, there))
                if phase == 4:
                    who = (a + 4 - k) % 4 if waiting else a
                    there = fin.at[self.rows_a(who, my_half)]
                    out.append(self.move(4, k, there, there))
            return out

        def begin(self, phase):
            for copy in self.moves(phase, False):
                copy.start()

        def finish(self, phase):
            for copy in self.moves(phase, False):
                copy.wait_send()
            for copy in self.moves(phase, True):
                copy.wait_recv()
            n = self.n
            a, b, c = self.at
            if phase == 0:
                own = acc[self.rows_a(a, 0), :]
                part_a[n] = (own + ra[4 * n + 1]) + (ra[4 * n + 2] + ra[4 * n + 3])
            if phase == 1:
                own = part_a[n, pl.ds(pl.multiple_of(b * SEG, 8), SEG), :]
                part = (own + rb[4 * n + 1]) + (rb[4 * n + 2] + rb[4 * n + 3])
                mine[n] = part
                rc[4 * n + c] = part
            if phase == 2:
                whole = (rc[4 * n] + rc[4 * n + 1]) + (rc[4 * n + 2] + rc[4 * n + 3])
                fin[self.rows_b(a, b, my_half), :] = whole

    colors = (
        Color(0, (z, y, x), (along_z, along_y, along_x)),
        Color(1, (y, x, z), (along_y, along_x, along_z)),
        Color(2, (x, z, y), (along_x, along_z, along_y)),
    )

    def phase_on(phase):
        for color in colors:
            color.begin(phase)

    def phase_off(phase):
        for color in colors:
            color.finish(phase)

    swap.wait()
    acc[...] = grad_ref[pl.ds(my_half, HALF), :] + r1[...]
    phase_on(0)
    tables[0].wait()
    pick_rows(came, me * CAP, pooled, slot_ref, me * 128)
    ready(1)
    for phase in range(4):
        send_rows(phase)
        phase_off(phase)
        phase_on(phase + 1)

    rows = pl.ds(0, (DEVICES - 1) * CAP)
    put(back.at[rows], came.at[rows], row_send, row_recv, device_at(peer_of(1))).wait()
    tables[1].wait()
    for move in state_moves:
        move.wait()
    mask = jnp.full((1, ROWS), mask_ref[0], i32)
    held_state = state_ref[...]
    for f in range(1, 4):
        held_state = jnp.where(mask == f, states[f], held_state)
    states[0] = held_state

    def take(n, carry):
        pick_rows(grads, n * CAP, came, where_ref, n * CAP)
        return carry

    lax.fori_loop(0, BAGS // CAP, take, 0)
    for q in range(BAGS // 128):
        here = slice(q * 128, (q + 1) * 128)
        hi, lo = split(grads[here, :].T)
        sides[0:128, here] = hi
        sides[128:256, here] = lo

    phase_off(4)
    half = fin.at[pl.ds(my_half, HALF)]
    rest = fin.at[pl.ds(other, HALF)]
    last = put(half, half, last_send, last_recv, twin)
    last.start()

    def block(n, carry):
        here = pl.ds(pl.multiple_of(n * 256, 256), 256)
        both = mxu(sides[...], c_ref[0:BAGS, here], NN)
        row_grad = both[:128] + both[128:]
        state = states[0, :, here] + jnp.sum(row_grad * row_grad, axis=0, keepdims=True) * (1.0 / E)
        new_state_ref[:, here] = state
        step = row_grad * (learn_rate / (jnp.sqrt(state) + epsilon))
        new_table_ref[here, :] = table_ref[here, :] - step.T
        return carry

    lax.fori_loop(0, ROWS // 256, block, 0)

    last.wait_send()
    put(rest, rest, last_send, last_recv, twin).wait_recv()
    for q in range(8):
        top_ref[:, q * 128 : (q + 1) * 128] = fin[q * INTER : (q + 1) * INTER, :]
        out_ref[:, q * 128 : (q + 1) * 128] = fin[8 * INTER + q : 8 * INTER + q + 1, :]


def params(**kw):
    return pltpu.CompilerParams(**kw)


def from_partner(block, flip):
    return lax.ppermute(block, "gy", [(y, y ^ flip) for y in range(4)])


def on_device(
    emb_table,
    row_state,
    pair_mask,
    look_rows,
    bag_sizes,
    bag_owner,
    bag_slot,
    dense_vectors,
    labels,
    top_weight,
    out_weight,
):
    mask = pair_mask[0]
    first, second = (mask == 1) | (mask == 2), mask >= 2
    upper, lower = emb_table[: ROWS // 2], emb_table[ROWS // 2 :]
    upper = jnp.where(first, from_partner(upper, 1), upper)
    lower = jnp.where(second, from_partner(lower, 3), lower)

    owners = bag_owner[:, 0]
    onehot = (owners[:, None] == jnp.arange(DEVICES, dtype=i32)[None, :]).astype(i32)
    placed_at = jnp.sum((jnp.cumsum(onehot, axis=0) - onehot) * onehot, axis=1)
    where_to = owners * CAP + placed_at
    spot = (placed_at[:, None] == jnp.arange(CAP, dtype=i32)[None, :]).astype(f32)
    sample, feature = bag_slot // F, bag_slot % F
    bag = jnp.arange(BAGS, dtype=i32)
    pieces = [sample, feature + 1, bag // 16, bag % 16]
    parts = jnp.concatenate([spot * piece.astype(f32)[:, None] for piece in pieces], axis=1)
    coded = mxu(onehot.astype(bf16), parts.astype(bf16), ((0,), (0,))).astype(i32)
    sample_at, feature_at = coded[:, :CAP], coded[:, CAP : 2 * CAP]
    send_slots = jnp.where(feature_at > 0, (feature_at - 1) * B_DEV + sample_at, BAGS)
    send_slots = jnp.pad(send_slots, ((0, 0), (0, 128 - CAP))).reshape(DEVICES, 1, 128)
    send_bags = (coded[:, 2 * CAP : 3 * CAP] * 16 + coded[:, 3 * CAP :]).reshape(DEVICES * CAP)

    sizes = bag_sizes[0]
    ends = jnp.cumsum(sizes)
    starts = ends - sizes
    bounds = jnp.arange(LOOKS // CHUNK, dtype=i32) * CHUNK
    first_bag = jnp.sum((ends[None, :] <= bounds[:, None]).astype(i32), axis=1) // 16 * 16
    extra = C_ROWS - BAGS
    ends2 = jnp.concatenate([ends, jnp.zeros((extra,), i32)]).reshape(C_ROWS // 128, 128)
    starts2 = jnp.concatenate([starts, jnp.full((extra,), LOOKS, i32)]).reshape(C_ROWS // 128, 128)
    upper, lower, look_rows, first_bag, starts2, ends2 = lax.optimization_barrier(
        (upper, lower, look_rows, first_bag, starts2, ends2)
    )
    upper2, lower2 = from_partner(upper, 3), from_partner(lower, 1)
    counts = pl.pallas_call(
        count_kernel,
        out_shape=jax.ShapeDtypeStruct((C_ROWS, ROWS), bf16),
        in_specs=[SMEM, VMEM, VMEM, VMEM],
        out_specs=VMEM,
        scratch_shapes=[pltpu.VMEM((C_ROWS, 128), i32), pltpu.VMEM((C_ROWS, 128), i32)],
        compiler_params=params(vmem_limit_bytes=24 << 20),
        cost_estimate=pl.CostEstimate(flops=2 * LOOKS * SPAN * ROWS, bytes_accessed=10 << 20, transcendentals=0),
        name="count",
    )(first_bag, look_rows.reshape(LOOKS // 128, 128), starts2, ends2)

    dma = pltpu.SemaphoreType.DMA
    got_rows, got_slots, held = pl.pallas_call(
        pool_kernel,
        out_shape=(
            jax.ShapeDtypeStruct((DEVICES * CAP, E), f32),
            jax.ShapeDtypeStruct((DEVICES, 1, 128), i32),
            jax.ShapeDtypeStruct((ROWS, E), f32),
        ),
        in_specs=[SMEM, ANY, VMEM, VMEM, VMEM, VMEM, VMEM, VMEM],
        out_specs=(VMEM, VMEM, VMEM),
        scratch_shapes=[
            pltpu.VMEM((ROWS, 256), bf16),
            pltpu.VMEM((BAGS, E), f32),
            pltpu.VMEM((DEVICES * CAP, E), f32),
            dma,
            dma,
            dma,
            dma,
            pltpu.SMEM((DEVICES * CAP,), i32),
            dma,
        ],
        compiler_params=params(collective_id=0, has_side_effects=True, vmem_limit_bytes=20 << 20),
        name="pool",
    )(pair_mask, send_bags, send_slots, counts, upper, upper2, lower, lower2)
    slot_of = got_slots.reshape(DEVICES * 128)

    sums = pl.pallas_call(
        place_kernel,
        out_shape=jax.ShapeDtypeStruct((BAGS, E), f32),
        in_specs=[ANY, VMEM],
        out_specs=VMEM,
        scratch_shapes=[pltpu.SMEM((DEVICES * 128,), i32), dma((8,))],
        compiler_params=params(vmem_limit_bytes=16 << 20),
        name="place",
    )(slot_of, got_rows)

    results = pl.pallas_call(
        update_kernel,
        out_shape=(
            jax.ShapeDtypeStruct((ROWS, E), f32),
            jax.ShapeDtypeStruct((1, ROWS), f32),
            jax.ShapeDtypeStruct((INTER, HID), f32),
            jax.ShapeDtypeStruct((1, HID), f32),
        ),
        in_specs=[SMEM, ANY, ANY] + [VMEM] * 8,
        out_specs=(VMEM, VMEM, VMEM, VMEM),
        scratch_shapes=[
            pltpu.VMEM((DEVICES * CAP, E), f32),
            pltpu.VMEM((DEVICES * CAP, E), f32),
            pltpu.VMEM((BAGS, E), f32),
            pltpu.VMEM((2 * E, BAGS), bf16),
            pltpu.VMEM((G_ROWS, 128), f32),
            pltpu.VMEM((BAGS + 8, E), f32),
            pltpu.VMEM((INTER, B_DEV), f32),
            pltpu.VMEM((F + 1, E, B_DEV), f32),
            pltpu.VMEM((B_DEV, HID), f32),
            pltpu.VMEM((G_ROWS, 128), f32),
            pltpu.VMEM((HALF, 128), f32),
            pltpu.VMEM((HALF, 128), f32),
            pltpu.VMEM((4, 1, ROWS), f32),
            pltpu.VMEM((12, 4 * SEG, 128), f32),
            pltpu.VMEM((3, 4 * SEG, 128), f32),
            pltpu.VMEM((12, SEG, 128), f32),
            pltpu.VMEM((3, SEG, 128), f32),
            pltpu.VMEM((12, SEG, 128), f32),
            pltpu.SMEM((DEVICES * 128,), i32),
            pltpu.SMEM((BAGS,), i32),
            dma((2,)),
            dma((4,)),
            dma((4,)),
            dma,
            dma,
            dma,
            dma,
            dma,
            dma,
            dma((60,)),
            dma((60,)),
        ],
        compiler_params=params(collective_id=1, has_side_effects=True, vmem_limit_bytes=30 << 20),
        name="update",
    )(
        pair_mask,
        slot_of,
        where_to,
        sums,
        dense_vectors,
        labels[:, None],
        top_weight,
        out_weight[None, :],
        counts,
        held,
        row_state[None, :],
    )
    new_table, new_state, top_grad, out_grad = pl.pallas_call(
        finish_kernel,
        out_shape=tuple(jax.ShapeDtypeStruct(r.shape, f32) for r in results),
        in_specs=[ANY] * 4,
        out_specs=(ANY,) * 4,
        scratch_shapes=[dma((4,))],
        compiler_params=params(vmem_limit_bytes=16 << 20),
        name="finish",
    )(*results)
    return new_table, new_state.reshape(ROWS), top_grad, out_grad.reshape(HID)


def solution(mesh):
    both = ("gx", "gy")
    in_specs = (
        P(both, None),
        P(both),
        P("gx"),
        P(both),
        P(both, None),
        P(both, None),
        P(both),
        P(both, None),
        P(both),
        P(),
        P(),
    )
    out_specs = (P(both, None), P(both), P(), P())
    return jax.shard_map(
        on_device, mesh=mesh, in_specs=in_specs, out_specs=out_specs, check_vma=False
    )
```

```python
import jax
import jax.numpy as jnp
from jax import lax
from jax.experimental import pallas as pl
from jax.experimental.pallas import tpu as pltpu
from jax.sharding import PartitionSpec as P

E = 128
F = 16
B_DEV = 128
BAGS = 2048
ROWS = 2048
LOOKS = 6144
DEVICES = 128
CAP = 32
INTER = 264
HID = 1024
CHUNK = 256
SPAN = CHUNK + 16
C_ROWS = 2304
G_ROWS = 2304
HALF = G_ROWS // 2
SEG = HALF // 48
STRIDE = 91
CUTS = (1, 12, 40, 70, 100, 128)
PAIRS = [(i, j) for i in range(F + 1) for j in range(i + 1, F + 1)]
PAIR_ROW = {pair: 128 + n for n, pair in enumerate(PAIRS)}

learn_rate = 0.05
epsilon = 1e-08
MESH = pl.DeviceIdType.MESH
f32, bf16, i32 = jnp.float32, jnp.bfloat16, jnp.int32

VMEM = pl.BlockSpec(memory_space=pltpu.VMEM)
SMEM = pl.BlockSpec(memory_space=pltpu.SMEM)
ANY = pl.BlockSpec(memory_space=pl.ANY)


def split(x):
    hi = x.astype(bf16)
    return hi, (x - hi.astype(f32)).astype(bf16)


def mxu(a, b, dims):
    return lax.dot_general(a, b, (dims, ((), ())), preferred_element_type=f32)


def dot3(a, b, dims):
    return mxu(a[0], b[0], dims) + (mxu(a[0], b[1], dims) + mxu(a[1], b[0], dims))


NN = ((1,), (0,))
NT = ((1,), (1,))


def down_sublanes(row):
    return jnp.broadcast_to(row, (128, 128)).T


def count_kernel(first_ref, look_ref, start_ref, end_ref, c_ref, start_t, end_t):
    for r in range(C_ROWS // 128):
        here = slice(r * 128, (r + 1) * 128)
        start_t[here, :] = down_sublanes(start_ref[r : r + 1, :])
        end_t[here, :] = down_sublanes(end_ref[r : r + 1, :])
    c_ref[0:16, :] = jnp.zeros((16, ROWS), bf16)
    lane = lax.broadcasted_iota(i32, (1, 128), 1)

    def chunk(t, carry):
        at = pl.multiple_of(first_ref[t], 16)
        start, end = start_t[pl.ds(at, SPAN), :], end_t[pl.ds(at, SPAN), :]
        halves, columns = [], []
        for h in range(2):
            k = lane + (t * CHUNK + h * 128)
            halves.append(((start <= k) & (k < end)).astype(f32).astype(bf16))
            columns.append(down_sublanes(look_ref[pl.ds(2 * t + h, 1), :]))
        in_bag = jnp.concatenate(halves, axis=1)
        column = jnp.concatenate(columns, axis=0)
        for n in range(0, 16, 4):
            of_row = jnp.concatenate(
                [(column == lane + 128 * q).astype(f32).astype(bf16) for q in range(n, n + 4)],
                axis=1,
            )
            counts = mxu(in_bag, of_row, NN)
            cols = slice(n * 128, (n + 4) * 128)
            before = c_ref[pl.ds(at, 16), cols].astype(f32)
            c_ref[pl.ds(at, 16), cols] = (counts[:16] + before).astype(bf16)
            c_ref[pl.ds(pl.multiple_of(at + 16, 16), SPAN - 16), cols] = counts[16:].astype(bf16)
        return carry

    lax.fori_loop(0, LOOKS // CHUNK, chunk, 0, unroll=2)


def device_at(n):
    return (n // 4, n % 4)


def my_number():
    return lax.axis_index("gx") * 4 + lax.axis_index("gy")


def peer_of(k):
    return (my_number() + STRIDE * k) % DEVICES


def greet_all(barrier):
    def greet(k, carry):
        pl.semaphore_signal(barrier, inc=1, device_id=device_at(peer_of(k)), device_id_type=MESH)
        return carry

    lax.fori_loop(1, DEVICES, greet, 0, unroll=8)


def put(src, dst, send, recv, device):
    return pltpu.make_async_remote_copy(
        src_ref=src, dst_ref=dst, send_sem=send, recv_sem=recv, device_id=device, device_id_type=MESH
    )


def chunk_at(n):
    return pl.ds(pl.multiple_of(n * CAP, CAP), CAP)


def pick_rows(dst, to, src, index_ref, at):
    for u in range(CAP):
        dst[pl.ds(to + u, 1), :] = src[pl.ds(index_ref[at + u], 1), :]


def pool_kernel(
    mask_ref,
    bag_in,
    slots_ref,
    c_ref,
    a_ref,
    a2_ref,
    b_ref,
    b2_ref,
    recv_ref,
    got_ref,
    held_ref,
    split_ref,
    partial_ref,
    send_ref,
    row_send,
    row_recv,
    slot_send,
    slot_recv,
    bag_ref,
    bag_sem,
):
    bag_copy = pltpu.make_async_copy(bag_in, bag_ref, bag_sem)
    bag_copy.start()
    barrier = pltpu.get_barrier_semaphore()
    greet_all(barrier)
    me = my_number()
    mask = jnp.full((ROWS // 2, E), mask_ref[0], i32)
    held_ref[: ROWS // 2, :] = jnp.where(mask >= 2, a2_ref[...], a_ref[...])
    held_ref[ROWS // 2 :, :] = jnp.where((mask == 1) | (mask == 2), b2_ref[...], b_ref[...])
    hi, lo = split(held_ref[...])
    split_ref[:, :128] = hi
    split_ref[:, 128:] = lo

    def block(m, carry):
        at = pl.multiple_of(m * 256, 256)
        both = mxu(c_ref[pl.ds(at, 256), :], split_ref[...], NN)
        partial_ref[pl.ds(at, 256), :] = both[:, :128] + both[:, 128:]
        return carry

    lax.fori_loop(0, BAGS // 256, block, 0)
    got_ref[me] = slots_ref[me]
    bag_copy.wait()
    pick_rows(recv_ref, me * CAP, partial_ref, bag_ref, me * CAP)

    def ready(k):
        at = peer_of(k) * CAP
        pick_rows(send_ref, at, partial_ref, bag_ref, at)

    def start(k):
        peer = peer_of(k)
        to = device_at(peer)
        put(slots_ref.at[peer], got_ref.at[me], slot_send, slot_recv, to).start()
        put(send_ref.at[chunk_at(peer)], recv_ref.at[chunk_at(me)], row_send, row_recv, to).start()

    ready(1)
    pl.semaphore_wait(barrier, DEVICES - 1)

    def step(k, carry):
        ready(k)
        start(k - 1)
        return carry

    lax.fori_loop(2, DEVICES, step, 0)
    start(DEVICES - 1)
    to = device_at(peer_of(1))
    some = pl.ds(0, DEVICES - 1)
    put(slots_ref.at[some], got_ref.at[some], slot_send, slot_recv, to).wait()
    rows = pl.ds(0, (DEVICES - 1) * CAP)
    put(send_ref.at[rows], recv_ref.at[rows], row_send, row_recv, to).wait()


def place_kernel(slot_in, got_ref, pooled, slot_ref, sems):
    part = DEVICES * 128 // 8
    copies = []
    for q in range(8):
        here = pl.ds(q * part, part)
        copies.append(pltpu.make_async_copy(slot_in.at[here], slot_ref.at[here], sems.at[q]))
        copies[q].start()

    def place(c, carry):
        @pl.when(slot_ref[c * 128] < BAGS)
        def _():
            for u in range(CAP):
                pooled[pl.ds(slot_ref[c * 128 + u], 1), :] = got_ref[pl.ds(c * CAP + u, 1), :]

        return carry

    for q in range(8):
        copies[q].wait()
        lax.fori_loop(q * DEVICES // 8, (q + 1) * DEVICES // 8, place, 0)


def finish_kernel(a, b, c, d, to_a, to_b, to_c, to_d, sems):
    pairs = ((a, to_a), (b, to_b), (c, to_c), (d, to_d))
    copies = [pltpu.make_async_copy(x, y, sems.at[n]) for n, (x, y) in enumerate(pairs)]
    for copy in copies:
        copy.start()
    for copy in copies:
        copy.wait()


def update_kernel(
    mask_ref,
    slot_in,
    where_in,
    sums_ref,
    dense_ref,
    label_ref,
    w_ref,
    wo_ref,
    c_ref,
    table_ref,
    state_ref,
    new_table_ref,
    new_state_ref,
    top_ref,
    out_ref,
    back,
    came,
    grads,
    sides,
    fin,
    pooled,
    inter_t,
    vt,
    d_pre_ref,
    grad_ref,
    r1,
    acc,
    states,
    ra,
    part_a,
    rb,
    mine,
    rc,
    slot_ref,
    where_ref,
    table_sem,
    state_send,
    state_recv,
    row_send,
    row_recv,
    swap_send,
    swap_recv,
    last_send,
    last_recv,
    color_send,
    color_recv,
):
    tables = [
        pltpu.make_async_copy(slot_in, slot_ref, table_sem.at[0]),
        pltpu.make_async_copy(where_in, where_ref, table_sem.at[1]),
    ]
    for copy in tables:
        copy.start()
    barrier = pltpu.get_barrier_semaphore()
    greet_all(barrier)
    me = my_number()
    gx, x = lax.axis_index("gx"), lax.axis_index("gy")
    yz, core = gx // 2, gx % 2
    twin = (gx + 1 - 2 * core, x)

    y, z = yz // 4, yz % 4

    def along_x(k):
        return (gx, (x + k) % 4)

    def along_y(k):
        return (((y + k) % 4 * 4 + z) * 2 + core, x)

    def along_z(k):
        return ((y * 4 + (z + k) % 4) * 2 + core, x)

    dense_t = dense_ref[...].T
    vt[0] = dense_t
    inter_t[0:128, :] = dense_t
    for f in range(F):
        vt[f + 1] = sums_ref[f * 128 : (f + 1) * 128, :].T
    for i in range(F):
        for j in range(i + 1, F + 1):
            row = PAIR_ROW[i, j]
            inter_t[row : row + 1, :] = jnp.sum(vt[i] * vt[j], axis=0, keepdims=True)

    it = inter_t[...]
    w = split(w_ref[...])
    pre = dot3(split(it.T), w, NN)
    sig = 1.0 / (1.0 + jnp.exp(-pre))
    hidden = pre * sig
    logits = jnp.sum(hidden * wo_ref[...], axis=1, keepdims=True)
    d_logits = 1.0 / (1.0 + jnp.exp(-logits)) - label_ref[...]
    out_grad = jnp.sum(hidden * d_logits, axis=0, keepdims=True)
    for q in range(8):
        grad_ref[8 * INTER + q : 8 * INTER + q + 1, :] = out_grad[:, q * 128 : (q + 1) * 128]
    grad_ref[8 * INTER + 8 :, :] = jnp.zeros((G_ROWS - 8 * INTER - 8, 128), f32)
    d_pre_ref[...] = d_logits * wo_ref[...] * (sig * (1.0 + pre * (1.0 - sig)))
    d_pre = split(d_pre_ref[...])
    top_grad = dot3(split(it), d_pre, NN)
    for q in range(8):
        grad_ref[q * INTER : (q + 1) * INTER, :] = top_grad[:, q * 128 : (q + 1) * 128]
    inter_t[...] = dot3(w, d_pre, NT)

    def pooled_grad(j):
        total = None
        for i in range(F + 1):
            if i != j:
                row = PAIR_ROW[min(i, j), max(i, j)]
                term = inter_t[row : row + 1, :] * vt[i]
                total = term if total is None else total + term
        pooled[(j - 1) * 128 : j * 128, :] = total.T

    for j in range(1, 7):
        pooled_grad(j)

    my_half = pl.multiple_of(core * HALF, 8)
    other = pl.multiple_of((1 - core) * HALF, 8)
    pl.semaphore_wait(barrier, DEVICES - 1)
    swap = put(grad_ref.at[pl.ds(other, HALF)], r1, swap_send, swap_recv, twin)
    swap.start()
    flips = [None, x + 1 - 2 * (x % 2), (x + 2) % 4, 3 - x]
    state_moves = [
        put(state_ref, states.at[f], state_send.at[f], state_recv.at[f], (gx, flips[f]))
        for f in range(1, 4)
    ]
    for move in state_moves:
        move.start()
    for j in range(7, F + 1):
        pooled_grad(j)
    pooled[BAGS:, :] = jnp.zeros((8, E), f32)

    def ready(k):
        peer = peer_of(k)
        pick_rows(back, peer * CAP, pooled, slot_ref, peer * 128)

    def start(k):
        peer = peer_of(k)
        put(
            back.at[chunk_at(peer)], came.at[chunk_at(me)], row_send, row_recv, device_at(peer)
        ).start()

    def send_rows(n):
        def step(k, carry):
            ready(k + 1)
            start(k)
            return carry

        last = DEVICES - 1 if CUTS[n + 1] == DEVICES else CUTS[n + 1]
        lax.fori_loop(CUTS[n], last, step, 0)
        if last < CUTS[n + 1]:
            start(last)

    class Color:
        def __init__(self, n, at, to):
            self.n, self.at = n, at
            self.to = (to[0], to[1], to[2], to[1], to[0])
            self.base = n * 16 * SEG

        def move(self, phase, k, src, dst):
            sem = (self.n * 5 + phase) * 4 + k
            return put(src, dst, color_send.at[sem], color_recv.at[sem], self.to[phase](k))

        def rows_a(self, a, base):
            return pl.ds(pl.multiple_of(base + self.base + a * (4 * SEG), 8), 4 * SEG)

        def rows_b(self, a, b, base):
            return pl.ds(pl.multiple_of(base + self.base + (a * 4 + b) * SEG, 8), SEG)

        def moves(self, phase, waiting):
            n = self.n
            a, b, c = self.at
            out = []
            for k in range(1, 4):
                if phase == 0:
                    there = acc.at[self.rows_a((a + k) % 4, 0)]
                    out.append(self.move(0, k, there, ra.at[4 * n + k]))
                if phase == 1:
                    there = pl.ds(pl.multiple_of((b + k) % 4 * SEG, 8), SEG)
                    out.append(self.move(1, k, part_a.at[n, there], rb.at[4 * n + k]))
                if phase == 2:
                    slot = (c + 4 - k) % 4 if waiting else c
                    out.append(self.move(2, k, mine.at[n], rc.at[4 * n + slot]))
                if phase == 3:
                    who = (b + 4 - k) % 4 if waiting else b
                    there = fin.at[self.rows_b(a, who, my_half)]
                    out.append(self.move(3, k, there, there))
                if phase == 4:
                    who = (a + 4 - k) % 4 if waiting else a
                    there = fin.at[self.rows_a(who, my_half)]
                    out.append(self.move(4, k, there, there))
            return out

        def begin(self, phase):
            for copy in self.moves(phase, False):
                copy.start()

        def finish(self, phase):
            for copy in self.moves(phase, False):
                copy.wait_send()
            for copy in self.moves(phase, True):
                copy.wait_recv()
            n = self.n
            a, b, c = self.at
            if phase == 0:
                own = acc[self.rows_a(a, 0), :]
                part_a[n] = (own + ra[4 * n + 1]) + (ra[4 * n + 2] + ra[4 * n + 3])
            if phase == 1:
                own = part_a[n, pl.ds(pl.multiple_of(b * SEG, 8), SEG), :]
                part = (own + rb[4 * n + 1]) + (rb[4 * n + 2] + rb[4 * n + 3])
                mine[n] = part
                rc[4 * n + c] = part
            if phase == 2:
                whole = (rc[4 * n] + rc[4 * n + 1]) + (rc[4 * n + 2] + rc[4 * n + 3])
                fin[self.rows_b(a, b, my_half), :] = whole

    colors = (
        Color(0, (z, y, x), (along_z, along_y, along_x)),
        Color(1, (y, x, z), (along_y, along_x, along_z)),
        Color(2, (x, z, y), (along_x, along_z, along_y)),
    )

    def phase_on(phase):
        for color in colors:
            color.begin(phase)

    def phase_off(phase):
        for color in colors:
            color.finish(phase)

    tables[0].wait()
    pick_rows(came, me * CAP, pooled, slot_ref, me * 128)
    ready(1)
    send_rows(0)
    swap.wait()
    acc[...] = grad_ref[pl.ds(my_half, HALF), :] + r1[...]
    phase_on(0)
    for phase in range(4):
        send_rows(phase + 1)
        phase_off(phase)
        phase_on(phase + 1)

    rows = pl.ds(0, (DEVICES - 1) * CAP)
    put(back.at[rows], came.at[rows], row_send, row_recv, device_at(peer_of(1))).wait()
    tables[1].wait()
    for move in state_moves:
        move.wait()
    mask = jnp.full((1, ROWS), mask_ref[0], i32)
    held_state = state_ref[...]
    for f in range(1, 4):
        held_state = jnp.where(mask == f, states[f], held_state)
    states[0] = held_state

    def take(n, carry):
        pick_rows(grads, n * CAP, came, where_ref, n * CAP)
        return carry

    lax.fori_loop(0, BAGS // CAP, take, 0)
    for q in range(BAGS // 128):
        here = slice(q * 128, (q + 1) * 128)
        hi, lo = split(grads[here, :].T)
        sides[0:128, here] = hi
        sides[128:256, here] = lo

    phase_off(4)
    half = fin.at[pl.ds(my_half, HALF)]
    rest = fin.at[pl.ds(other, HALF)]
    last = put(half, half, last_send, last_recv, twin)
    last.start()

    def block(n, carry):
        here = pl.ds(pl.multiple_of(n * 256, 256), 256)
        both = mxu(sides[...], c_ref[0:BAGS, here], NN)
        row_grad = both[:128] + both[128:]
        state = states[0, :, here] + jnp.sum(row_grad * row_grad, axis=0, keepdims=True) * (1.0 / E)
        new_state_ref[:, here] = state
        step = row_grad * (learn_rate / (jnp.sqrt(state) + epsilon))
        new_table_ref[here, :] = table_ref[here, :] - step.T
        return carry

    lax.fori_loop(0, ROWS // 256, block, 0)

    last.wait_send()
    put(rest, rest, last_send, last_recv, twin).wait_recv()
    for q in range(8):
        top_ref[:, q * 128 : (q + 1) * 128] = fin[q * INTER : (q + 1) * INTER, :]
        out_ref[:, q * 128 : (q + 1) * 128] = fin[8 * INTER + q : 8 * INTER + q + 1, :]


def params(**kw):
    return pltpu.CompilerParams(**kw)


def from_partner(block, flip):
    return lax.ppermute(block, "gy", [(y, y ^ flip) for y in range(4)])


def on_device(
    emb_table,
    row_state,
    pair_mask,
    look_rows,
    bag_sizes,
    bag_owner,
    bag_slot,
    dense_vectors,
    labels,
    top_weight,
    out_weight,
):
    mask = pair_mask[0]
    first, second = (mask == 1) | (mask == 2), mask >= 2
    upper, lower = emb_table[: ROWS // 2], emb_table[ROWS // 2 :]
    upper = jnp.where(first, from_partner(upper, 1), upper)
    lower = jnp.where(second, from_partner(lower, 3), lower)

    owners = bag_owner[:, 0]
    onehot = (owners[:, None] == jnp.arange(DEVICES, dtype=i32)[None, :]).astype(i32)
    placed_at = jnp.sum((jnp.cumsum(onehot, axis=0) - onehot) * onehot, axis=1)
    where_to = owners * CAP + placed_at
    spot = (placed_at[:, None] == jnp.arange(CAP, dtype=i32)[None, :]).astype(f32)
    sample, feature = bag_slot // F, bag_slot % F
    bag = jnp.arange(BAGS, dtype=i32)
    pieces = [sample, feature + 1, bag // 16, bag % 16]
    parts = jnp.concatenate([spot * piece.astype(f32)[:, None] for piece in pieces], axis=1)
    coded = mxu(onehot.astype(bf16), parts.astype(bf16), ((0,), (0,))).astype(i32)
    sample_at, feature_at = coded[:, :CAP], coded[:, CAP : 2 * CAP]
    send_slots = jnp.where(feature_at > 0, (feature_at - 1) * B_DEV + sample_at, BAGS)
    send_slots = jnp.pad(send_slots, ((0, 0), (0, 128 - CAP))).reshape(DEVICES, 1, 128)
    send_bags = (coded[:, 2 * CAP : 3 * CAP] * 16 + coded[:, 3 * CAP :]).reshape(DEVICES * CAP)

    sizes = bag_sizes[0]
    ends = jnp.cumsum(sizes)
    starts = ends - sizes
    bounds = jnp.arange(LOOKS // CHUNK, dtype=i32) * CHUNK
    first_bag = jnp.sum((ends[None, :] <= bounds[:, None]).astype(i32), axis=1) // 16 * 16
    extra = C_ROWS - BAGS
    ends2 = jnp.concatenate([ends, jnp.zeros((extra,), i32)]).reshape(C_ROWS // 128, 128)
    starts2 = jnp.concatenate([starts, jnp.full((extra,), LOOKS, i32)]).reshape(C_ROWS // 128, 128)
    upper, lower, look_rows, first_bag, starts2, ends2 = lax.optimization_barrier(
        (upper, lower, look_rows, first_bag, starts2, ends2)
    )
    upper2, lower2 = from_partner(upper, 3), from_partner(lower, 1)
    counts = pl.pallas_call(
        count_kernel,
        out_shape=jax.ShapeDtypeStruct((C_ROWS, ROWS), bf16),
        in_specs=[SMEM, VMEM, VMEM, VMEM],
        out_specs=VMEM,
        scratch_shapes=[pltpu.VMEM((C_ROWS, 128), i32), pltpu.VMEM((C_ROWS, 128), i32)],
        compiler_params=params(vmem_limit_bytes=24 << 20),
        cost_estimate=pl.CostEstimate(flops=2 * LOOKS * SPAN * ROWS, bytes_accessed=10 << 20, transcendentals=0),
        name="count",
    )(first_bag, look_rows.reshape(LOOKS // 128, 128), starts2, ends2)

    dma = pltpu.SemaphoreType.DMA
    got_rows, got_slots, held = pl.pallas_call(
        pool_kernel,
        out_shape=(
            jax.ShapeDtypeStruct((DEVICES * CAP, E), f32),
            jax.ShapeDtypeStruct((DEVICES, 1, 128), i32),
            jax.ShapeDtypeStruct((ROWS, E), f32),
        ),
        in_specs=[SMEM, ANY, VMEM, VMEM, VMEM, VMEM, VMEM, VMEM],
        out_specs=(VMEM, VMEM, VMEM),
        scratch_shapes=[
            pltpu.VMEM((ROWS, 256), bf16),
            pltpu.VMEM((BAGS, E), f32),
            pltpu.VMEM((DEVICES * CAP, E), f32),
            dma,
            dma,
            dma,
            dma,
            pltpu.SMEM((DEVICES * CAP,), i32),
            dma,
        ],
        compiler_params=params(collective_id=0, has_side_effects=True, vmem_limit_bytes=20 << 20),
        name="pool",
    )(pair_mask, send_bags, send_slots, counts, upper, upper2, lower, lower2)
    slot_of = got_slots.reshape(DEVICES * 128)

    sums = pl.pallas_call(
        place_kernel,
        out_shape=jax.ShapeDtypeStruct((BAGS, E), f32),
        in_specs=[ANY, VMEM],
        out_specs=VMEM,
        scratch_shapes=[pltpu.SMEM((DEVICES * 128,), i32), dma((8,))],
        compiler_params=params(vmem_limit_bytes=16 << 20),
        name="place",
    )(slot_of, got_rows)

    results = pl.pallas_call(
        update_kernel,
        out_shape=(
            jax.ShapeDtypeStruct((ROWS, E), f32),
            jax.ShapeDtypeStruct((1, ROWS), f32),
            jax.ShapeDtypeStruct((INTER, HID), f32),
            jax.ShapeDtypeStruct((1, HID), f32),
        ),
        in_specs=[SMEM, ANY, ANY] + [VMEM] * 8,
        out_specs=(VMEM, VMEM, VMEM, VMEM),
        scratch_shapes=[
            pltpu.VMEM((DEVICES * CAP, E), f32),
            pltpu.VMEM((DEVICES * CAP, E), f32),
            pltpu.VMEM((BAGS, E), f32),
            pltpu.VMEM((2 * E, BAGS), bf16),
            pltpu.VMEM((G_ROWS, 128), f32),
            pltpu.VMEM((BAGS + 8, E), f32),
            pltpu.VMEM((INTER, B_DEV), f32),
            pltpu.VMEM((F + 1, E, B_DEV), f32),
            pltpu.VMEM((B_DEV, HID), f32),
            pltpu.VMEM((G_ROWS, 128), f32),
            pltpu.VMEM((HALF, 128), f32),
            pltpu.VMEM((HALF, 128), f32),
            pltpu.VMEM((4, 1, ROWS), f32),
            pltpu.VMEM((12, 4 * SEG, 128), f32),
            pltpu.VMEM((3, 4 * SEG, 128), f32),
            pltpu.VMEM((12, SEG, 128), f32),
            pltpu.VMEM((3, SEG, 128), f32),
            pltpu.VMEM((12, SEG, 128), f32),
            pltpu.SMEM((DEVICES * 128,), i32),
            pltpu.SMEM((BAGS,), i32),
            dma((2,)),
            dma((4,)),
            dma((4,)),
            dma,
            dma,
            dma,
            dma,
            dma,
            dma,
            dma((60,)),
            dma((60,)),
        ],
        compiler_params=params(collective_id=1, has_side_effects=True, vmem_limit_bytes=30 << 20),
        name="update",
    )(
        pair_mask,
        slot_of,
        where_to,
        sums,
        dense_vectors,
        labels[:, None],
        top_weight,
        out_weight[None, :],
        counts,
        held,
        row_state[None, :],
    )
    new_table, new_state, top_grad, out_grad = pl.pallas_call(
        finish_kernel,
        out_shape=tuple(jax.ShapeDtypeStruct(r.shape, f32) for r in results),
        in_specs=[ANY] * 4,
        out_specs=(ANY,) * 4,
        scratch_shapes=[dma((4,))],
        compiler_params=params(vmem_limit_bytes=16 << 20),
        name="finish",
    )(*results)
    return new_table, new_state.reshape(ROWS), top_grad, out_grad.reshape(HID)


def solution(mesh):
    both = ("gx", "gy")
    in_specs = (
        P(both, None),
        P(both),
        P("gx"),
        P(both),
        P(both, None),
        P(both, None),
        P(both),
        P(both, None),
        P(both),
        P(),
        P(),
    )
    out_specs = (P(both, None), P(both), P(), P())
    return jax.shard_map(
        on_device, mesh=mesh, in_specs=in_specs, out_specs=out_specs, check_vma=False
    )
```

```python
import jax
import jax.numpy as jnp
from jax import lax
from jax.experimental import pallas as pl
from jax.experimental.pallas import tpu as pltpu
from jax.sharding import PartitionSpec as P

E = 128
F = 16
B_DEV = 128
BAGS = 2048
ROWS = 2048
LOOKS = 6144
DEVICES = 128
CAP = 32
INTER = 264
HID = 1024
CHUNK = 256
SPAN = CHUNK + 16
C_ROWS = 2304
G_ROWS = 2304
HALF = G_ROWS // 2
SEG = HALF // 48
STRIDE = 91
CUTS = (1, 12, 40, 70, 100, 128)
PAIRS = [(i, j) for i in range(F + 1) for j in range(i + 1, F + 1)]
PAIR_ROW = {pair: 128 + n for n, pair in enumerate(PAIRS)}

learn_rate = 0.05
epsilon = 1e-08
MESH = pl.DeviceIdType.MESH
f32, bf16, i32 = jnp.float32, jnp.bfloat16, jnp.int32

VMEM = pl.BlockSpec(memory_space=pltpu.VMEM)
SMEM = pl.BlockSpec(memory_space=pltpu.SMEM)
ANY = pl.BlockSpec(memory_space=pl.ANY)


def split(x):
    hi = x.astype(bf16)
    return hi, (x - hi.astype(f32)).astype(bf16)


def mxu(a, b, dims):
    return lax.dot_general(a, b, (dims, ((), ())), preferred_element_type=f32)


def dot3(a, b, dims):
    return mxu(a[0], b[0], dims) + (mxu(a[0], b[1], dims) + mxu(a[1], b[0], dims))


NN = ((1,), (0,))
NT = ((1,), (1,))


def down_sublanes(row):
    return jnp.broadcast_to(row, (128, 128)).T


def count_kernel(first_ref, look_ref, start_ref, end_ref, c_ref, start_t, end_t):
    for r in range(C_ROWS // 128):
        here = slice(r * 128, (r + 1) * 128)
        start_t[here, :] = down_sublanes(start_ref[r : r + 1, :])
        end_t[here, :] = down_sublanes(end_ref[r : r + 1, :])
    c_ref[0:16, :] = jnp.zeros((16, ROWS), bf16)
    lane = lax.broadcasted_iota(i32, (1, 128), 1)

    def chunk(t, carry):
        at = pl.multiple_of(first_ref[t], 16)
        start, end = start_t[pl.ds(at, SPAN), :], end_t[pl.ds(at, SPAN), :]
        halves, columns = [], []
        for h in range(2):
            k = lane + (t * CHUNK + h * 128)
            halves.append(((start <= k) & (k < end)).astype(f32).astype(bf16))
            columns.append(down_sublanes(look_ref[pl.ds(2 * t + h, 1), :]))
        in_bag = jnp.concatenate(halves, axis=1)
        column = jnp.concatenate(columns, axis=0)
        for n in range(0, 16, 4):
            of_row = jnp.concatenate(
                [(column == lane + 128 * q).astype(f32).astype(bf16) for q in range(n, n + 4)],
                axis=1,
            )
            counts = mxu(in_bag, of_row, NN)
            cols = slice(n * 128, (n + 4) * 128)
            before = c_ref[pl.ds(at, 16), cols].astype(f32)
            c_ref[pl.ds(at, 16), cols] = (counts[:16] + before).astype(bf16)
            c_ref[pl.ds(pl.multiple_of(at + 16, 16), SPAN - 16), cols] = counts[16:].astype(bf16)
        return carry

    lax.fori_loop(0, LOOKS // CHUNK, chunk, 0, unroll=2)


def device_at(n):
    return (n // 4, n % 4)


def my_number():
    return lax.axis_index("gx") * 4 + lax.axis_index("gy")


def peer_of(k):
    return (my_number() + STRIDE * k) % DEVICES


def greet_all(barrier):
    def greet(k, carry):
        pl.semaphore_signal(barrier, inc=1, device_id=device_at(peer_of(k)), device_id_type=MESH)
        return carry

    lax.fori_loop(1, DEVICES, greet, 0, unroll=32)


def put(src, dst, send, recv, device):
    return pltpu.make_async_remote_copy(
        src_ref=src, dst_ref=dst, send_sem=send, recv_sem=recv, device_id=device, device_id_type=MESH
    )


def chunk_at(n):
    return pl.ds(pl.multiple_of(n * CAP, CAP), CAP)


def pick_rows(dst, to, src, index_ref, at):
    for u in range(CAP):
        dst[pl.ds(to + u, 1), :] = src[pl.ds(index_ref[at + u], 1), :]


def pool_kernel(
    mask_ref,
    bag_in,
    slots_ref,
    c_ref,
    a_ref,
    a2_ref,
    b_ref,
    b2_ref,
    recv_ref,
    got_ref,
    held_ref,
    split_ref,
    partial_ref,
    send_ref,
    row_send,
    row_recv,
    slot_send,
    slot_recv,
    bag_ref,
    bag_sem,
):
    bag_copy = pltpu.make_async_copy(bag_in, bag_ref, bag_sem)
    bag_copy.start()
    barrier = pltpu.get_barrier_semaphore()
    greet_all(barrier)
    me = my_number()
    mask = jnp.full((ROWS // 2, E), mask_ref[0], i32)
    held_ref[: ROWS // 2, :] = jnp.where(mask >= 2, a2_ref[...], a_ref[...])
    held_ref[ROWS // 2 :, :] = jnp.where((mask == 1) | (mask == 2), b2_ref[...], b_ref[...])
    hi, lo = split(held_ref[...])
    split_ref[:, :128] = hi
    split_ref[:, 128:] = lo

    def block(m, carry):
        at = pl.multiple_of(m * 256, 256)
        both = mxu(c_ref[pl.ds(at, 256), :], split_ref[...], NN)
        partial_ref[pl.ds(at, 256), :] = both[:, :128] + both[:, 128:]
        return carry

    lax.fori_loop(0, BAGS // 256, block, 0)
    got_ref[me] = slots_ref[me]
    bag_copy.wait()
    pick_rows(recv_ref, me * CAP, partial_ref, bag_ref, me * CAP)

    def ready(k):
        at = peer_of(k) * CAP
        pick_rows(send_ref, at, partial_ref, bag_ref, at)

    def start(k):
        peer = peer_of(k)
        to = device_at(peer)
        put(slots_ref.at[peer], got_ref.at[me], slot_send, slot_recv, to).start()
        put(send_ref.at[chunk_at(peer)], recv_ref.at[chunk_at(me)], row_send, row_recv, to).start()

    ready(1)
    pl.semaphore_wait(barrier, DEVICES - 1)

    def step(k, carry):
        ready(k)
        start(k - 1)
        return carry

    lax.fori_loop(2, DEVICES, step, 0, unroll=2)
    start(DEVICES - 1)
    to = device_at(peer_of(1))
    some = pl.ds(0, DEVICES - 1)
    put(slots_ref.at[some], got_ref.at[some], slot_send, slot_recv, to).wait()
    rows = pl.ds(0, (DEVICES - 1) * CAP)
    put(send_ref.at[rows], recv_ref.at[rows], row_send, row_recv, to).wait()


def place_kernel(slot_in, got_ref, pooled, slot_ref, sems):
    part = DEVICES * 128 // 8
    copies = []
    for q in range(8):
        here = pl.ds(q * part, part)
        copies.append(pltpu.make_async_copy(slot_in.at[here], slot_ref.at[here], sems.at[q]))
        copies[q].start()

    def place(c, carry):
        @pl.when(slot_ref[c * 128] < BAGS)
        def _():
            for u in range(CAP):
                pooled[pl.ds(slot_ref[c * 128 + u], 1), :] = got_ref[pl.ds(c * CAP + u, 1), :]

        return carry

    for q in range(8):
        copies[q].wait()
        lax.fori_loop(q * DEVICES // 8, (q + 1) * DEVICES // 8, place, 0)


def finish_kernel(a, b, c, d, to_a, to_b, to_c, to_d, sems):
    pairs = ((a, to_a), (b, to_b), (c, to_c), (d, to_d))
    copies = [pltpu.make_async_copy(x, y, sems.at[n]) for n, (x, y) in enumerate(pairs)]
    for copy in copies:
        copy.start()
    for copy in copies:
        copy.wait()


def update_kernel(
    mask_ref,
    slot_in,
    where_in,
    sums_ref,
    dense_ref,
    label_ref,
    w_ref,
    wo_ref,
    c_ref,
    table_ref,
    state_ref,
    new_table_ref,
    new_state_ref,
    top_ref,
    out_ref,
    back,
    came,
    grads,
    sides,
    fin,
    pooled,
    inter_t,
    vt,
    d_pre_ref,
    grad_ref,
    r1,
    acc,
    states,
    ra,
    part_a,
    rb,
    mine,
    rc,
    slot_ref,
    where_ref,
    table_sem,
    state_send,
    state_recv,
    row_send,
    row_recv,
    swap_send,
    swap_recv,
    last_send,
    last_recv,
    color_send,
    color_recv,
):
    tables = [
        pltpu.make_async_copy(slot_in, slot_ref, table_sem.at[0]),
        pltpu.make_async_copy(where_in, where_ref, table_sem.at[1]),
    ]
    for copy in tables:
        copy.start()
    barrier = pltpu.get_barrier_semaphore()
    greet_all(barrier)
    me = my_number()
    gx, x = lax.axis_index("gx"), lax.axis_index("gy")
    yz, core = gx // 2, gx % 2
    twin = (gx + 1 - 2 * core, x)

    y, z = yz // 4, yz % 4

    def along_x(k):
        return (gx, (x + k) % 4)

    def along_y(k):
        return (((y + k) % 4 * 4 + z) * 2 + core, x)

    def along_z(k):
        return ((y * 4 + (z + k) % 4) * 2 + core, x)

    dense_t = dense_ref[...].T
    vt[0] = dense_t
    inter_t[0:128, :] = dense_t
    for f in range(F):
        vt[f + 1] = sums_ref[f * 128 : (f + 1) * 128, :].T
    for i in range(F):
        for j in range(i + 1, F + 1):
            row = PAIR_ROW[i, j]
            inter_t[row : row + 1, :] = jnp.sum(vt[i] * vt[j], axis=0, keepdims=True)

    it = inter_t[...]
    w = split(w_ref[...])
    pre = dot3(split(it.T), w, NN)
    sig = 1.0 / (1.0 + jnp.exp(-pre))
    hidden = pre * sig
    logits = jnp.sum(hidden * wo_ref[...], axis=1, keepdims=True)
    d_logits = 1.0 / (1.0 + jnp.exp(-logits)) - label_ref[...]
    out_grad = jnp.sum(hidden * d_logits, axis=0, keepdims=True)
    for q in range(8):
        grad_ref[8 * INTER + q : 8 * INTER + q + 1, :] = out_grad[:, q * 128 : (q + 1) * 128]
    grad_ref[8 * INTER + 8 :, :] = jnp.zeros((G_ROWS - 8 * INTER - 8, 128), f32)
    d_pre_ref[...] = d_logits * wo_ref[...] * (sig * (1.0 + pre * (1.0 - sig)))
    d_pre = split(d_pre_ref[...])
    top_grad = dot3(split(it), d_pre, NN)
    for q in range(8):
        grad_ref[q * INTER : (q + 1) * INTER, :] = top_grad[:, q * 128 : (q + 1) * 128]
    inter_t[...] = dot3(w, d_pre, NT)

    def pooled_grad(j):
        total = None
        for i in range(F + 1):
            if i != j:
                row = PAIR_ROW[min(i, j), max(i, j)]
                term = inter_t[row : row + 1, :] * vt[i]
                total = term if total is None else total + term
        pooled[(j - 1) * 128 : j * 128, :] = total.T

    for j in range(1, 7):
        pooled_grad(j)

    my_half = pl.multiple_of(core * HALF, 8)
    other = pl.multiple_of((1 - core) * HALF, 8)
    pl.semaphore_wait(barrier, DEVICES - 1)
    swap = put(grad_ref.at[pl.ds(other, HALF)], r1, swap_send, swap_recv, twin)
    swap.start()
    flips = [None, x + 1 - 2 * (x % 2), (x + 2) % 4, 3 - x]
    state_moves = [
        put(state_ref, states.at[f], state_send.at[f], state_recv.at[f], (gx, flips[f]))
        for f in range(1, 4)
    ]
    for move in state_moves:
        move.start()
    for j in range(7, F + 1):
        pooled_grad(j)
    pooled[BAGS:, :] = jnp.zeros((8, E), f32)

    def ready(k):
        peer = peer_of(k)
        pick_rows(back, peer * CAP, pooled, slot_ref, peer * 128)

    def start(k):
        peer = peer_of(k)
        put(
            back.at[chunk_at(peer)], came.at[chunk_at(me)], row_send, row_recv, device_at(peer)
        ).start()

    def send_rows(n):
        def step(k, carry):
            ready(k + 1)
            start(k)
            return carry

        last = DEVICES - 1 if CUTS[n + 1] == DEVICES else CUTS[n + 1]
        lax.fori_loop(CUTS[n], last, step, 0, unroll=2)
        if last < CUTS[n + 1]:
            start(last)

    class Color:
        def __init__(self, n, at, to):
            self.n, self.at = n, at
            self.to = (to[0], to[1], to[2], to[1], to[0])
            self.base = n * 16 * SEG

        def move(self, phase, k, src, dst):
            sem = (self.n * 5 + phase) * 4 + k
            return put(src, dst, color_send.at[sem], color_recv.at[sem], self.to[phase](k))

        def rows_a(self, a, base):
            return pl.ds(pl.multiple_of(base + self.base + a * (4 * SEG), 8), 4 * SEG)

        def rows_b(self, a, b, base):
            return pl.ds(pl.multiple_of(base + self.base + (a * 4 + b) * SEG, 8), SEG)

        def moves(self, phase, waiting):
            n = self.n
            a, b, c = self.at
            out = []
            for k in range(1, 4):
                if phase == 0:
                    there = acc.at[self.rows_a((a + k) % 4, 0)]
                    out.append(self.move(0, k, there, ra.at[4 * n + k]))
                if phase == 1:
                    there = pl.ds(pl.multiple_of((b + k) % 4 * SEG, 8), SEG)
                    out.append(self.move(1, k, part_a.at[n, there], rb.at[4 * n + k]))
                if phase == 2:
                    slot = (c + 4 - k) % 4 if waiting else c
                    out.append(self.move(2, k, mine.at[n], rc.at[4 * n + slot]))
                if phase == 3:
                    who = (b + 4 - k) % 4 if waiting else b
                    there = fin.at[self.rows_b(a, who, my_half)]
                    out.append(self.move(3, k, there, there))
                if phase == 4:
                    who = (a + 4 - k) % 4 if waiting else a
                    there = fin.at[self.rows_a(who, my_half)]
                    out.append(self.move(4, k, there, there))
            return out

        def begin(self, phase):
            for copy in self.moves(phase, False):
                copy.start()

        def finish(self, phase):
            for copy in self.moves(phase, False):
                copy.wait_send()
            for copy in self.moves(phase, True):
                copy.wait_recv()
            n = self.n
            a, b, c = self.at
            if phase == 0:
                own = acc[self.rows_a(a, 0), :]
                part_a[n] = (own + ra[4 * n + 1]) + (ra[4 * n + 2] + ra[4 * n + 3])
            if phase == 1:
                own = part_a[n, pl.ds(pl.multiple_of(b * SEG, 8), SEG), :]
                part = (own + rb[4 * n + 1]) + (rb[4 * n + 2] + rb[4 * n + 3])
                mine[n] = part
                rc[4 * n + c] = part
            if phase == 2:
                whole = (rc[4 * n] + rc[4 * n + 1]) + (rc[4 * n + 2] + rc[4 * n + 3])
                fin[self.rows_b(a, b, my_half), :] = whole

    colors = (
        Color(0, (z, y, x), (along_z, along_y, along_x)),
        Color(1, (y, x, z), (along_y, along_x, along_z)),
        Color(2, (x, z, y), (along_x, along_z, along_y)),
    )

    def phase_on(phase):
        for color in colors:
            color.begin(phase)

    def phase_off(phase):
        for color in colors:
            color.finish(phase)

    tables[0].wait()
    pick_rows(came, me * CAP, pooled, slot_ref, me * 128)
    ready(1)
    send_rows(0)
    swap.wait()
    acc[...] = grad_ref[pl.ds(my_half, HALF), :] + r1[...]
    phase_on(0)
    for phase in range(4):
        send_rows(phase + 1)
        phase_off(phase)
        phase_on(phase + 1)

    rows = pl.ds(0, (DEVICES - 1) * CAP)
    put(back.at[rows], came.at[rows], row_send, row_recv, device_at(peer_of(1))).wait()
    tables[1].wait()
    for move in state_moves:
        move.wait()
    mask = jnp.full((1, ROWS), mask_ref[0], i32)
    held_state = state_ref[...]
    for f in range(1, 4):
        held_state = jnp.where(mask == f, states[f], held_state)
    states[0] = held_state

    def take(n, carry):
        pick_rows(grads, n * CAP, came, where_ref, n * CAP)
        return carry

    lax.fori_loop(0, BAGS // CAP, take, 0)
    for q in range(BAGS // 128):
        here = slice(q * 128, (q + 1) * 128)
        hi, lo = split(grads[here, :].T)
        sides[0:128, here] = hi
        sides[128:256, here] = lo

    phase_off(4)
    half = fin.at[pl.ds(my_half, HALF)]
    rest = fin.at[pl.ds(other, HALF)]
    last = put(half, half, last_send, last_recv, twin)
    last.start()

    def block(n, carry):
        here = pl.ds(pl.multiple_of(n * 256, 256), 256)
        both = mxu(sides[...], c_ref[0:BAGS, here], NN)
        row_grad = both[:128] + both[128:]
        state = states[0, :, here] + jnp.sum(row_grad * row_grad, axis=0, keepdims=True) * (1.0 / E)
        new_state_ref[:, here] = state
        step = row_grad * (learn_rate / (jnp.sqrt(state) + epsilon))
        new_table_ref[here, :] = table_ref[here, :] - step.T
        return carry

    lax.fori_loop(0, ROWS // 256, block, 0)

    last.wait_send()
    put(rest, rest, last_send, last_recv, twin).wait_recv()
    for q in range(8):
        top_ref[:, q * 128 : (q + 1) * 128] = fin[q * INTER : (q + 1) * INTER, :]
        out_ref[:, q * 128 : (q + 1) * 128] = fin[8 * INTER + q : 8 * INTER + q + 1, :]


def params(**kw):
    return pltpu.CompilerParams(**kw)


def from_partner(block, flip):
    return lax.ppermute(block, "gy", [(y, y ^ flip) for y in range(4)])


def on_device(
    emb_table,
    row_state,
    pair_mask,
    look_rows,
    bag_sizes,
    bag_owner,
    bag_slot,
    dense_vectors,
    labels,
    top_weight,
    out_weight,
):
    mask = pair_mask[0]
    first, second = (mask == 1) | (mask == 2), mask >= 2
    upper, lower = emb_table[: ROWS // 2], emb_table[ROWS // 2 :]
    upper = jnp.where(first, from_partner(upper, 1), upper)
    lower = jnp.where(second, from_partner(lower, 3), lower)

    owners = bag_owner[:, 0]
    onehot = (owners[:, None] == jnp.arange(DEVICES, dtype=i32)[None, :]).astype(i32)
    placed_at = jnp.sum((jnp.cumsum(onehot, axis=0) - onehot) * onehot, axis=1)
    where_to = owners * CAP + placed_at
    spot = (placed_at[:, None] == jnp.arange(CAP, dtype=i32)[None, :]).astype(f32)
    sample, feature = bag_slot // F, bag_slot % F
    bag = jnp.arange(BAGS, dtype=i32)
    pieces = [sample, feature + 1, bag // 16, bag % 16]
    parts = jnp.concatenate([spot * piece.astype(f32)[:, None] for piece in pieces], axis=1)
    coded = mxu(onehot.astype(bf16), parts.astype(bf16), ((0,), (0,))).astype(i32)
    sample_at, feature_at = coded[:, :CAP], coded[:, CAP : 2 * CAP]
    send_slots = jnp.where(feature_at > 0, (feature_at - 1) * B_DEV + sample_at, BAGS)
    send_slots = jnp.pad(send_slots, ((0, 0), (0, 128 - CAP))).reshape(DEVICES, 1, 128)
    send_bags = (coded[:, 2 * CAP : 3 * CAP] * 16 + coded[:, 3 * CAP :]).reshape(DEVICES * CAP)

    sizes = bag_sizes[0]
    ends = jnp.cumsum(sizes)
    starts = ends - sizes
    bounds = jnp.arange(LOOKS // CHUNK, dtype=i32) * CHUNK
    first_bag = jnp.sum((ends[None, :] <= bounds[:, None]).astype(i32), axis=1) // 16 * 16
    extra = C_ROWS - BAGS
    ends2 = jnp.concatenate([ends, jnp.zeros((extra,), i32)]).reshape(C_ROWS // 128, 128)
    starts2 = jnp.concatenate([starts, jnp.full((extra,), LOOKS, i32)]).reshape(C_ROWS // 128, 128)
    upper, lower, look_rows, first_bag, starts2, ends2 = lax.optimization_barrier(
        (upper, lower, look_rows, first_bag, starts2, ends2)
    )
    upper2, lower2 = from_partner(upper, 3), from_partner(lower, 1)
    counts = pl.pallas_call(
        count_kernel,
        out_shape=jax.ShapeDtypeStruct((C_ROWS, ROWS), bf16),
        in_specs=[SMEM, VMEM, VMEM, VMEM],
        out_specs=VMEM,
        scratch_shapes=[pltpu.VMEM((C_ROWS, 128), i32), pltpu.VMEM((C_ROWS, 128), i32)],
        compiler_params=params(vmem_limit_bytes=24 << 20),
        cost_estimate=pl.CostEstimate(flops=2 * LOOKS * SPAN * ROWS, bytes_accessed=10 << 20, transcendentals=0),
        name="count",
    )(first_bag, look_rows.reshape(LOOKS // 128, 128), starts2, ends2)

    dma = pltpu.SemaphoreType.DMA
    got_rows, got_slots, held = pl.pallas_call(
        pool_kernel,
        out_shape=(
            jax.ShapeDtypeStruct((DEVICES * CAP, E), f32),
            jax.ShapeDtypeStruct((DEVICES, 1, 128), i32),
            jax.ShapeDtypeStruct((ROWS, E), f32),
        ),
        in_specs=[SMEM, ANY, VMEM, VMEM, VMEM, VMEM, VMEM, VMEM],
        out_specs=(VMEM, VMEM, VMEM),
        scratch_shapes=[
            pltpu.VMEM((ROWS, 256), bf16),
            pltpu.VMEM((BAGS, E), f32),
            pltpu.VMEM((DEVICES * CAP, E), f32),
            dma,
            dma,
            dma,
            dma,
            pltpu.SMEM((DEVICES * CAP,), i32),
            dma,
        ],
        compiler_params=params(collective_id=0, has_side_effects=True, vmem_limit_bytes=20 << 20),
        name="pool",
    )(pair_mask, send_bags, send_slots, counts, upper, upper2, lower, lower2)
    slot_of = got_slots.reshape(DEVICES * 128)

    sums = pl.pallas_call(
        place_kernel,
        out_shape=jax.ShapeDtypeStruct((BAGS, E), f32),
        in_specs=[ANY, VMEM],
        out_specs=VMEM,
        scratch_shapes=[pltpu.SMEM((DEVICES * 128,), i32), dma((8,))],
        compiler_params=params(vmem_limit_bytes=16 << 20),
        name="place",
    )(slot_of, got_rows)

    results = pl.pallas_call(
        update_kernel,
        out_shape=(
            jax.ShapeDtypeStruct((ROWS, E), f32),
            jax.ShapeDtypeStruct((1, ROWS), f32),
            jax.ShapeDtypeStruct((INTER, HID), f32),
            jax.ShapeDtypeStruct((1, HID), f32),
        ),
        in_specs=[SMEM, ANY, ANY] + [VMEM] * 8,
        out_specs=(VMEM, VMEM, VMEM, VMEM),
        scratch_shapes=[
            pltpu.VMEM((DEVICES * CAP, E), f32),
            pltpu.VMEM((DEVICES * CAP, E), f32),
            pltpu.VMEM((BAGS, E), f32),
            pltpu.VMEM((2 * E, BAGS), bf16),
            pltpu.VMEM((G_ROWS, 128), f32),
            pltpu.VMEM((BAGS + 8, E), f32),
            pltpu.VMEM((INTER, B_DEV), f32),
            pltpu.VMEM((F + 1, E, B_DEV), f32),
            pltpu.VMEM((B_DEV, HID), f32),
            pltpu.VMEM((G_ROWS, 128), f32),
            pltpu.VMEM((HALF, 128), f32),
            pltpu.VMEM((HALF, 128), f32),
            pltpu.VMEM((4, 1, ROWS), f32),
            pltpu.VMEM((12, 4 * SEG, 128), f32),
            pltpu.VMEM((3, 4 * SEG, 128), f32),
            pltpu.VMEM((12, SEG, 128), f32),
            pltpu.VMEM((3, SEG, 128), f32),
            pltpu.VMEM((12, SEG, 128), f32),
            pltpu.SMEM((DEVICES * 128,), i32),
            pltpu.SMEM((BAGS,), i32),
            dma((2,)),
            dma((4,)),
            dma((4,)),
            dma,
            dma,
            dma,
            dma,
            dma,
            dma,
            dma((60,)),
            dma((60,)),
        ],
        compiler_params=params(collective_id=1, has_side_effects=True, vmem_limit_bytes=30 << 20),
        name="update",
    )(
        pair_mask,
        slot_of,
        where_to,
        sums,
        dense_vectors,
        labels[:, None],
        top_weight,
        out_weight[None, :],
        counts,
        held,
        row_state[None, :],
    )
    new_table, new_state, top_grad, out_grad = pl.pallas_call(
        finish_kernel,
        out_shape=tuple(jax.ShapeDtypeStruct(r.shape, f32) for r in results),
        in_specs=[ANY] * 4,
        out_specs=(ANY,) * 4,
        scratch_shapes=[dma((4,))],
        compiler_params=params(vmem_limit_bytes=16 << 20),
        name="finish",
    )(*results)
    return new_table, new_state.reshape(ROWS), top_grad, out_grad.reshape(HID)


def solution(mesh):
    both = ("gx", "gy")
    in_specs = (
        P(both, None),
        P(both),
        P("gx"),
        P(both),
        P(both, None),
        P(both, None),
        P(both),
        P(both, None),
        P(both),
        P(),
        P(),
    )
    out_specs = (P(both, None), P(both), P(), P())
    return jax.shard_map(
        on_device, mesh=mesh, in_specs=in_specs, out_specs=out_specs, check_vma=False
    )
```
